32 devices in a mesh: member: 2 (over y), gx: 4 (over z), gy: 4 (over x, core).
Axes of the slice: x: 2, y: 2, z: 4, core: 2. Of those that a mesh axis runs over, the one named last changes fastest.
Arguments:
- populations: float32 [19, 32, 64, 128], P(None, ('member', 'gx'), 'gy'), parts along dimension 1, may hold values from 0 to 1, as said below
- heat_level: int32 [32, 64, 128], P(('member', 'gx'), 'gy'), parts along dimension 0, may hold values from 0 to 7
- obstacle: int32 [32, 64, 128], P(('member', 'gx'), 'gy'), parts along dimension 0, may hold values 0 or 1
- heat_table: float32 [8], replicated, may hold values from 0.02 to 0.5
Outputs:
- final_populations: float32 [19, 32, 64, 128], P(None, ('member', 'gx'), 'gy'), parts along dimension 1
- velocity: float32 [3, 32, 64, 128], P(None, ('member', 'gx'), 'gy'), parts along dimension 1
The draws below stay inside these ranges and needn't reach their ends.
There are 2 independent parts, one for each index of `member`. The reference program is written for one: setup_inputs(seed, part) draws one part's arguments, and reference() takes and returns one part's arrays. A program takes and returns all parts, laid end to end along the dimension named above; an argument that names none is the same for every part. Nothing has to cross between parts.
Inputs may be any that keep to these rules, and one draw needn't show every extreme that they name: Positive populations near a local equilibrium, in the direction order of the steps.
All inputs are finite; a program needn't handle non-finite values. No bound on the sum of `obstacle` on one device may be relied on, other than what follows from the above.
Results may differ from the reference program's by a relative error of at most 0.0001.
Values sent between devices are 32-bit elements; how exact they have to be, the bound alone decides.
A program may use at most 64 MiB of HBM per device.

```python
import math
import jax
import jax.numpy as jnp
import numpy as np
from jax import lax

NZ = 128
STEPS = 2
LEVELS = 8
NX = 16
NY = 64


lattice = np.array([[0, 0, 0], [1, 0, 0], [-1, 0, 0], [0, 1, 0], [0, -1, 0], [0, 0, 1], [0, 0, -1], [1, 1, 0], [-1, -1, 0], [1, -1, 0], [-1, 1, 0], [1, 0, 1], [-1, 0, -1], [1, 0, -1], [-1, 0, 1], [0, 1, 1], [0, -1, -1], [0, 1, -1], [0, -1, 1]])


lattice_weight = [1.0 / 3.0] + [1.0 / 18.0] * 6 + [1.0 / 36.0] * 12


def draw_populations(key, part):
    key_one, key_two, key_three, key_four, key_five, key_six, key_seven = jax.random.split(jax.random.fold_in(key, 11), 7)
    grid_x = lax.broadcasted_iota(jnp.float32, (NX, NY, NZ), 0)
    grid_y = lax.broadcasted_iota(jnp.float32, (NX, NY, NZ), 1)
    amplitude = jnp.exp(jax.random.uniform(key_four, (), jnp.float32, math.log(0.01), math.log(0.03)))
    speed_ramp = amplitude * (1.0 + grid_x / NX + grid_y / NY)
    sample = jnp.clip(jax.random.normal(key_one, (3, NX, NY, NZ), jnp.float32), -2.5, 2.5)
    density = 1.0 + jax.random.uniform(key_two, (NX, NY, NZ), jnp.float32, -0.05, 0.05)
    velocity = sample * speed_ramp[None]
    plant_speed = jax.random.uniform(key_five, (), jnp.float32, 0.15, 0.4)
    plant_angle = jax.random.uniform(key_six, (), jnp.float32, -math.pi, math.pi)
    key_cx, key_cy, key_cz = jax.random.split(key_seven, 3)
    centre_x = jax.random.randint(key_cx, (), 2, NX - 2)
    centre_y = jax.random.randint(key_cy, (), 3, NY - 3)
    centre_z = jax.random.randint(key_cz, (), 3, NZ - 3)
    index_x = lax.broadcasted_iota(jnp.int32, (NX, NY, NZ), 0)
    index_y = lax.broadcasted_iota(jnp.int32, (NX, NY, NZ), 1)
    index_z = lax.broadcasted_iota(jnp.int32, (NX, NY, NZ), 2)
    region = (jnp.abs(index_x - centre_x) <= 2) & (jnp.abs(index_y - centre_y) <= 2) & (jnp.abs(index_z - centre_z) <= 2)
    planted = plant_speed * jnp.stack([0.9 * jnp.cos(plant_angle), 0.9 * jnp.sin(plant_angle), jnp.float32(0.436)])
    velocity = jnp.where(region[None], planted[:, None, None, None], velocity)
    jitter = jnp.clip(jax.random.normal(key_three, (19, NX, NY, NZ), jnp.float32), -3.0, 3.0)
    speed_sq = velocity[0] * velocity[0] + velocity[1] * velocity[1] + velocity[2] * velocity[2]
    pieces = []
    for number in range(19):
        project = float(lattice[number][0]) * velocity[0] + float(lattice[number][1]) * velocity[1] + float(lattice[number][2]) * velocity[2]
        equilibrium = lattice_weight[number] * density * (1.0 + 3.0 * project + 4.5 * project * project - 1.5 * speed_sq)
        pieces.append(equilibrium * (1.0 + 0.05 * jitter[number]))
    return jnp.stack(pieces).astype(jnp.float32)


def with_ends(values, own_key, least, top_value):
    index_at = [jax.random.randint(jax.random.fold_in(own_key, axis), (), 0, length) for axis, length in enumerate(values.shape)]
    main_axis = values.shape.index(max(values.shape))
    next_to = index_at[:main_axis] + [(index_at[main_axis] + 1) % values.shape[main_axis]] + index_at[main_axis + 1:]
    return values.at[tuple(index_at)].set(least).at[tuple(next_to)].set(top_value)


def setup_inputs(seed: int = 0, part: int = 0) -> dict:
    key_of = jax.random.split(jax.random.key(seed), 5)
    own_keys = jax.random.split(jax.random.fold_in(key_of[4], part), 5)
    populations = draw_populations(jax.random.fold_in(jax.random.fold_in(key_of[4], part), 71), part)
    heat_level = with_ends(jax.random.randint(own_keys[1], (NX, NY, NZ), 0, LEVELS), jax.random.fold_in(own_keys[1], 1), 0, LEVELS - 1).astype(jnp.int32)
    obstacle = with_ends((jax.random.randint(own_keys[2], (NX, NY, NZ), 0, 10) < 1).astype(jnp.int32), jax.random.fold_in(own_keys[2], 1), 0, 1)
    heat_table = jnp.clip(jnp.exp(jax.random.uniform(key_of[3], (LEVELS,), jnp.float32, math.log(0.02), math.log(0.5))), 0.02, 0.5)
    return {"populations": populations, "heat_level": heat_level, "obstacle": obstacle, "heat_table": heat_table}


lattice = np.array([[0, 0, 0], [1, 0, 0], [-1, 0, 0], [0, 1, 0], [0, -1, 0], [0, 0, 1], [0, 0, -1], [1, 1, 0], [-1, -1, 0], [1, -1, 0], [-1, 1, 0], [1, 0, 1], [-1, 0, -1], [1, 0, -1], [-1, 0, 1], [0, 1, 1], [0, -1, -1], [0, 1, -1], [0, -1, 1]])
lattice_weight = [1.0 / 3.0] + [1.0 / 18.0] * 6 + [1.0 / 36.0] * 12
opposite = [0, 2, 1, 4, 3, 6, 5, 8, 7, 10, 9, 12, 11, 14, 13, 16, 15, 18, 17]
base_tau = 0.52
smag_coef = 0.04
speed_cap = 0.1
strain_floor = 1e-06

def stream_all(padded, span_x, span_y, depth_z):
    pieces = []
    for number in range(19):
        shift_x = int(lattice[number][0])
        shift_y = int(lattice[number][1])
        shift_z = int(lattice[number][2])
        pieces.append(padded[number, 1 - shift_x:1 - shift_x + span_x, 1 - shift_y:1 - shift_y + span_y, 1 - shift_z:1 - shift_z + depth_z])
    return jnp.stack(pieces)

def moments(read, solid):
    density = lax.optimization_barrier(jnp.sum(read, axis=0))
    components = []
    for component in range(3):
        moment = jnp.zeros(density.shape, jnp.float32)
        for number in range(19):
            factor = int(lattice[number][component])
            if factor != 0:
                moment = moment + float(factor) * read[number]
        components.append(moment)
    momentum = jnp.stack(components)
    safe_density = jnp.where(solid, 1.0, density)
    velocity = jnp.where(solid[None], 0.0, momentum / safe_density[None])
    return (density, velocity)

def strain_size(vel_wide):
    padded = jnp.pad(vel_wide, ((0, 0), (0, 0), (0, 0), (1, 1)))
    gradient = [(padded[:, 2:, 1:-1, 1:-1] - padded[:, :-2, 1:-1, 1:-1]) * 0.5, (padded[:, 1:-1, 2:, 1:-1] - padded[:, 1:-1, :-2, 1:-1]) * 0.5, (padded[:, 1:-1, 1:-1, 2:] - padded[:, 1:-1, 1:-1, :-2]) * 0.5]
    strain_sum = jnp.zeros(gradient[0].shape[1:], jnp.float32)
    for row_axis in range(3):
        for col_axis in range(3):
            strain_ab = 0.5 * (gradient[col_axis][row_axis] + gradient[row_axis][col_axis])
            strain_sum = strain_sum + strain_ab * strain_ab
    return jnp.sqrt(2.0 * strain_sum + strain_floor)

def collide(read, density, velocity, solid, magnitude, lift_force):
    relax_time = base_tau + 3.0 * smag_coef * magnitude
    speed_sq = velocity[0] * velocity[0] + velocity[1] * velocity[1] + velocity[2] * velocity[2]
    collided = []
    for number in range(19):
        project = float(lattice[number][0]) * velocity[0] + float(lattice[number][1]) * velocity[1] + float(lattice[number][2]) * velocity[2]
        equilibrium = lattice_weight[number] * density * (1.0 + 3.0 * project + 4.5 * project * project - 1.5 * speed_sq)
        fluid_post = read[number] - (read[number] - equilibrium) / relax_time + 3.0 * lattice_weight[number] * float(lattice[number][2]) * lift_force
        collided.append(jnp.where(solid, read[opposite[number]], fluid_post))
    return jnp.stack(collided)

def lookup(heat_level, heat_table):
    heat_force = jnp.zeros(heat_level.shape, jnp.float32)
    for level_no in range(heat_table.shape[0]):
        heat_force = heat_force + jnp.where(heat_level == level_no, heat_table[level_no], 0.0)
    return heat_force

def reference(populations, heat_level, obstacle, heat_table):
    grid_y = lax.broadcasted_iota(jnp.int32, (NX, NY, NZ), 1)
    grid_z = lax.broadcasted_iota(jnp.int32, (NX, NY, NZ), 2)
    solid = (obstacle == 1) | (grid_y == 0) | (grid_y == NY - 1) | (grid_z == 0) | (grid_z == NZ - 1)
    heat_force = lookup(heat_level, heat_table)
    current = populations
    velocity = jnp.zeros((3, NX, NY, NZ), jnp.float32)
    for repeat in range(STEPS):
        padded = jnp.pad(current, ((0, 0), (1, 1), (0, 0), (0, 0)), mode='wrap')
        padded = jnp.pad(padded, ((0, 0), (0, 0), (1, 1), (1, 1)))
        read = stream_all(padded, NX, NY, NZ)
        density, velocity = moments(read, solid)
        peak_speed = jnp.max(velocity[0] * velocity[0] + velocity[1] * velocity[1] + velocity[2] * velocity[2])
        force_scale = speed_cap / jnp.sqrt(speed_cap * speed_cap + peak_speed)
        vel_wide = jnp.pad(velocity, ((0, 0), (1, 1), (0, 0), (0, 0)), mode='wrap')
        vel_wide = jnp.pad(vel_wide, ((0, 0), (0, 0), (1, 1), (0, 0)))
        magnitude = strain_size(vel_wide)
        current = collide(read, density, velocity, solid, magnitude, force_scale * heat_force)
    return (current, velocity)
```

```python
import functools

import jax
import jax.numpy as jnp
import numpy as np
from jax import lax
from jax.experimental import pallas as pl
from jax.experimental.pallas import tpu as pltpu
from jax.sharding import PartitionSpec as P

STEPS = 2
ROW = 8

lattice = np.array(
    [
        [0, 0, 0],
        [1, 0, 0],
        [-1, 0, 0],
        [0, 1, 0],
        [0, -1, 0],
        [0, 0, 1],
        [0, 0, -1],
        [1, 1, 0],
        [-1, -1, 0],
        [1, -1, 0],
        [-1, 1, 0],
        [1, 0, 1],
        [-1, 0, -1],
        [1, 0, -1],
        [-1, 0, 1],
        [0, 1, 1],
        [0, -1, -1],
        [0, 1, -1],
        [0, -1, 1],
    ]
)
CS = [tuple(int(c) for c in row) for row in lattice]
NUMBER = {c: k for k, c in enumerate(CS)}
WEIGHT = [1.0 / 3.0] + [1.0 / 18.0] * 6 + [1.0 / 36.0] * 12
OPP = [0, 2, 1, 4, 3, 6, 5, 8, 7, 10, 9, 12, 11, 14, 13, 16, 15, 18, 17]
base_tau = 0.52
smag_coef = 0.04
speed_cap = 0.1
strain_floor = 1e-06
LIFTED = [k for k in range(19) if CS[k][2] != 0]
ACROSS_X = {c: [NUMBER[(c, 0, 0)], NUMBER[(c, 1, 0)], NUMBER[(c, -1, 0)], NUMBER[(c, 0, 1)], NUMBER[(c, 0, -1)]] for c in (1, -1)}
ACROSS_Y = {c: [NUMBER[(0, c, 0)], NUMBER[(1, c, 0)], NUMBER[(-1, c, 0)], NUMBER[(0, c, 1)], NUMBER[(0, c, -1)]] for c in (1, -1)}
OUT = (-1, 1)
IN = (1, -1)


def tree_sum(items):
    items = list(items)
    while len(items) > 1:
        items = [items[i] + items[i + 1] if i + 1 < len(items) else items[i] for i in range(0, len(items), 2)]
    return items[0]


def peak_groups(ngx, ngy):
    if ngx * ngy <= 64:
        return [[(dx, dy) for dx in range(ngx) for dy in range(ngy) if dx or dy]]
    return [[(0, dy) for dy in range(1, ngy)], [(dx, 0) for dx in range(1, ngx)]]


def kernel(
    ngx, ngy,
    pops, heat_level, obstacle, table,
    out_p, out_v,
    st0, st1, rd, ms, rho_s, vel, hl, ob, tb, solid_s,
    hb, hzp, hzm, hm, hmy,
    xr, xm_out, xm_in, yb_out, yb_in, cg, cm_out, cr_in, cm_in,
    ox, oy, dr, dm, tu, ex, ey, gfx, gfy, pm_src, *rest,
):
    (*pm_bufs, load_sem, xr_send, xr_recv, xm_send, xm_recv, yr_send, yr_recv, ym_send, ym_recv,
     cr_send, cr_recv, cm_send, cm_recv, h_send, h_recv, p_send, p_recv) = rest
    _, sx, sy, nz = pops.shape
    levels = table.shape[0]
    gx = lax.axis_index("gx")
    gy = lax.axis_index("gy")
    has_up = gy < ngy - 1
    has_down = gy > 0
    right = lax.rem(gx + 1, ngx)
    left = lax.rem(gx + ngx - 1, ngx)
    own_y = pl.ds(ROW, sy)
    face_x = (0, sx - 1)
    edge_y = (0, sy - 1)
    x_of = (left, right)
    y_of = (gy - 1, gy + 1)
    has_y = (has_down, has_up)

    load_p = pltpu.make_async_copy(pops, st0.at[:, :, own_y, :], load_sem.at[0])
    load_h = pltpu.make_async_copy(heat_level, hl, load_sem.at[1])
    load_o = pltpu.make_async_copy(obstacle, ob, load_sem.at[2])
    load_p.start()
    load_h.start()
    load_o.start()
    load_t = pltpu.make_async_copy(table, tb, load_sem.at[3])
    load_t.start()

    barrier = pltpu.get_barrier_semaphore()

    def greet(x, y):
        pl.semaphore_signal(barrier, inc=1, device_id={"gx": x, "gy": y}, device_id_type=pl.DeviceIdType.MESH)

    groups = peak_groups(ngx, ngy)
    partners = sum(len(group) for group in groups)
    for group in groups:
        for dx, dy in group:
            greet(lax.rem(gx + dx, ngx), lax.rem(gy + dy, ngy))
    if len(groups) > 1:
        partners = partners + 2 * (jnp.where(has_up, 1, 0) + jnp.where(has_down, 1, 0))
        for s in (0, 1):

            @pl.when(has_y[s])
            def _():
                greet(right, y_of[s])
                greet(left, y_of[s])

    def zeros(ref, *index):
        part = ref.at[index]
        part[...] = jnp.zeros(part.shape, jnp.float32)

    every = slice(None)
    for row in (ROW - 1, ROW + sy):
        for st in (st0, st1):
            for c in (1, -1):
                for k in ACROSS_Y[c]:
                    zeros(st, k, every, pl.ds(row, 1), every)
        zeros(xr, every, every, every, pl.ds(row, 1), every)
    for ref in (cg, tu, ey):
        ref[...] = jnp.zeros(ref.shape, jnp.float32)

    for s in (0, 1):

        @pl.when(jnp.logical_not(has_y[s]))
        def _():
            zeros(yb_in, every, every, pl.ds(s * sx, sx), every)
            for xs in (0, 1):
                zeros(cr_in, every, pl.ds(xs * 2 + s, 1), every)
                zeros(cm_in, every, every, pl.ds(xs * 2 + s, 1), every)
            zeros(hb, every, pl.ds((ROW - 2, ROW + sy)[s], 2), every)

    gone = []

    def guarded(cond, fn):
        if cond is None:
            fn()
        else:
            pl.when(cond)(fn)

    def send(cond, pairs, send_sem, recv_sem, x, y):
        def go():
            for src, dst in pairs:
                pltpu.make_async_remote_copy(
                    src_ref=src, dst_ref=dst, send_sem=send_sem, recv_sem=recv_sem,
                    device_id={"gx": x, "gy": y}, device_id_type=pl.DeviceIdType.MESH,
                ).start()

        guarded(cond, go)

    def await_bytes(cond, view, sem):
        guarded(cond, lambda: pltpu.make_async_copy(view, view, sem).wait())

    def send_later(cond, view, sem):
        gone.append(lambda: await_bytes(cond, view, sem))

    states = (st0, st1)

    def x_raw(step, s):
        st = states[step]
        return [(st.at[k, face_x[s], own_y, :], xr.at[step, 1 - s, j, own_y, :]) for j, k in enumerate(ACROSS_X[OUT[s]])]

    def send_x_raw(step):
        def go(s):
            send(None, x_raw(step, s), xr_send.at[step, s], xr_recv.at[step, 1 - s], x_of[s], gy)

        @pl.when(gx == 0)
        def _():
            go(0)
            go(1)

        @pl.when(gx != 0)
        def _():
            go(1)
            go(0)

        for s in (0, 1):
            send_later(None, states[step].at[pl.ds(0, 5), 0, own_y, :], xr_send.at[step, s])

    def send_x_sums(step):
        def go(s):
            send(None, [(xm_out.at[step, s], xm_in.at[step, 1 - s])], xm_send.at[step, s], xm_recv.at[step, 1 - s], x_of[s], gy)

        @pl.when(gx == 0)
        def _():
            go(0)
            go(1)

        @pl.when(gx != 0)
        def _():
            go(1)
            go(0)

        for s in (0, 1):
            send_later(None, xm_out.at[step, s], xm_send.at[step, s])

    def send_y(step, fields, send_sem, recv_sem):
        for s in (0, 1):
            src = yb_out.at[step, fields, pl.ds(s * sx, sx), :]
            dst = yb_in.at[step, fields, pl.ds((1 - s) * sx, sx), :]
            send(has_y[s], [(src, dst)], send_sem.at[step, s], recv_sem.at[step, 1 - s], gx, y_of[s])
            send_later(has_y[s], src, send_sem.at[step, s])

    corners = [(xs, ys) for xs in (0, 1) for ys in (0, 1)]

    def send_corner_raw(step):
        st = states[step]
        for c, (xs, ys) in enumerate(corners):
            k = NUMBER[(OUT[xs], OUT[ys], 0)]
            src = st.at[k, face_x[xs], pl.ds(ROW + edge_y[ys], 1), :]
            send(has_y[ys], [(src, cr_in.at[step, pl.ds(3 - c, 1), :])], cr_send.at[step, c], cr_recv.at[step, 3 - c], x_of[xs], y_of[ys])
            send_later(has_y[ys], src, cr_send.at[step, c])

    def send_corner_sums(step):
        for c, (xs, ys) in enumerate(corners):
            src = cm_out.at[step, :, pl.ds(c, 1), :]
            send(has_y[ys], [(src, cm_in.at[step, :, pl.ds(3 - c, 1), :])], cm_send.at[step, c], cm_recv.at[step, 3 - c], x_of[xs], y_of[ys])
            send_later(has_y[ys], src, cm_send.at[step, c])

    def await_raw(step):
        for s in (0, 1):
            await_bytes(has_y[s], yb_in.at[step, pl.ds(0, 5), pl.ds(s * sx, sx), :], yr_recv.at[step, s])
        for c, (xs, ys) in enumerate(corners):
            await_bytes(has_y[ys], cr_in.at[step, pl.ds(c, 1), :], cr_recv.at[step, c])
        for s in (0, 1):
            await_bytes(None, xr.at[step, s, :, own_y, :], xr_recv.at[step, s])

    def await_sums(step):
        for s in (0, 1):
            await_bytes(has_y[s], yb_in.at[step, pl.ds(5, 4), pl.ds(s * sx, sx), :], ym_recv.at[step, s])
        for c, (xs, ys) in enumerate(corners):
            await_bytes(has_y[ys], cm_in.at[step, :, pl.ds(c, 1), :], cm_recv.at[step, c])
        for s in (0, 1):
            await_bytes(None, xm_in.at[step, s], xm_recv.at[step, s])

    raw_fields = pl.ds(0, 5)
    sum_fields = pl.ds(5, 4)

    def heat_moves():
        moves = []
        layers = ((2, sx), (0, sx + 2))
        for s in (0, 1):
            src = hb.at[pl.ds(layers[0][s], 2), own_y, :]
            dst = hb.at[pl.ds((sx + 2, 0)[s], 2), own_y, :]
            moves.append((None, src, dst, x_of[s], gy))
        for s in (0, 1):
            src = hb.at[pl.ds(2, sx), pl.ds((ROW, ROW + sy - 2)[s], 2), :]
            dst = hb.at[pl.ds(2, sx), pl.ds((ROW + sy, ROW - 2)[s], 2), :]
            moves.append((has_y[s], src, dst, gx, y_of[s]))
        for xs, ys in corners:
            src = hb.at[2 + face_x[xs], pl.ds(ROW + edge_y[ys], 1), :]
            dst = hb.at[(sx + 2, 1)[xs], pl.ds((ROW + sy, ROW - 1)[ys], 1), :]
            moves.append((has_y[ys], src, dst, x_of[xs], y_of[ys]))
        return moves

    arrives_on = (1, 0, 3, 2, 7, 6, 5, 4)

    def send_heat():
        for number, (cond, src, dst, x, y) in enumerate(heat_moves()):
            send(cond, [(src, dst)], h_send.at[number], h_recv.at[number], x, y)
            send_later(cond, src, h_send.at[number])

    def await_heat():
        moves = heat_moves()
        for number, (_, src, dst, _, _) in enumerate(moves):
            await_bytes(moves[arrives_on[number]][0], dst, h_recv.at[number])

    def spread(step, phase, value):
        group = peak_groups(ngx, ngy)[phase]
        count = len(group)
        buf = pm_bufs[phase]
        pm_src[step, phase] = value
        for d, (dx, dy) in enumerate(group, 1):
            place = {"gx": lax.rem(gx + dx, ngx), "gy": lax.rem(gy + dy, ngy)}
            pltpu.make_async_remote_copy(
                src_ref=pm_src.at[step, phase],
                dst_ref=buf.at[step, pl.ds(d - 1, 1), :],
                send_sem=p_send.at[step, phase],
                recv_sem=p_recv.at[step, phase],
                device_id=place,
                device_id_type=pl.DeviceIdType.MESH,
            ).start()
        view = buf.at[step, pl.ds(0, count), :]
        send_later(None, view, p_send.at[step, phase])

        def wait():
            await_bytes(None, view, p_recv.at[step, phase])
            return jnp.maximum(value, jnp.max(buf[step, pl.ds(0, count), :], axis=0, keepdims=True))

        return wait

    def spread_all(step, tile):
        wait = spread(step, 0, jnp.max(tile, axis=0, keepdims=True))

        def finish():
            best = wait()
            for phase in range(1, len(pm_bufs)):
                best = spread(step, phase, best)()
            peak = jnp.broadcast_to(jnp.max(best, axis=1, keepdims=True), (ROW, nz))
            return speed_cap / jnp.sqrt(speed_cap * speed_cap + peak)

        return finish

    blocks = [(x, r) for x in range(sx) for r in range(0, sy, ROW)]
    outer = [(x, r) for x, r in blocks if x in face_x]
    inner = [(x, r) for x, r in blocks if x not in face_x]
    lane = lax.broadcasted_iota(jnp.int32, (ROW, nz), 1)
    row_no = lax.broadcasted_iota(jnp.int32, (ROW, nz), 0)
    first_lane = lane == 0
    last_lane = lane == nz - 1
    edge_row = (row_no == 0, row_no == ROW - 1)
    pack_row = lax.broadcasted_iota(jnp.int32, (2 * sx, nz), 0)
    pack_sign = jnp.where(pack_row < sx, 1.0, -1.0)
    corner_x = jnp.where(row_no < 2, 1.0, -1.0)
    corner_y = jnp.where(lax.rem(row_no, 2) == 0, 1.0, -1.0)

    def shift_z(cells, cz):
        if not cz:
            return cells
        at = lax.broadcasted_iota(jnp.int32, cells.shape, 1)
        return jnp.where(at == (0 if cz > 0 else nz - 1), 0.0, pltpu.roll(cells, cz % nz, 1))

    def edges_of(r):
        return [s for s in (0, 1) if r == (0, sy - ROW)[s]]

    def own_sums(step, tiles):
        st = states[step]
        for x, r in tiles:
            rows = pl.ds(r, ROW)
            reads = {}
            for k, (cx, cy, cz) in enumerate(CS):
                if 0 <= x - cx < sx:
                    reads[k] = shift_z(st[k, x - cx, pl.ds(ROW + r - cy, ROW), :], cz)
                    rd[k, x, rows, :] = reads[k]
            sums = [tree_sum(list(reads.values()))]
            for c in range(3):
                plus = [reads[k] for k in reads if CS[k][c] > 0]
                minus = [reads[k] for k in reads if CS[k][c] < 0]
                if plus and minus:
                    sums.append(tree_sum(plus) - tree_sum(minus))
                else:
                    sums.append(tree_sum(plus) if plus else -tree_sum(minus))
            for m in range(4):
                ms[m, x, rows, :] = sums[m]
            sums[0] = jnp.where(solid_s[x, rows, :] != 0, 0.0, sums[0])
            for s in (0, 1):
                if x == face_x[s]:
                    for m in range(4):
                        xm_out[step, s, m, rows, :] = sums[m]
                if s in edges_of(r):
                    at = (0, ROW - 1)[s]
                    for m in range(4):
                        yb_out[step, 5 + m, pl.ds(s * sx + x, 1), :] = sums[m][at : at + 1, :]

    def pack_y_raw(step):
        st = states[step]
        for s in (0, 1):
            for j, k in enumerate(ACROSS_Y[OUT[s]]):
                for x in range(sx):
                    yb_out[step, j, pl.ds(s * sx + x, 1), :] = st[k, x, pl.ds(ROW + edge_y[s], 1), :]

    def corner_sums(step):
        st = states[step]
        for c, (xs, ys) in enumerate(corners):
            dx, dy = OUT[xs], OUT[ys]
            fx, fy = face_x[xs], edge_y[ys]
            places = [
                ((0, dy, 0), fx, fy), ((0, dy, 1), fx, fy), ((0, dy, -1), fx, fy), ((dx, dy, 0), fx - dx, fy),
                ((dx, 0, 0), fx, fy), ((dx, 0, 1), fx, fy), ((dx, 0, -1), fx, fy), ((dx, dy, 0), fx, fy - dy),
            ]
            for f, (direction, x, y) in enumerate(places):
                cg[f, pl.ds(c, 1), :] = st[NUMBER[direction], x, pl.ds(ROW + y, 1), :]
        for half, sign in ((0, -corner_x), (1, -corner_y)):
            a, b, d, e = (cg[4 * half + f] for f in range(4))
            b, d = shift_z(b, 1), shift_z(d, -1)
            cm_out[step, 3 * half + 0] = (a + b) + (d + e)
            cm_out[step, 3 * half + 1] = sign * e
            cm_out[step, 3 * half + 2] = b - d

    def packed(fields, fill):
        plus = jnp.where(lax.rem(pack_row, sx) == 0, 0.0, pltpu.roll(fields[1], 1, 0))
        minus = jnp.where(lax.rem(pack_row, sx) == sx - 1, 0.0, pltpu.roll(fields[2], 2 * sx - 1, 0))
        if fill is not None:
            for ys in (0, 1):
                plus = jnp.where(pack_row == ys * sx, fill(ys), plus)
                minus = jnp.where(pack_row == ys * sx + sx - 1, fill(2 + ys), minus)
        return [fields[0], plus, minus, shift_z(fields[3], 1), shift_z(fields[4], -1)]

    def ghost_shares(step):
        st = states[step]
        for s in (0, 1):
            for r in range(0, sy, ROW):
                ks = ACROSS_X[OUT[s]]
                a, b, c, d, e = (st[k, face_x[s], pl.ds(ROW + r - CS[k][1], ROW), :] for k in ks)
                d, e = shift_z(d, 1), shift_z(e, -1)
                ox[s, 0, pl.ds(r, ROW), :] = ((a + b) + (c + d)) + e
                ox[s, 1, pl.ds(r, ROW), :] = b - c
                ox[s, 2, pl.ds(r, ROW), :] = d - e
        a, b, c, d, e = packed([yb_out[step, j] for j in range(5)], None)
        total = ((a + b) + (c + d)) + e
        oy[0] = total
        oy[1] = b - c
        oy[2] = -pack_sign * total
        oy[3] = d - e

    def velocity_pass(step, fs):
        fields = packed([yb_in[step, j] for j in range(5)], lambda c: cr_in[step, pl.ds(c, 1), :])
        for j in range(5):
            dr[j] = fields[j]
        a, b, c, d, e = fields
        total = ((a + b) + (c + d)) + e
        for m, value in enumerate((total, b - c, pack_sign * total, d - e)):
            dm[m] = value
        peak = jnp.zeros((ROW, nz), jnp.float32)
        for x, r in blocks:
            rows = pl.ds(r, ROW)
            sums = [ms[m, x, rows, :] for m in range(4)]
            for s in (0, 1):
                if x == face_x[s]:
                    ks = ACROSS_X[IN[s]]
                    parts = [
                        shift_z(xr[step, s, j, pl.ds(ROW + r - CS[k][1], ROW), :], CS[k][2]) for j, k in enumerate(ks)
                    ]
                    for k, part in zip(ks, parts):
                        rd[k, x, rows, :] = part
                    share = tree_sum(parts)
                    sums[0] = sums[0] + share
                    sums[1] = sums[1] + share if s == 0 else sums[1] - share
                    sums[2] = sums[2] + (parts[1] - parts[2])
                    sums[3] = sums[3] + (parts[3] - parts[4])
            for s in edges_of(r):
                for m in range(4):
                    sums[m] = sums[m] + jnp.where(edge_row[s], dm[m, pl.ds(s * sx + x, 1), :], 0.0)
            if fs is not None:
                sums = [sums[m] + fs * hm[m, x + 1, rows, :] for m in range(4)]
            solid = solid_s[x, rows, :] != 0
            inv = jnp.where(solid, 0.0, 1.0 / jnp.where(solid, 1.0, sums[0]))
            rho_s[x, rows, :] = sums[0]
            speed = []
            for c in range(3):
                u = sums[1 + c] * inv
                vel[c, x + 1, pl.ds(ROW + r, ROW), :] = u
                speed.append(u * u)
            peak = jnp.maximum(peak, speed[0] + speed[1] + speed[2])
        return peak

    def edge_reads():
        for s in (0, 1):
            for j, k in enumerate(ACROSS_Y[IN[s]]):
                for x in range(sx):
                    rd[k, x, pl.ds(edge_y[s], 1), :] = dr[j, pl.ds(s * sx + x, 1), :]

    def ghost_pass(step, fs):
        for c, (xs, ys) in enumerate(corners):
            j = 1 if OUT[xs] > 0 else 2
            tu[0, pl.ds(c, 1), :] = yb_in[step, j, pl.ds(ys * sx + face_x[xs], 1), :]
            j = 1 if OUT[ys] > 0 else 2
            tu[1, pl.ds(c, 1), :] = xr[step, xs, j, pl.ds(ROW + edge_y[ys], 1), :]
        over, up = tu[0], tu[1]
        total = cm_in[step, 0] + over
        for m, value in enumerate((total, cm_in[step, 1] - corner_x * over, corner_y * total, cm_in[step, 2])):
            ex[m] = value
        total = cm_in[step, 3] + up
        for m, value in enumerate((total, corner_x * total, cm_in[step, 4] - corner_y * up, cm_in[step, 5])):
            for c, (xs, ys) in enumerate(corners):
                ey[m, pl.ds(ys * sx + face_x[xs], 1), :] = value[c : c + 1, :]
        for s in (0, 1):
            for r in range(0, sy, ROW):
                rows = pl.ds(r, ROW)
                share = ox[s, 0, rows, :]
                sums = [xm_in[step, s, m, rows, :] for m in range(4)]
                if step == 0:
                    gfx[s, rows, :] = sums[0]
                fluid = gfx[s, rows, :] > 0.0
                sums[0] = sums[0] + share
                sums[1] = sums[1] - share if s == 0 else sums[1] + share
                sums[2] = sums[2] + ox[s, 1, rows, :]
                sums[3] = sums[3] + ox[s, 2, rows, :]
                for ys in edges_of(r):
                    for m in range(4):
                        sums[m] = sums[m] + jnp.where(edge_row[ys], ex[m, pl.ds(s * 2 + ys, 1), :], 0.0)
                at = (0, sx + 1)[s]
                if fs is not None:
                    sums = [sums[m] + fs * hm[m, at, rows, :] for m in range(4)]
                inv = jnp.where(fluid, 1.0 / jnp.where(fluid, sums[0], 1.0), 0.0)
                for c in range(3):
                    vel[c, at, pl.ds(ROW + r, ROW), :] = sums[1 + c] * inv
        sums = [yb_in[step, 5 + m] for m in range(4)]
        if step == 0:
            gfy[...] = sums[0]
        fluid = gfy[...] > 0.0
        sums = [sums[m] + oy[m] + ey[m] for m in range(4)]
        if fs is not None:
            sums = [sums[m] + fs[0:1, :] * hmy[m] for m in range(4)]
        inv = jnp.where(fluid, 1.0 / jnp.where(fluid, sums[0], 1.0), 0.0)
        for c in range(3):
            u = sums[1 + c] * inv
            for s in (0, 1):
                for x in range(sx):
                    at = s * sx + x
                    vel[c, x + 1, pl.ds((ROW - 1, ROW + sy)[s], 1), :] = u[at : at + 1, :]

    def heat_sums():
        for x in range(sx + 4):
            spans = [(ROW + r, ROW) for r in range(0, sy, ROW)]
            if 1 <= x <= sx + 2:
                spans += [(ROW - 2, 2), (ROW + sy, 2)]
            for at, span in spans:
                if span != ROW and x in (1, sx + 2):
                    at, span = (at + 1, 1) if at < ROW else (at, 1)
                cells = hb[x, pl.ds(at, span), :]
                hzp[x, pl.ds(at, span), :] = shift_z(cells, 1)
                hzm[x, pl.ds(at, span), :] = shift_z(cells, -1)

        def at(x, row, span):
            cells = [
                (hzp[i, pl.ds(y, span), :], hzm[i, pl.ds(y, span), :])
                for i, y in ((x, row), (x - 1, row), (x + 1, row), (x, row - 1), (x, row + 1))
            ]
            diff = [a - b for a, b in cells]
            both = [a + b for a, b in cells]
            main, side = 3.0 * WEIGHT[5], 3.0 * WEIGHT[11]
            return (
                main * diff[0] + side * ((diff[1] + diff[2]) + (diff[3] + diff[4])),
                side * (diff[1] - diff[2]),
                side * (diff[3] - diff[4]),
                main * both[0] + side * ((both[1] + both[2]) + (both[3] + both[4])),
            )

        for x in range(sx + 2):
            for r in range(0, sy, ROW):
                for m, value in enumerate(at(x + 1, ROW + r, ROW)):
                    hm[m, x, pl.ds(r, ROW), :] = value
        for s in (0, 1):
            for x in range(sx):
                for m, value in enumerate(at(x + 2, (ROW - 1, ROW + sy)[s], 1)):
                    hmy[m, pl.ds(s * sx + x, 1), :] = value

    def collided(tiles, fs, store):
        for x, r in tiles:
            mid = pl.ds(ROW + r, ROW)
            u = [vel[c, x + 1, mid, :] for c in range(3)]
            diff = []
            for a in range(3):
                diff.append(
                    (
                        vel[a, x + 2, mid, :] - vel[a, x, mid, :],
                        vel[a, x + 1, pl.ds(ROW + r + 1, ROW), :] - vel[a, x + 1, pl.ds(ROW + r - 1, ROW), :],
                        pltpu.roll(u[a], nz - 1, 1) - pltpu.roll(u[a], 1, 1),
                    )
                )
            own = diff[0][0] * diff[0][0] + diff[1][1] * diff[1][1] + diff[2][2] * diff[2][2]
            xy = diff[0][1] + diff[1][0]
            xz = diff[0][2] + diff[2][0]
            yz = diff[1][2] + diff[2][1]
            size = jnp.sqrt(0.5 * own + 0.25 * (xy * xy + xz * xz + yz * yz) + strain_floor)
            omega = 1.0 / (base_tau + 3.0 * smag_coef * size)
            solid = solid_s[x, pl.ds(r, ROW), :] != 0
            density = rho_s[x, pl.ds(r, ROW), :]
            still = 1.0 - 1.5 * (u[0] * u[0] + u[1] * u[1] + u[2] * u[2])
            reads = [rd[k, x, pl.ds(r, ROW), :] for k in range(19)]
            if fs is not None:
                for k in LIFTED:
                    cx, cy, cz = CS[k]
                    source = hzp if cz > 0 else hzm
                    reads[k] = reads[k] + (3.0 * WEIGHT[k] * cz) * (fs * source[x + 2 - cx, pl.ds(ROW + r - cy, ROW), :])
            scaled = {w: (w * density) * omega for w in sorted(set(WEIGHT))}
            keep = 1.0 - omega
            store(0, x, r, jnp.where(solid, reads[0], keep * reads[0] + scaled[WEIGHT[0]] * still))
            for k in range(1, 19, 2):
                other = OPP[k]
                project = None
                for c in range(3):
                    if CS[k][c]:
                        if project is None:
                            project = u[c] if CS[k][c] > 0 else -u[c]
                        else:
                            project = project + u[c] if CS[k][c] > 0 else project - u[c]
                even = still + 4.5 * project * project
                odd = 3.0 * project
                weight = scaled[WEIGHT[k]]
                store(k, x, r, jnp.where(solid, reads[other], keep * reads[k] + weight * (even + odd)))
                store(other, x, r, jnp.where(solid, reads[k], keep * reads[other] + weight * (even - odd)))

    load_h.wait()
    load_o.wait()
    load_t.wait()
    for x, r in blocks:
        rows = pl.ds(r, ROW)
        code = hl[x, rows, :]
        heat = jnp.zeros((ROW, nz), jnp.float32)
        for level in range(levels):
            heat = jnp.where(code == level, tb[level], heat)
        grid_y = gy * sy + r + row_no
        solid = (
            (ob[x, rows, :] == 1) | (grid_y == 0) | (grid_y == ngy * sy - 1) | first_lane | last_lane
        )
        solid_s[x, rows, :] = jnp.where(solid, 1, 0)
        hb[x + 2, pl.ds(ROW + r, ROW), :] = jnp.where(solid, 0.0, heat)

    load_p.wait()
    own_sums(0, blocks)
    pack_y_raw(0)
    corner_sums(0)
    pl.semaphore_wait(barrier, partners)
    send_corner_raw(0)
    send_corner_sums(0)
    send_x_raw(0)
    send_x_sums(0)
    send_y(0, raw_fields, yr_send, yr_recv)
    send_y(0, sum_fields, ym_send, ym_recv)
    ghost_shares(0)
    await_raw(0)
    finish_peak = spread_all(0, velocity_pass(0, None))
    edge_reads()
    await_sums(0)
    ghost_pass(0, None)

    def store_st1(k, x, r, value):
        st1[k, x, pl.ds(ROW + r, ROW), :] = value

    collided(outer, None, store_st1)
    send_x_raw(1)
    collided(inner, None, store_st1)
    send_corner_raw(1)
    pack_y_raw(1)
    send_y(1, raw_fields, yr_send, yr_recv)
    own_sums(1, outer)
    send_x_sums(1)
    own_sums(1, inner)
    send_y(1, sum_fields, ym_send, ym_recv)
    corner_sums(1)
    send_corner_sums(1)
    send_heat()
    ghost_shares(1)
    await_heat()
    heat_sums()
    fs = finish_peak()
    await_raw(1)
    finish_peak = spread_all(1, velocity_pass(1, fs))
    for x, r in blocks:
        for c in range(3):
            out_v[c, x, pl.ds(r, ROW), :] = vel[c, x + 1, pl.ds(ROW + r, ROW), :]
    edge_reads()
    await_sums(1)
    ghost_pass(1, fs)

    def store_out(k, x, r, value):
        out_p[k, x, pl.ds(r, ROW), :] = value

    collided(blocks, fs, store_out)
    fs = finish_peak()
    lift = {(x, r): fs * hb[x + 2, pl.ds(ROW + r, ROW), :] for x, r in blocks}
    for k in LIFTED:
        for x, r in blocks:
            rows = pl.ds(r, ROW)
            out_p[k, x, rows, :] = out_p[k, x, rows, :] + (3.0 * WEIGHT[k] * CS[k][2]) * lift[(x, r)]
    for sent in gone:
        sent()


def write_out(pops, vel, out_p, out_v, sems):
    copies = [
        pltpu.make_async_copy(pops, out_p, sems.at[0]),
        pltpu.make_async_copy(vel, out_v, sems.at[1]),
    ]
    for copy in copies:
        copy.start()
    for copy in copies:
        copy.wait()


def local(populations, heat_level, obstacle, heat_table):
    ngx = lax.axis_size("gx")
    ngy = lax.axis_size("gy")
    _, sx, sy, nz = populations.shape
    f32 = jnp.float32
    tall = sy + 2 * ROW
    dma = pltpu.SemaphoreType.DMA
    groups = peak_groups(ngx, ngy)
    phases = len(groups)
    vmem = pl.BlockSpec(memory_space=pltpu.VMEM)
    anywhere = pl.BlockSpec(memory_space=pltpu.HBM)
    shapes = (
        jax.ShapeDtypeStruct(populations.shape, f32),
        jax.ShapeDtypeStruct((3, sx, sy, nz), f32),
    )

    def floats(*shape):
        return pltpu.VMEM(shape, f32)

    def ints(*shape):
        return pltpu.VMEM(shape, jnp.int32)

    pops, velocity = pl.pallas_call(
        functools.partial(kernel, ngx, ngy),
        out_shape=shapes,
        in_specs=[anywhere] * 4,
        out_specs=[vmem] * 2,
        scratch_shapes=[
            floats(19, sx, tall, nz),
            floats(19, sx, tall, nz),
            floats(19, sx, sy, nz),
            floats(4, sx, sy, nz),
            floats(sx, sy, nz),
            floats(3, sx + 2, tall, nz),
            ints(sx, sy, nz),
            ints(sx, sy, nz),
            pltpu.SMEM(heat_table.shape, f32),
            ints(sx, sy, nz),
            floats(sx + 4, tall, nz),
            floats(sx + 4, tall, nz),
            floats(sx + 4, tall, nz),
            floats(4, sx + 2, sy, nz),
            floats(4, 2 * sx, nz),
            floats(STEPS, 2, 5, tall, nz),
            floats(STEPS, 2, 4, sy, nz),
            floats(STEPS, 2, 4, sy, nz),
            floats(STEPS, 9, 2 * sx, nz),
            floats(STEPS, 9, 2 * sx, nz),
            floats(8, ROW, nz),
            floats(STEPS, 6, ROW, nz),
            floats(STEPS, ROW, nz),
            floats(STEPS, 6, ROW, nz),
            floats(2, 3, sy, nz),
            floats(4, 2 * sx, nz),
            floats(5, 2 * sx, nz),
            floats(4, 2 * sx, nz),
            floats(2, ROW, nz),
            floats(4, ROW, nz),
            floats(4, 2 * sx, nz),
            floats(2, sy, nz),
            floats(2 * sx, nz),
            floats(STEPS, phases, 1, nz),
            *[floats(STEPS, -(-len(group) // ROW) * ROW, nz) for group in groups],
            dma((4,)),
            *[dma((STEPS, 2))] * 8,
            *[dma((STEPS, 4))] * 4,
            *[dma((8,))] * 2,
            *[dma((STEPS, phases))] * 2,
        ],
        compiler_params=pltpu.CompilerParams(
            collective_id=0, has_side_effects=True, vmem_limit_bytes=24 * 1024 * 1024
        ),
        name="lattice_steps",
    )(*[pltpu.with_memory_space_constraint(a, pltpu.HBM) for a in (populations, heat_level, obstacle, heat_table)])
    return pl.pallas_call(
        write_out,
        out_shape=shapes,
        in_specs=[vmem] * 2,
        out_specs=[anywhere] * 2,
        scratch_shapes=[dma((2,))],
        compiler_params=pltpu.CompilerParams(vmem_limit_bytes=8 * 1024 * 1024),
        name="write_out",
    )(pops, velocity)


def solution(mesh):
    return jax.shard_map(
        local,
        mesh=mesh,
        in_specs=(
            P(None, ("member", "gx"), "gy", None),
            P(("member", "gx"), "gy", None),
            P(("member", "gx"), "gy", None),
            P(),
        ),
        out_specs=(P(None, ("member", "gx"), "gy", None), P(None, ("member", "gx"), "gy", None)),
        check_vma=False,
    )
```

```python
import functools

import jax
import jax.numpy as jnp
import numpy as np
from jax import lax
from jax.experimental import pallas as pl
from jax.experimental.pallas import tpu as pltpu
from jax.sharding import PartitionSpec as P

STEPS = 2
ROW = 8

lattice = np.array(
    [
        [0, 0, 0],
        [1, 0, 0],
        [-1, 0, 0],
        [0, 1, 0],
        [0, -1, 0],
        [0, 0, 1],
        [0, 0, -1],
        [1, 1, 0],
        [-1, -1, 0],
        [1, -1, 0],
        [-1, 1, 0],
        [1, 0, 1],
        [-1, 0, -1],
        [1, 0, -1],
        [-1, 0, 1],
        [0, 1, 1],
        [0, -1, -1],
        [0, 1, -1],
        [0, -1, 1],
    ]
)
CS = [tuple(int(c) for c in row) for row in lattice]
NUMBER = {c: k for k, c in enumerate(CS)}
WEIGHT = [1.0 / 3.0] + [1.0 / 18.0] * 6 + [1.0 / 36.0] * 12
OPP = [0, 2, 1, 4, 3, 6, 5, 8, 7, 10, 9, 12, 11, 14, 13, 16, 15, 18, 17]
base_tau = 0.52
smag_coef = 0.04
speed_cap = 0.1
strain_floor = 1e-06
LIFTED = [k for k in range(19) if CS[k][2] != 0]
ACROSS_X = {c: [NUMBER[(c, 0, 0)], NUMBER[(c, 1, 0)], NUMBER[(c, -1, 0)], NUMBER[(c, 0, 1)], NUMBER[(c, 0, -1)]] for c in (1, -1)}
ACROSS_Y = {c: [NUMBER[(0, c, 0)], NUMBER[(1, c, 0)], NUMBER[(-1, c, 0)], NUMBER[(0, c, 1)], NUMBER[(0, c, -1)]] for c in (1, -1)}
OUT = (-1, 1)
IN = (1, -1)


def tree_sum(items):
    items = list(items)
    while len(items) > 1:
        items = [items[i] + items[i + 1] if i + 1 < len(items) else items[i] for i in range(0, len(items), 2)]
    return items[0]


def peak_groups(ngx, ngy):
    if ngx * ngy <= 64:
        return [[(dx, dy) for dx in range(ngx) for dy in range(ngy) if dx or dy]]
    return [[(0, dy) for dy in range(1, ngy)], [(dx, 0) for dx in range(1, ngx)]]


def kernel(
    ngx, ngy,
    pops, heat_level, obstacle, table,
    out_p, out_v,
    st0, st1, rd, ms, rho_s, vel, hl, ob, tb, solid_s,
    hb, hzp, hzm, hm, hmy,
    xr, xm_out, xm_in, yb_out, yb_in, cg, cm_out, cr_in, cm_in,
    ox, xo_in, oy, dr, dm, tu, ex, ey, gfx, gfy, flat, pm_src, *rest,
):
    (*pm_bufs, load_sem, in_sem, x_send, y_send, xr_recv, xm_recv, xo_recv, yr_recv, ym_recv,
     hx_recv, hy_recv, h2_recv, p_send, p_recv) = rest
    _, sx, sy, nz = pops.shape
    levels = table.shape[0]
    gx = lax.axis_index("gx")
    gy = lax.axis_index("gy")
    has_up = gy < ngy - 1
    has_down = gy > 0
    right = lax.rem(gx + 1, ngx)
    left = lax.rem(gx + ngx - 1, ngx)
    own_y = pl.ds(ROW, sy)
    face_x = (0, sx - 1)
    edge_y = (0, sy - 1)
    x_of = (left, right)
    y_of = (gy - 1, gy + 1)
    has_y = (has_down, has_up)

    barrier = pltpu.get_barrier_semaphore()

    def greet(sem, x, y):
        pl.semaphore_signal(sem, inc=1, device_id={"gx": x, "gy": y}, device_id_type=pl.DeviceIdType.MESH)

    groups = peak_groups(ngx, ngy)
    beside = sorted({1, ngx - 1} - {0})
    column = [(0, dy) for dy in range(1, ngy)]
    by_word = len(groups) == 1 and ngx <= 5
    greeted = [(dx, 0) for dx in beside] + column if by_word else [place for group in groups for place in group]
    partners = len(greeted)
    for dx, dy in greeted:
        greet(barrier, lax.rem(gx + dx, ngx), lax.rem(gy + dy, ngy))
    if len(groups) > 1:
        partners = partners + 2 * (jnp.where(has_up, 1, 0) + jnp.where(has_down, 1, 0))
        for s in (0, 1):

            @pl.when(has_y[s])
            def _():
                greet(barrier, right, y_of[s])
                greet(barrier, left, y_of[s])

    load_p = pltpu.make_async_copy(pops, st0.at[:, :, own_y, :], load_sem.at[0])
    load_h = pltpu.make_async_copy(heat_level, hl, load_sem.at[1])
    load_o = pltpu.make_async_copy(obstacle, ob, load_sem.at[2])
    load_t = pltpu.make_async_copy(table, tb, load_sem.at[3])
    load_p.start()
    load_h.start()
    load_o.start()
    load_t.start()

    def zeros(ref, *index):
        part = ref.at[index]
        part[...] = jnp.zeros(part.shape, jnp.float32)

    every = slice(None)
    for row in (ROW - 1, ROW + sy):
        for st in (st0, st1):
            for c in (1, -1):
                for k in ACROSS_Y[c]:
                    zeros(st, k, every, pl.ds(row, 1), every)
        zeros(xr, every, every, every, pl.ds(row, 1), every)
    for ref in (cg, tu, ey):
        ref[...] = jnp.zeros(ref.shape, jnp.float32)

    for s in (0, 1):

        @pl.when(jnp.logical_not(has_y[s]))
        def _():
            zeros(yb_in, every, every, pl.ds(s * sx, sx), every)
            for xs in (0, 1):
                zeros(cr_in, every, pl.ds(xs * 2 + s, 1), every)
                zeros(cm_in, every, every, pl.ds(xs * 2 + s, 1), every)
            zeros(hb, every, pl.ds((ROW - 2, ROW + sy)[s], 2), every)

    def guarded(cond, fn):
        if cond is None:
            fn()
        else:
            pl.when(cond)(fn)

    def send(cond, pairs, send_sem, recv_sem, x, y):
        def go():
            for src, dst in pairs:
                pltpu.make_async_remote_copy(
                    src_ref=src, dst_ref=dst, send_sem=send_sem, recv_sem=recv_sem,
                    device_id={"gx": x, "gy": y}, device_id_type=pl.DeviceIdType.MESH,
                ).start()

        guarded(cond, go)

    def await_bytes(cond, view, sem):
        guarded(cond, lambda: pltpu.make_async_copy(view, view, sem).wait())

    states = (st0, st1)
    corners = [(xs, ys) for xs in (0, 1) for ys in (0, 1)]
    raw_fields = pl.ds(0, 5)
    sum_fields = pl.ds(5, 4)

    def along_x(pairs_of, recv_sem):
        def go(s):
            send(None, pairs_of(s), x_send, recv_sem, x_of[s], gy)

        @pl.when(gx == 0)
        def _():
            go(0)
            go(1)

        @pl.when(gx != 0)
        def _():
            go(1)
            go(0)

    def send_x_raw(step):
        st = states[step]
        along_x(
            lambda s: [(st.at[k, face_x[s], own_y, :], xr.at[step, 1 - s, j, own_y, :]) for j, k in enumerate(ACROSS_X[OUT[s]])],
            xr_recv.at[step],
        )

    def send_x_sums(step):
        along_x(lambda s: [(xm_out.at[step, s], xm_in.at[step, 1 - s])], xm_recv.at[step])

    def send_x_shares():
        along_x(lambda s: [(ox.at[s], xo_in.at[1 - s])], xo_recv)

    def send_heat_x(recv_sem, near):
        at = ((2, sx + 1), (sx + 2, 1)) if near else ((3, sx), (sx + 3, 0))
        along_x(lambda s: [(hb.at[at[0][s], own_y, :], hb.at[at[1][s], own_y, :])], recv_sem)

    def send_y(step, fields, recv_sem):
        for s in (0, 1):
            src = yb_out.at[step, fields, pl.ds(s * sx, sx), :]
            dst = yb_in.at[step, fields, pl.ds((1 - s) * sx, sx), :]
            send(has_y[s], [(src, dst)], y_send.at[s], recv_sem.at[step, 1 - s], gx, y_of[s])

    def send_heat_y():
        for s in (0, 1):
            src = hb.at[pl.ds(2, sx), pl.ds((ROW, ROW + sy - 2)[s], 2), :]
            dst = hb.at[pl.ds(2, sx), pl.ds((ROW + sy, ROW - 2)[s], 2), :]
            send(has_y[s], [(src, dst)], y_send.at[s], hy_recv.at[1 - s], gx, y_of[s])

    def to_corners(pair_of, sem_of):
        for c, (xs, ys) in enumerate(corners):
            send(has_y[ys], [pair_of(c, xs, ys)], y_send.at[ys], sem_of(1 - ys), x_of[xs], y_of[ys])

    def send_corner_raw(step):
        st = states[step]

        def pair(c, xs, ys):
            k = NUMBER[(OUT[xs], OUT[ys], 0)]
            return st.at[k, face_x[xs], pl.ds(ROW + edge_y[ys], 1), :], cr_in.at[step, pl.ds(3 - c, 1), :]

        to_corners(pair, lambda s: yr_recv.at[step, s])

    def send_corner_sums(step):
        to_corners(
            lambda c, xs, ys: (cm_out.at[step, :, pl.ds(c, 1), :], cm_in.at[step, :, pl.ds(3 - c, 1), :]),
            lambda s: ym_recv.at[step, s],
        )

    def send_heat_corner():
        to_corners(
            lambda c, xs, ys: (
                hb.at[2 + face_x[xs], pl.ds(ROW + edge_y[ys], 1), :],
                hb.at[(sx + 2, 1)[xs], pl.ds((ROW + sy, ROW - 1)[ys], 1), :],
            ),
            lambda s: h2_recv.at[s],
        )

    def await_y_raw(step):
        for s in (0, 1):
            await_bytes(has_y[s], flat.at[pl.ds(0, 5 * sx + 2), :], yr_recv.at[step, s])

    def await_x_raw(step):
        await_bytes(None, xr.at[step, :, :, own_y, :], xr_recv.at[step])

    def await_sums(step):
        for s in (0, 1):
            await_bytes(has_y[s], flat.at[pl.ds(0, 4 * sx + 12), :], ym_recv.at[step, s])
        await_bytes(None, xm_in.at[step], xm_recv.at[step])

    def await_near_heat():
        for s in (0, 1):
            await_bytes(has_y[s], hb.at[pl.ds(2, sx), pl.ds(ROW, 2), :], hy_recv.at[s])
        await_bytes(None, hb.at[pl.ds(0, 2), own_y, :], hx_recv.at[0])

    def await_far_heat():
        for s in (0, 1):
            await_bytes(has_y[s], flat.at[pl.ds(0, 2), :], h2_recv.at[s])
        await_bytes(None, hb.at[pl.ds(0, 2), own_y, :], hx_recv.at[1])

    def await_sends():
        for view in (xr.at[:, :, :, own_y, :], xm_out, ox, hb.at[pl.ds(0, 4), own_y, :]):
            await_bytes(None, view, x_send)
        for s in (0, 1):
            for view in (
                yb_out.at[:, :, pl.ds(0, sx), :],
                hb.at[pl.ds(2, sx), pl.ds(ROW, 2), :],
                flat.at[pl.ds(0, STEPS * 14 + 2), :],
            ):
                await_bytes(has_y[s], view, y_send.at[s])
        for phase, group in enumerate(groups):
            for step in range(STEPS):
                await_bytes(None, pm_bufs[phase].at[step, pl.ds(0, len(group)), :], p_send.at[phase])

    def spread(step, phase, value):
        group = peak_groups(ngx, ngy)[phase]
        count = len(group)
        buf = pm_bufs[phase]
        pm_src[step, phase] = value
        for d, (dx, dy) in enumerate(group, 1):
            place = {"gx": lax.rem(gx + dx, ngx), "gy": lax.rem(gy + dy, ngy)}
            pltpu.make_async_remote_copy(
                src_ref=pm_src.at[step, phase],
                dst_ref=buf.at[step, pl.ds(d - 1, 1), :],
                send_sem=p_send.at[phase],
                recv_sem=p_recv.at[step, phase],
                device_id=place,
                device_id_type=pl.DeviceIdType.MESH,
            ).start()
        view = buf.at[step, pl.ds(0, count), :]

        def wait():
            await_bytes(None, view, p_recv.at[step, phase])
            return jnp.maximum(value, jnp.max(buf[step, pl.ds(0, count), :], axis=0, keepdims=True))

        return wait

    def spread_all(step, tile):
        wait = spread(step, 0, jnp.max(tile, axis=0, keepdims=True))

        def finish():
            best = wait()
            for phase in range(1, len(pm_bufs)):
                best = spread(step, phase, best)()
            peak = jnp.broadcast_to(jnp.max(best, axis=1, keepdims=True), (ROW, nz))
            return speed_cap / jnp.sqrt(speed_cap * speed_cap + peak)

        return finish

    blocks = [(x, r) for x in range(sx) for r in range(0, sy, ROW)]
    outer = [(x, r) for x, r in blocks if x in face_x]
    inner = [(x, r) for x, r in blocks if x not in face_x]
    lane = lax.broadcasted_iota(jnp.int32, (ROW, nz), 1)
    row_no = lax.broadcasted_iota(jnp.int32, (ROW, nz), 0)
    first_lane = lane == 0
    last_lane = lane == nz - 1
    edge_row = (row_no == 0, row_no == ROW - 1)
    pack_row = lax.broadcasted_iota(jnp.int32, (2 * sx, nz), 0)
    pack_sign = jnp.where(pack_row < sx, 1.0, -1.0)
    corner_x = jnp.where(row_no < 2, 1.0, -1.0)
    corner_y = jnp.where(lax.rem(row_no, 2) == 0, 1.0, -1.0)

    def shift_z(cells, cz):
        if not cz:
            return cells
        at = lax.broadcasted_iota(jnp.int32, cells.shape, 1)
        return jnp.where(at == (0 if cz > 0 else nz - 1), 0.0, pltpu.roll(cells, cz % nz, 1))

    def edges_of(r):
        return [s for s in (0, 1) if r == (0, sy - ROW)[s]]

    def own_sums(step, tiles):
        st = states[step]
        for x, r in tiles:
            rows = pl.ds(r, ROW)
            reads = {}
            for k, (cx, cy, cz) in enumerate(CS):
                if 0 <= x - cx < sx:
                    reads[k] = shift_z(st[k, x - cx, pl.ds(ROW + r - cy, ROW), :], cz)
                    rd[k, x, rows, :] = reads[k]
            sums = [tree_sum(list(reads.values()))]
            for c in range(3):
                plus = [reads[k] for k in reads if CS[k][c] > 0]
                minus = [reads[k] for k in reads if CS[k][c] < 0]
                if plus and minus:
                    sums.append(tree_sum(plus) - tree_sum(minus))
                else:
                    sums.append(tree_sum(plus) if plus else -tree_sum(minus))
            for m in range(4):
                ms[m, x, rows, :] = sums[m]
            sums[0] = jnp.where(solid_s[x, rows, :] != 0, 0.0, sums[0])
            for s in (0, 1):
                if x == face_x[s]:
                    for m in range(4):
                        xm_out[step, s, m, rows, :] = sums[m]
                if s in edges_of(r):
                    at = (0, ROW - 1)[s]
                    for m in range(4):
                        yb_out[step, 5 + m, pl.ds(s * sx + x, 1), :] = sums[m][at : at + 1, :]

    def pack_y_raw(step):
        st = states[step]
        for s in (0, 1):
            for j, k in enumerate(ACROSS_Y[OUT[s]]):
                for x in range(sx):
                    yb_out[step, j, pl.ds(s * sx + x, 1), :] = st[k, x, pl.ds(ROW + edge_y[s], 1), :]

    def corner_sums(step):
        st = states[step]
        for c, (xs, ys) in enumerate(corners):
            dx, dy = OUT[xs], OUT[ys]
            fx, fy = face_x[xs], edge_y[ys]
            places = [
                ((0, dy, 0), fx, fy), ((0, dy, 1), fx, fy), ((0, dy, -1), fx, fy), ((dx, dy, 0), fx - dx, fy),
                ((dx, 0, 0), fx, fy), ((dx, 0, 1), fx, fy), ((dx, 0, -1), fx, fy), ((dx, dy, 0), fx, fy - dy),
            ]
            for f, (direction, x, y) in enumerate(places):
                cg[f, pl.ds(c, 1), :] = st[NUMBER[direction], x, pl.ds(ROW + y, 1), :]
        for half, sign in ((0, -corner_x), (1, -corner_y)):
            a, b, d, e = (cg[4 * half + f] for f in range(4))
            b, d = shift_z(b, 1), shift_z(d, -1)
            cm_out[step, 3 * half + 0] = (a + b) + (d + e)
            cm_out[step, 3 * half + 1] = sign * e
            cm_out[step, 3 * half + 2] = b - d

    def packed(fields, fill):
        plus = jnp.where(lax.rem(pack_row, sx) == 0, 0.0, pltpu.roll(fields[1], 1, 0))
        minus = jnp.where(lax.rem(pack_row, sx) == sx - 1, 0.0, pltpu.roll(fields[2], 2 * sx - 1, 0))
        if fill is not None:
            for ys in (0, 1):
                plus = jnp.where(pack_row == ys * sx, fill(ys), plus)
                minus = jnp.where(pack_row == ys * sx + sx - 1, fill(2 + ys), minus)
        return [fields[0], plus, minus, shift_z(fields[3], 1), shift_z(fields[4], -1)]

    def face_shares(step):
        st = states[step]
        for s in (0, 1):
            for r in range(0, sy, ROW):
                ks = ACROSS_X[OUT[s]]
                a, b, c, d, e = (st[k, face_x[s], pl.ds(ROW + r - CS[k][1], ROW), :] for k in ks)
                d, e = shift_z(d, 1), shift_z(e, -1)
                ox[s, 0, pl.ds(r, ROW), :] = ((a + b) + (c + d)) + e
                ox[s, 1, pl.ds(r, ROW), :] = b - c
                ox[s, 2, pl.ds(r, ROW), :] = d - e

    def edge_shares(step):
        a, b, c, d, e = packed([yb_out[step, j] for j in range(5)], None)
        total = ((a + b) + (c + d)) + e
        oy[0] = total
        oy[1] = b - c
        oy[2] = -pack_sign * total
        oy[3] = d - e

    def velocity_pass(step, fs):
        fields = packed([yb_in[step, j] for j in range(5)], lambda c: cr_in[step, pl.ds(c, 1), :])
        for j in range(5):
            dr[j] = fields[j]
        a, b, c, d, e = fields
        total = ((a + b) + (c + d)) + e
        for m, value in enumerate((total, b - c, pack_sign * total, d - e)):
            dm[m] = value
        peak = jnp.zeros((ROW, nz), jnp.float32)
        for x, r in blocks:
            rows = pl.ds(r, ROW)
            sums = [ms[m, x, rows, :] for m in range(4)]
            for s in (0, 1):
                if x == face_x[s]:
                    if step == 0:
                        parts = face_reads(step, s, r)
                        shares = tree_sum(parts), parts[1] - parts[2], parts[3] - parts[4]
                    else:
                        shares = [xo_in[s, m, rows, :] for m in range(3)]
                    sums[0] = sums[0] + shares[0]
                    sums[1] = sums[1] + shares[0] if s == 0 else sums[1] - shares[0]
                    sums[2] = sums[2] + shares[1]
                    sums[3] = sums[3] + shares[2]
            for s in edges_of(r):
                for m in range(4):
                    sums[m] = sums[m] + jnp.where(edge_row[s], dm[m, pl.ds(s * sx + x, 1), :], 0.0)
            if fs is not None:
                sums = [sums[m] + fs * hm[m, x + 1, rows, :] for m in range(4)]
            solid = solid_s[x, rows, :] != 0
            inv = jnp.where(solid, 0.0, 1.0 / jnp.where(solid, 1.0, sums[0]))
            rho_s[x, rows, :] = sums[0]
            speed = []
            for c in range(3):
                u = sums[1 + c] * inv
                vel[c, x + 1, pl.ds(ROW + r, ROW), :] = u
                speed.append(u * u)
            peak = jnp.maximum(peak, speed[0] + speed[1] + speed[2])
        return peak

    def face_reads(step, s, r):
        parts = []
        for j, k in enumerate(ACROSS_X[IN[s]]):
            part = shift_z(xr[step, s, j, pl.ds(ROW + r - CS[k][1], ROW), :], CS[k][2])
            rd[k, face_x[s], pl.ds(r, ROW), :] = part
            parts.append(part)
        return parts

    def edge_reads():
        for s in (0, 1):
            for j, k in enumerate(ACROSS_Y[IN[s]]):
                for x in range(sx):
                    rd[k, x, pl.ds(edge_y[s], 1), :] = dr[j, pl.ds(s * sx + x, 1), :]

    def ghost_pass(step, fs):
        for c, (xs, ys) in enumerate(corners):
            j = 1 if OUT[xs] > 0 else 2
            tu[0, pl.ds(c, 1), :] = yb_in[step, j, pl.ds(ys * sx + face_x[xs], 1), :]
            j = 1 if OUT[ys] > 0 else 2
            tu[1, pl.ds(c, 1), :] = xr[step, xs, j, pl.ds(ROW + edge_y[ys], 1), :]
        over, up = tu[0], tu[1]
        total = cm_in[step, 0] + over
        for m, value in enumerate((total, cm_in[step, 1] - corner_x * over, corner_y * total, cm_in[step, 2])):
            ex[m] = value
        total = cm_in[step, 3] + up
        for m, value in enumerate((total, corner_x * total, cm_in[step, 4] - corner_y * up, cm_in[step, 5])):
            for c, (xs, ys) in enumerate(corners):
                ey[m, pl.ds(ys * sx + face_x[xs], 1), :] = value[c : c + 1, :]
        for s in (0, 1):
            for r in range(0, sy, ROW):
                rows = pl.ds(r, ROW)
                share = ox[s, 0, rows, :]
                sums = [xm_in[step, s, m, rows, :] for m in range(4)]
                if step == 0:
                    gfx[s, rows, :] = sums[0]
                fluid = gfx[s, rows, :] > 0.0
                sums[0] = sums[0] + share
                sums[1] = sums[1] - share if s == 0 else sums[1] + share
                sums[2] = sums[2] + ox[s, 1, rows, :]
                sums[3] = sums[3] + ox[s, 2, rows, :]
                for ys in edges_of(r):
                    for m in range(4):
                        sums[m] = sums[m] + jnp.where(edge_row[ys], ex[m, pl.ds(s * 2 + ys, 1), :], 0.0)
                at = (0, sx + 1)[s]
                if fs is not None:
                    sums = [sums[m] + fs * hm[m, at, rows, :] for m in range(4)]
                inv = jnp.where(fluid, 1.0 / jnp.where(fluid, sums[0], 1.0), 0.0)
                for c in range(3):
                    vel[c, at, pl.ds(ROW + r, ROW), :] = sums[1 + c] * inv
        sums = [yb_in[step, 5 + m] for m in range(4)]
        if step == 0:
            gfy[...] = sums[0]
        fluid = gfy[...] > 0.0
        sums = [sums[m] + oy[m] + ey[m] for m in range(4)]
        if fs is not None:
            sums = [sums[m] + fs[0:1, :] * hmy[m] for m in range(4)]
        inv = jnp.where(fluid, 1.0 / jnp.where(fluid, sums[0], 1.0), 0.0)
        for c in range(3):
            u = sums[1 + c] * inv
            for s in (0, 1):
                for x in range(sx):
                    at = s * sx + x
                    vel[c, x + 1, pl.ds((ROW - 1, ROW + sy)[s], 1), :] = u[at : at + 1, :]

    def shift_heat(x, row, span):
        cells = hb[x, pl.ds(row, span), :]
        hzp[x, pl.ds(row, span), :] = shift_z(cells, 1)
        hzm[x, pl.ds(row, span), :] = shift_z(cells, -1)

    def heat_moments(x, row, span):
        cells = [
            (hzp[i, pl.ds(y, span), :], hzm[i, pl.ds(y, span), :])
            for i, y in ((x, row), (x - 1, row), (x + 1, row), (x, row - 1), (x, row + 1))
        ]
        diff = [a - b for a, b in cells]
        both = [a + b for a, b in cells]
        main, side = 3.0 * WEIGHT[5], 3.0 * WEIGHT[11]
        return (
            main * diff[0] + side * ((diff[1] + diff[2]) + (diff[3] + diff[4])),
            side * (diff[1] - diff[2]),
            side * (diff[3] - diff[4]),
            main * both[0] + side * ((both[1] + both[2]) + (both[3] + both[4])),
        )

    def heat_sums(columns):
        for x in columns:
            for r in range(0, sy, ROW):
                for m, value in enumerate(heat_moments(x + 1, ROW + r, ROW)):
                    hm[m, x, pl.ds(r, ROW), :] = value

    def near_heat():
        for x in range(1, sx + 3):
            for r in range(0, sy, ROW):
                shift_heat(x, ROW + r, ROW)
        for x in range(2, sx + 2):
            shift_heat(x, ROW - 2, 2)
            shift_heat(x, ROW + sy, 2)
        heat_sums(range(1, sx + 1))

    def far_heat():
        for x in (0, sx + 3):
            for r in range(0, sy, ROW):
                shift_heat(x, ROW + r, ROW)
        for x in (1, sx + 2):
            shift_heat(x, ROW - 1, 1)
            shift_heat(x, ROW + sy, 1)
        heat_sums((0, sx + 1))
        for s in (0, 1):
            for x in range(sx):
                for m, value in enumerate(heat_moments(x + 2, (ROW - 1, ROW + sy)[s], 1)):
                    hmy[m, pl.ds(s * sx + x, 1), :] = value

    def collided(tiles, fs, store):
        for x, r in tiles:
            mid = pl.ds(ROW + r, ROW)
            u = [vel[c, x + 1, mid, :] for c in range(3)]
            diff = []
            for a in range(3):
                diff.append(
                    (
                        vel[a, x + 2, mid, :] - vel[a, x, mid, :],
                        vel[a, x + 1, pl.ds(ROW + r + 1, ROW), :] - vel[a, x + 1, pl.ds(ROW + r - 1, ROW), :],
                        pltpu.roll(u[a], nz - 1, 1) - pltpu.roll(u[a], 1, 1),
                    )
                )
            own = diff[0][0] * diff[0][0] + diff[1][1] * diff[1][1] + diff[2][2] * diff[2][2]
            xy = diff[0][1] + diff[1][0]
            xz = diff[0][2] + diff[2][0]
            yz = diff[1][2] + diff[2][1]
            size = jnp.sqrt(0.5 * own + 0.25 * (xy * xy + xz * xz + yz * yz) + strain_floor)
            omega = 1.0 / (base_tau + 3.0 * smag_coef * size)
            solid = solid_s[x, pl.ds(r, ROW), :] != 0
            density = rho_s[x, pl.ds(r, ROW), :]
            still = 1.0 - 1.5 * (u[0] * u[0] + u[1] * u[1] + u[2] * u[2])
            reads = [rd[k, x, pl.ds(r, ROW), :] for k in range(19)]
            if fs is not None:
                for k in LIFTED:
                    cx, cy, cz = CS[k]
                    source = hzp if cz > 0 else hzm
                    reads[k] = reads[k] + (3.0 * WEIGHT[k] * cz) * (fs * source[x + 2 - cx, pl.ds(ROW + r - cy, ROW), :])
            scaled = {w: (w * density) * omega for w in sorted(set(WEIGHT))}
            keep = 1.0 - omega
            store(0, x, r, jnp.where(solid, reads[0], keep * reads[0] + scaled[WEIGHT[0]] * still))
            for k in range(1, 19, 2):
                other = OPP[k]
                project = None
                for c in range(3):
                    if CS[k][c]:
                        if project is None:
                            project = u[c] if CS[k][c] > 0 else -u[c]
                        else:
                            project = project + u[c] if CS[k][c] > 0 else project - u[c]
                even = still + 4.5 * project * project
                odd = 3.0 * project
                weight = scaled[WEIGHT[k]]
                store(k, x, r, jnp.where(solid, reads[other], keep * reads[k] + weight * (even + odd)))
                store(other, x, r, jnp.where(solid, reads[k], keep * reads[other] + weight * (even - odd)))

    load_h.wait()
    load_o.wait()
    load_t.wait()
    for x, r in blocks:
        rows = pl.ds(r, ROW)
        code = hl[x, rows, :]
        heat = jnp.zeros((ROW, nz), jnp.float32)
        for level in range(levels):
            heat = jnp.where(code == level, tb[level], heat)
        grid_y = gy * sy + r + row_no
        solid = (
            (ob[x, rows, :] == 1) | (grid_y == 0) | (grid_y == ngy * sy - 1) | first_lane | last_lane
        )
        solid_s[x, rows, :] = jnp.where(solid, 1, 0)
        hb[x + 2, pl.ds(ROW + r, ROW), :] = jnp.where(solid, 0.0, heat)

    load_p.wait()
    own_sums(0, blocks)
    pack_y_raw(0)
    if not by_word:
        corner_sums(0)
    pl.semaphore_wait(barrier, partners)
    if by_word:
        for dx, dy in column:
            greet(in_sem, gx, lax.rem(gy + dy, ngy))
    send_x_raw(0)
    send_x_sums(0)
    send_y(0, raw_fields, yr_recv)
    send_y(0, sum_fields, ym_recv)
    if by_word:
        corner_sums(0)
        pl.semaphore_wait(in_sem, len(column))
    send_corner_raw(0)
    send_corner_sums(0)
    face_shares(0)
    edge_shares(0)
    await_y_raw(0)
    await_x_raw(0)
    await_sums(0)
    finish_peak = spread_all(0, velocity_pass(0, None))
    send_heat_x(hx_recv.at[0], True)
    send_heat_y()
    edge_reads()
    ghost_pass(0, None)

    def store_st1(k, x, r, value):
        st1[k, x, pl.ds(ROW + r, ROW), :] = value

    collided(outer, None, store_st1)
    face_shares(1)
    send_x_shares()
    collided(inner, None, store_st1)
    send_corner_raw(1)
    pack_y_raw(1)
    send_y(1, raw_fields, yr_recv)
    send_x_raw(1)
    own_sums(1, outer)
    send_x_sums(1)
    own_sums(1, inner)
    send_y(1, sum_fields, ym_recv)
    corner_sums(1)
    send_corner_sums(1)
    send_heat_x(hx_recv.at[1], False)
    send_heat_corner()
    edge_shares(1)
    await_near_heat()
    near_heat()
    fs = finish_peak()
    await_y_raw(1)
    await_bytes(None, xo_in, xo_recv)
    finish_peak = spread_all(1, velocity_pass(1, fs))
    for x, r in blocks:
        for c in range(3):
            out_v[c, x, pl.ds(r, ROW), :] = vel[c, x + 1, pl.ds(ROW + r, ROW), :]
    await_far_heat()
    far_heat()
    await_x_raw(1)
    for s in (0, 1):
        for r in range(0, sy, ROW):
            face_reads(1, s, r)
    edge_reads()
    await_sums(1)
    ghost_pass(1, fs)

    def store_out(k, x, r, value):
        out_p[k, x, pl.ds(r, ROW), :] = value

    collided(blocks, fs, store_out)
    await_sends()
    fs = finish_peak()
    lift = {(x, r): fs * hb[x + 2, pl.ds(ROW + r, ROW), :] for x, r in blocks}
    for k in LIFTED:
        for x, r in blocks:
            rows = pl.ds(r, ROW)
            out_p[k, x, rows, :] = out_p[k, x, rows, :] + (3.0 * WEIGHT[k] * CS[k][2]) * lift[(x, r)]


def write_out(pops, vel, out_p, out_v, sems):
    copies = [
        pltpu.make_async_copy(pops, out_p, sems.at[0]),
        pltpu.make_async_copy(vel, out_v, sems.at[1]),
    ]
    for copy in copies:
        copy.start()
    for copy in copies:
        copy.wait()


def local(populations, heat_level, obstacle, heat_table):
    ngx = lax.axis_size("gx")
    ngy = lax.axis_size("gy")
    _, sx, sy, nz = populations.shape
    f32 = jnp.float32
    tall = sy + 2 * ROW
    dma = pltpu.SemaphoreType.DMA
    groups = peak_groups(ngx, ngy)
    phases = len(groups)
    vmem = pl.BlockSpec(memory_space=pltpu.VMEM)
    anywhere = pl.BlockSpec(memory_space=pltpu.HBM)
    shapes = (
        jax.ShapeDtypeStruct(populations.shape, f32),
        jax.ShapeDtypeStruct((3, sx, sy, nz), f32),
    )

    def floats(*shape):
        return pltpu.VMEM(shape, f32)

    def ints(*shape):
        return pltpu.VMEM(shape, jnp.int32)

    pops, velocity = pl.pallas_call(
        functools.partial(kernel, ngx, ngy),
        out_shape=shapes,
        in_specs=[anywhere] * 4,
        out_specs=[vmem] * 2,
        scratch_shapes=[
            floats(19, sx, tall, nz),
            floats(19, sx, tall, nz),
            floats(19, sx, sy, nz),
            floats(4, sx, sy, nz),
            floats(sx, sy, nz),
            floats(3, sx + 2, tall, nz),
            ints(sx, sy, nz),
            ints(sx, sy, nz),
            pltpu.SMEM(heat_table.shape, f32),
            ints(sx, sy, nz),
            floats(sx + 4, tall, nz),
            floats(sx + 4, tall, nz),
            floats(sx + 4, tall, nz),
            floats(4, sx + 2, sy, nz),
            floats(4, 2 * sx, nz),
            floats(STEPS, 2, 5, tall, nz),
            floats(STEPS, 2, 4, sy, nz),
            floats(STEPS, 2, 4, sy, nz),
            floats(STEPS, 9, 2 * sx, nz),
            floats(STEPS, 9, 2 * sx, nz),
            floats(8, ROW, nz),
            floats(STEPS, 6, ROW, nz),
            floats(STEPS, ROW, nz),
            floats(STEPS, 6, ROW, nz),
            floats(2, 3, sy, nz),
            floats(2, 3, sy, nz),
            floats(4, 2 * sx, nz),
            floats(5, 2 * sx, nz),
            floats(4, 2 * sx, nz),
            floats(2, ROW, nz),
            floats(4, ROW, nz),
            floats(4, 2 * sx, nz),
            floats(2, sy, nz),
            floats(2 * sx, nz),
            floats(8 * ROW, nz),
            floats(STEPS, phases, 1, nz),
            *[floats(STEPS, -(-len(group) // ROW) * ROW, nz) for group in groups],
            dma((4,)),
            pltpu.SemaphoreType.REGULAR,
            dma,
            dma((2,)),
            dma((STEPS,)),
            dma((STEPS,)),
            dma,
            dma((STEPS, 2)),
            dma((STEPS, 2)),
            dma((2,)),
            dma((2,)),
            dma((2,)),
            dma((phases,)),
            dma((STEPS, phases)),
        ],
        compiler_params=pltpu.CompilerParams(
            collective_id=0, has_side_effects=True, vmem_limit_bytes=24 * 1024 * 1024
        ),
        name="lattice_steps",
    )(*[pltpu.with_memory_space_constraint(a, pltpu.HBM) for a in (populations, heat_level, obstacle, heat_table)])
    return pl.pallas_call(
        write_out,
        out_shape=shapes,
        in_specs=[vmem] * 2,
        out_specs=[anywhere] * 2,
        scratch_shapes=[dma((2,))],
        compiler_params=pltpu.CompilerParams(vmem_limit_bytes=8 * 1024 * 1024),
        name="write_out",
    )(pops, velocity)


def solution(mesh):
    return jax.shard_map(
        local,
        mesh=mesh,
        in_specs=(
            P(None, ("member", "gx"), "gy", None),
            P(("member", "gx"), "gy", None),
            P(("member", "gx"), "gy", None),
            P(),
        ),
        out_specs=(P(None, ("member", "gx"), "gy", None), P(None, ("member", "gx"), "gy", None)),
        check_vma=False,
    )
```

```python
import functools

import jax
import jax.numpy as jnp
import numpy as np
from jax import lax
from jax.experimental import pallas as pl
from jax.experimental.pallas import tpu as pltpu
from jax.sharding import PartitionSpec as P

STEPS = 2
ROW = 8

lattice = np.array(
    [
        [0, 0, 0],
        [1, 0, 0],
        [-1, 0, 0],
        [0, 1, 0],
        [0, -1, 0],
        [0, 0, 1],
        [0, 0, -1],
        [1, 1, 0],
        [-1, -1, 0],
        [1, -1, 0],
        [-1, 1, 0],
        [1, 0, 1],
        [-1, 0, -1],
        [1, 0, -1],
        [-1, 0, 1],
        [0, 1, 1],
        [0, -1, -1],
        [0, 1, -1],
        [0, -1, 1],
    ]
)
CS = [tuple(int(c) for c in row) for row in lattice]
NUMBER = {c: k for k, c in enumerate(CS)}
WEIGHT = [1.0 / 3.0] + [1.0 / 18.0] * 6 + [1.0 / 36.0] * 12
OPP = [0, 2, 1, 4, 3, 6, 5, 8, 7, 10, 9, 12, 11, 14, 13, 16, 15, 18, 17]
base_tau = 0.52
smag_coef = 0.04
speed_cap = 0.1
strain_floor = 1e-06
LIFTED = [k for k in range(19) if CS[k][2] != 0]
ACROSS_X = {c: [NUMBER[(c, 0, 0)], NUMBER[(c, 1, 0)], NUMBER[(c, -1, 0)], NUMBER[(c, 0, 1)], NUMBER[(c, 0, -1)]] for c in (1, -1)}
ACROSS_Y = {c: [NUMBER[(0, c, 0)], NUMBER[(1, c, 0)], NUMBER[(-1, c, 0)], NUMBER[(0, c, 1)], NUMBER[(0, c, -1)]] for c in (1, -1)}
OUT = (-1, 1)
IN = (1, -1)


def tree_sum(items):
    items = list(items)
    while len(items) > 1:
        items = [items[i] + items[i + 1] if i + 1 < len(items) else items[i] for i in range(0, len(items), 2)]
    return items[0]


def peak_groups(ngx, ngy):
    if ngx * ngy <= 64:
        return [[(dx, dy) for dx in range(ngx) for dy in range(ngy) if dx or dy]]
    return [[(0, dy) for dy in range(1, ngy)], [(dx, 0) for dx in range(1, ngx)]]


def kernel(
    ngx, ngy,
    pops, heat_level, obstacle, table,
    out_p, out_v,
    st0, st1, rd, ms, rho_s, vel, hl, ob, tb, solid_s,
    hb, hzp, hzm, hm, hmy,
    xr, xm_out, xm_in, yb_out, yb_in, cg, cm_out, cr_in, cm_in,
    ox, ox2, xo_in, x2_in, oy, dr, dm, tu, ex, ey, gfx, gfy, flat, pm_src, *rest,
):
    (*pm_bufs, load_sem, in_sem, col_sem, x_send, y_send, xr_recv, xm_recv, xo_recv, yr_recv, ym_recv,
     hx_recv, hy_recv, p_send, p_recv) = rest
    _, sx, sy, nz = pops.shape
    levels = table.shape[0]
    gx = lax.axis_index("gx")
    gy = lax.axis_index("gy")
    has_up = gy < ngy - 1
    has_down = gy > 0
    right = lax.rem(gx + 1, ngx)
    left = lax.rem(gx + ngx - 1, ngx)
    own_y = pl.ds(ROW, sy)
    face_x = (0, sx - 1)
    edge_y = (0, sy - 1)
    x_of = (left, right)
    y_of = (gy - 1, gy + 1)
    has_y = (has_down, has_up)

    barrier = pltpu.get_barrier_semaphore()

    def greet(sem, x, y):
        pl.semaphore_signal(sem, inc=1, device_id={"gx": x, "gy": y}, device_id_type=pl.DeviceIdType.MESH)

    groups = peak_groups(ngx, ngy)
    beside = sorted({1, ngx - 1} - {0})
    column = [(0, dy) for dy in range(1, ngy)]
    by_word = len(groups) == 1 and ngx <= 5
    greeted = [(dx, 0) for dx in beside] + column if by_word else [place for group in groups for place in group]
    partners = len(greeted)
    for dx, dy in greeted:
        greet(barrier, lax.rem(gx + dx, ngx), lax.rem(gy + dy, ngy))
    if len(groups) > 1:
        partners = partners + 2 * (jnp.where(has_up, 1, 0) + jnp.where(has_down, 1, 0))
        for s in (0, 1):

            @pl.when(has_y[s])
            def _():
                greet(barrier, right, y_of[s])
                greet(barrier, left, y_of[s])

    load_p = pltpu.make_async_copy(pops, st0.at[:, :, own_y, :], load_sem.at[0])
    load_h = pltpu.make_async_copy(heat_level, hl, load_sem.at[1])
    load_o = pltpu.make_async_copy(obstacle, ob, load_sem.at[2])
    load_t = pltpu.make_async_copy(table, tb, load_sem.at[3])
    load_p.start()
    load_h.start()
    load_o.start()
    load_t.start()

    def zeros(ref, *index):
        part = ref.at[index]
        part[...] = jnp.zeros(part.shape, jnp.float32)

    every = slice(None)
    for row in (ROW - 1, ROW + sy):
        for st in (st0, st1):
            for c in (1, -1):
                for k in ACROSS_Y[c]:
                    zeros(st, k, every, pl.ds(row, 1), every)
        zeros(xr, every, every, pl.ds(row, 1), every)
    for ref in (cg, tu, ey):
        ref[...] = jnp.zeros(ref.shape, jnp.float32)

    for s in (0, 1):

        @pl.when(jnp.logical_not(has_y[s]))
        def _():
            zeros(yb_in, every, every, pl.ds(s * sx, sx), every)
            for xs in (0, 1):
                zeros(cr_in, every, pl.ds(xs * 2 + s, 1), every)
                zeros(cm_in, every, every, pl.ds(xs * 2 + s, 1), every)
            zeros(hb, every, pl.ds((ROW - 2, ROW + sy)[s], 2), every)

    def guarded(cond, fn):
        if cond is None:
            fn()
        else:
            pl.when(cond)(fn)

    def send(cond, pairs, send_sem, recv_sem, x, y):
        def go():
            for src, dst in pairs:
                pltpu.make_async_remote_copy(
                    src_ref=src, dst_ref=dst, send_sem=send_sem, recv_sem=recv_sem,
                    device_id={"gx": x, "gy": y}, device_id_type=pl.DeviceIdType.MESH,
                ).start()

        guarded(cond, go)

    def await_bytes(cond, view, sem):
        guarded(cond, lambda: pltpu.make_async_copy(view, view, sem).wait())

    states = (st0, st1)
    corners = [(xs, ys) for xs in (0, 1) for ys in (0, 1)]
    raw_fields = pl.ds(0, 5)
    sum_fields = pl.ds(5, 4)

    at_end = (gx == 0, gx == ngx - 1)

    def along_x(pairs_of, recv_sem):
        def far():
            for s in (0, 1):
                send(at_end[s], pairs_of(s), x_send, recv_sem, x_of[s], gy)

        def near():
            for s in (0, 1):
                send(jnp.logical_not(at_end[s]), pairs_of(s), x_send, recv_sem, x_of[s], gy)

        return far, near

    def send_x_raw():
        return along_x(
            lambda s: [(st0.at[k, face_x[s], own_y, :], xr.at[1 - s, j, own_y, :]) for j, k in enumerate(ACROSS_X[OUT[s]])],
            xr_recv.at[0],
        )

    def send_x_sums(step):
        return along_x(lambda s: [(xm_out.at[step, s], xm_in.at[step, 1 - s])], xm_recv.at[step])

    rest_rows = pl.ds(0, 2 * sy + 2)

    def send_x_shares():
        return along_x(lambda s: [(ox.at[s], xo_in.at[1 - s])], xo_recv)

    def send_x_rest():
        return along_x(lambda s: [(ox2.at[s, rest_rows, :], x2_in.at[1 - s, rest_rows, :])], xr_recv.at[1])

    def send_heat():
        for part in along_x(lambda s: [(hb.at[pl.ds((2, sx)[s], 2), own_y, :], hb.at[pl.ds((sx + 2, 0)[s], 2), own_y, :])], hx_recv):
            part()
        for s in (0, 1):
            src = hb.at[pl.ds(2, sx), pl.ds((ROW, ROW + sy - 2)[s], 2), :]
            dst = hb.at[pl.ds(2, sx), pl.ds((ROW + sy, ROW - 2)[s], 2), :]
            send(has_y[s], [(src, dst)], y_send.at[s], hy_recv.at[1 - s], gx, y_of[s])
        to_corners(
            lambda c, xs, ys: (
                hb.at[2 + face_x[xs], pl.ds(ROW + edge_y[ys], 1), :],
                hb.at[(sx + 2, 1)[xs], pl.ds((ROW + sy, ROW - 1)[ys], 1), :],
            ),
            lambda s: hy_recv.at[s],
        )

    def send_y(step, fields, recv_sem):
        for s in (0, 1):
            src = yb_out.at[step, fields, pl.ds(s * sx, sx), :]
            dst = yb_in.at[step, fields, pl.ds((1 - s) * sx, sx), :]
            send(has_y[s], [(src, dst)], y_send.at[s], recv_sem.at[step, 1 - s], gx, y_of[s])

    def to_corners(pair_of, sem_of):
        for c, (xs, ys) in enumerate(corners):
            send(has_y[ys], [pair_of(c, xs, ys)], y_send.at[ys], sem_of(1 - ys), x_of[xs], y_of[ys])

    def send_corner_raw(step):
        st = states[step]

        def pair(c, xs, ys):
            k = NUMBER[(OUT[xs], OUT[ys], 0)]
            return st.at[k, face_x[xs], pl.ds(ROW + edge_y[ys], 1), :], cr_in.at[step, pl.ds(3 - c, 1), :]

        to_corners(pair, lambda s: yr_recv.at[step, s])

    def send_corner_sums(step):
        to_corners(
            lambda c, xs, ys: (cm_out.at[step, :, pl.ds(c, 1), :], cm_in.at[step, :, pl.ds(3 - c, 1), :]),
            lambda s: ym_recv.at[step, s],
        )

    def await_y_raw(step):
        for s in (0, 1):
            await_bytes(has_y[s], flat.at[pl.ds(0, 5 * sx + 2), :], yr_recv.at[step, s])

    def await_x_raw():
        await_bytes(None, xr.at[:, :, own_y, :], xr_recv.at[0])

    def await_x_rest():
        await_bytes(None, x2_in.at[:, rest_rows, :], xr_recv.at[1])

    def await_sums(step):
        for s in (0, 1):
            await_bytes(has_y[s], flat.at[pl.ds(0, 4 * sx + 12), :], ym_recv.at[step, s])
        await_bytes(None, xm_in.at[step], xm_recv.at[step])

    def await_heat():
        for s in (0, 1):
            await_bytes(has_y[s], flat.at[pl.ds(0, 2 * sx + 2), :], hy_recv.at[s])
        await_bytes(None, hb.at[pl.ds(0, 4), own_y, :], hx_recv)

    def await_sends():
        for view in (xr.at[:, :, own_y, :], xm_out, ox, ox2.at[:, rest_rows, :], hb.at[pl.ds(0, 4), own_y, :]):
            await_bytes(None, view, x_send)
        for s in (0, 1):
            for view in (yb_out.at[:, :, pl.ds(0, sx), :], flat.at[pl.ds(0, 2 * sx + STEPS * 14 + 2), :]):
                await_bytes(has_y[s], view, y_send.at[s])
        for phase, group in enumerate(groups):
            for step in range(STEPS):
                await_bytes(None, pm_bufs[phase].at[step, pl.ds(0, len(group)), :], p_send.at[phase])

    def spread(step, phase, value):
        group = peak_groups(ngx, ngy)[phase]
        count = len(group)
        buf = pm_bufs[phase]
        pm_src[step, phase] = value
        for d, (dx, dy) in enumerate(group, 1):
            place = {"gx": lax.rem(gx + dx, ngx), "gy": lax.rem(gy + dy, ngy)}
            pltpu.make_async_remote_copy(
                src_ref=pm_src.at[step, phase],
                dst_ref=buf.at[step, pl.ds(d - 1, 1), :],
                send_sem=p_send.at[phase],
                recv_sem=p_recv.at[step, phase],
                device_id=place,
                device_id_type=pl.DeviceIdType.MESH,
            ).start()
        view = buf.at[step, pl.ds(0, count), :]

        def wait():
            await_bytes(None, view, p_recv.at[step, phase])
            return jnp.maximum(value, jnp.max(buf[step, pl.ds(0, count), :], axis=0, keepdims=True))

        return wait

    def spread_all(step, tile):
        wait = spread(step, 0, jnp.max(tile, axis=0, keepdims=True))

        def finish():
            best = wait()
            for phase in range(1, len(pm_bufs)):
                best = spread(step, phase, best)()
            peak = jnp.broadcast_to(jnp.max(best, axis=1, keepdims=True), (ROW, nz))
            return speed_cap * lax.rsqrt(speed_cap * speed_cap + peak)

        return finish

    blocks = [(x, r) for x in range(sx) for r in range(0, sy, ROW)]
    outer = [(x, r) for x, r in blocks if x in face_x]
    inner = [(x, r) for x, r in blocks if x not in face_x]
    lane = lax.broadcasted_iota(jnp.int32, (ROW, nz), 1)
    row_no = lax.broadcasted_iota(jnp.int32, (ROW, nz), 0)
    first_lane = lane == 0
    last_lane = lane == nz - 1
    edge_row = (row_no == 0, row_no == ROW - 1)
    pack_row = lax.broadcasted_iota(jnp.int32, (2 * sx, nz), 0)
    pack_sign = jnp.where(pack_row < sx, 1.0, -1.0)
    corner_x = jnp.where(row_no < 2, 1.0, -1.0)
    corner_y = jnp.where(lax.rem(row_no, 2) == 0, 1.0, -1.0)

    def shift_z(cells, cz):
        if not cz:
            return cells
        at = lax.broadcasted_iota(jnp.int32, cells.shape, 1)
        return jnp.where(at == (0 if cz > 0 else nz - 1), 0.0, pltpu.roll(cells, cz % nz, 1))

    def edges_of(r):
        return [s for s in (0, 1) if r == (0, sy - ROW)[s]]

    def own_sums(step, tiles):
        st = states[step]
        for x, r in tiles:
            rows = pl.ds(r, ROW)
            reads = {}
            for k, (cx, cy, cz) in enumerate(CS):
                if 0 <= x - cx < sx:
                    reads[k] = shift_z(st[k, x - cx, pl.ds(ROW + r - cy, ROW), :], cz)
                    rd[k, x, rows, :] = reads[k]
            sums = [tree_sum(list(reads.values()))]
            for c in range(3):
                plus = [reads[k] for k in reads if CS[k][c] > 0]
                minus = [reads[k] for k in reads if CS[k][c] < 0]
                if plus and minus:
                    sums.append(tree_sum(plus) - tree_sum(minus))
                else:
                    sums.append(tree_sum(plus) if plus else -tree_sum(minus))
            for m in range(4):
                ms[m, x, rows, :] = sums[m]
            sums[0] = jnp.where(solid_s[x, rows, :] != 0, 0.0, sums[0])
            for s in (0, 1):
                if x == face_x[s]:
                    for m in range(4):
                        xm_out[step, s, m, rows, :] = sums[m]
                if s in edges_of(r):
                    at = (0, ROW - 1)[s]
                    for m in range(4):
                        yb_out[step, 5 + m, pl.ds(s * sx + x, 1), :] = sums[m][at : at + 1, :]

    def pack_y_raw(step):
        st = states[step]
        for s in (0, 1):
            for j, k in enumerate(ACROSS_Y[OUT[s]]):
                for x in range(sx):
                    yb_out[step, j, pl.ds(s * sx + x, 1), :] = st[k, x, pl.ds(ROW + edge_y[s], 1), :]

    def corner_sums(step):
        st = states[step]
        for c, (xs, ys) in enumerate(corners):
            dx, dy = OUT[xs], OUT[ys]
            fx, fy = face_x[xs], edge_y[ys]
            places = [
                ((0, dy, 0), fx, fy), ((0, dy, 1), fx, fy), ((0, dy, -1), fx, fy), ((dx, dy, 0), fx - dx, fy),
                ((dx, 0, 0), fx, fy), ((dx, 0, 1), fx, fy), ((dx, 0, -1), fx, fy), ((dx, dy, 0), fx, fy - dy),
            ]
            for f, (direction, x, y) in enumerate(places):
                cg[f, pl.ds(c, 1), :] = st[NUMBER[direction], x, pl.ds(ROW + y, 1), :]
        for half, sign in ((0, -corner_x), (1, -corner_y)):
            a, b, d, e = (cg[4 * half + f] for f in range(4))
            b, d = shift_z(b, 1), shift_z(d, -1)
            cm_out[step, 3 * half + 0] = (a + b) + (d + e)
            cm_out[step, 3 * half + 1] = sign * e
            cm_out[step, 3 * half + 2] = b - d

    def packed(fields, fill):
        plus = jnp.where(lax.rem(pack_row, sx) == 0, 0.0, pltpu.roll(fields[1], 1, 0))
        minus = jnp.where(lax.rem(pack_row, sx) == sx - 1, 0.0, pltpu.roll(fields[2], 2 * sx - 1, 0))
        if fill is not None:
            for ys in (0, 1):
                plus = jnp.where(pack_row == ys * sx, fill(ys), plus)
                minus = jnp.where(pack_row == ys * sx + sx - 1, fill(2 + ys), minus)
        return [fields[0], plus, minus, shift_z(fields[3], 1), shift_z(fields[4], -1)]

    def face_shares(step):
        st = states[step]
        for s in (0, 1):
            for r in range(0, sy, ROW):
                ks = ACROSS_X[OUT[s]]
                a, b, c, d, e = (st[k, face_x[s], pl.ds(ROW + r - CS[k][1], ROW), :] for k in ks)
                d, e = shift_z(d, 1), shift_z(e, -1)
                ox[s, 0, pl.ds(r, ROW), :] = ((a + b) + (c + d)) + e
                ox[s, 1, pl.ds(r, ROW), :] = b - c
                ox[s, 2, pl.ds(r, ROW), :] = d - e
                if step == 1:
                    ox2[s, pl.ds(r, ROW), :] = b
                    ox2[s, pl.ds(sy + r, ROW), :] = d
            if step == 1:
                ox2[s, pl.ds(2 * sy, 1), :] = st[ACROSS_X[OUT[s]][2], face_x[s], pl.ds(ROW, 1), :]
                ox2[s, pl.ds(2 * sy + 1, 1), :] = st[ACROSS_X[OUT[s]][1], face_x[s], pl.ds(ROW + sy - 1, 1), :]

    def edge_shares(step):
        a, b, c, d, e = packed([yb_out[step, j] for j in range(5)], None)
        total = ((a + b) + (c + d)) + e
        oy[0] = total
        oy[1] = b - c
        oy[2] = -pack_sign * total
        oy[3] = d - e

    def velocity_pass(step, fs):
        fields = packed([yb_in[step, j] for j in range(5)], lambda c: cr_in[step, pl.ds(c, 1), :])
        for j in range(5):
            dr[j] = fields[j]
        a, b, c, d, e = fields
        total = ((a + b) + (c + d)) + e
        for m, value in enumerate((total, b - c, pack_sign * total, d - e)):
            dm[m] = value
        peak = jnp.zeros((ROW, nz), jnp.float32)
        for x, r in blocks:
            rows = pl.ds(r, ROW)
            sums = [ms[m, x, rows, :] for m in range(4)]
            for s in (0, 1):
                if x == face_x[s]:
                    if step == 0:
                        parts = face_raw(s, r)
                        shares = tree_sum(parts), parts[1] - parts[2], parts[3] - parts[4]
                        face_reads(s, r, parts)
                    else:
                        shares = [xo_in[s, m, rows, :] for m in range(3)]
                    sums[0] = sums[0] + shares[0]
                    sums[1] = sums[1] + shares[0] if s == 0 else sums[1] - shares[0]
                    sums[2] = sums[2] + shares[1]
                    sums[3] = sums[3] + shares[2]
            for s in edges_of(r):
                for m in range(4):
                    sums[m] = sums[m] + jnp.where(edge_row[s], dm[m, pl.ds(s * sx + x, 1), :], 0.0)
            if fs is not None:
                sums = [sums[m] + fs * hm[m, x + 1, rows, :] for m in range(4)]
            solid = solid_s[x, rows, :] != 0
            inv = jnp.where(solid, 0.0, 1.0 / jnp.where(solid, 1.0, sums[0]))
            rho_s[x, rows, :] = sums[0]
            speed = []
            for c in range(3):
                u = sums[1 + c] * inv
                vel[c, x + 1, pl.ds(ROW + r, ROW), :] = u
                speed.append(u * u)
            peak = jnp.maximum(peak, speed[0] + speed[1] + speed[2])
        return peak

    def face_raw(s, r):
        return [
            shift_z(xr[s, j, pl.ds(ROW + r - CS[k][1], ROW), :], CS[k][2]) for j, k in enumerate(ACROSS_X[IN[s]])
        ]

    def face_rest(s, r):
        total, along, height = (xo_in[s, m, pl.ds(r, ROW), :] for m in range(3))
        b, d = x2_in[s, pl.ds(r, ROW), :], x2_in[s, pl.ds(sy + r, ROW), :]
        c, e = b - along, d - height
        return [total - ((b + c) + (d + e)), b, c, d, e]

    def face_reads(s, r, parts):
        for k, part in zip(ACROSS_X[IN[s]], parts):
            rd[k, face_x[s], pl.ds(r, ROW), :] = part

    def edge_reads():
        for s in (0, 1):
            for j, k in enumerate(ACROSS_Y[IN[s]]):
                for x in range(sx):
                    rd[k, x, pl.ds(edge_y[s], 1), :] = dr[j, pl.ds(s * sx + x, 1), :]

    def ghost_pass(step, fs):
        for c, (xs, ys) in enumerate(corners):
            j = 1 if OUT[xs] > 0 else 2
            tu[0, pl.ds(c, 1), :] = yb_in[step, j, pl.ds(ys * sx + face_x[xs], 1), :]
            j = 1 if OUT[ys] > 0 else 2
            if step == 0:
                tu[1, pl.ds(c, 1), :] = xr[xs, j, pl.ds(ROW + edge_y[ys], 1), :]
            else:
                tu[1, pl.ds(c, 1), :] = x2_in[xs, pl.ds(2 * sy + ys, 1), :]
        over, up = tu[0], tu[1]
        total = cm_in[step, 0] + over
        for m, value in enumerate((total, cm_in[step, 1] - corner_x * over, corner_y * total, cm_in[step, 2])):
            ex[m] = value
        total = cm_in[step, 3] + up
        for m, value in enumerate((total, corner_x * total, cm_in[step, 4] - corner_y * up, cm_in[step, 5])):
            for c, (xs, ys) in enumerate(corners):
                ey[m, pl.ds(ys * sx + face_x[xs], 1), :] = value[c : c + 1, :]
        for s in (0, 1):
            for r in range(0, sy, ROW):
                rows = pl.ds(r, ROW)
                share = ox[s, 0, rows, :]
                sums = [xm_in[step, s, m, rows, :] for m in range(4)]
                if step == 0:
                    gfx[s, rows, :] = sums[0]
                fluid = gfx[s, rows, :] > 0.0
                sums[0] = sums[0] + share
                sums[1] = sums[1] - share if s == 0 else sums[1] + share
                sums[2] = sums[2] + ox[s, 1, rows, :]
                sums[3] = sums[3] + ox[s, 2, rows, :]
                for ys in edges_of(r):
                    for m in range(4):
                        sums[m] = sums[m] + jnp.where(edge_row[ys], ex[m, pl.ds(s * 2 + ys, 1), :], 0.0)
                at = (0, sx + 1)[s]
                if fs is not None:
                    sums = [sums[m] + fs * hm[m, at, rows, :] for m in range(4)]
                inv = jnp.where(fluid, 1.0 / jnp.where(fluid, sums[0], 1.0), 0.0)
                for c in range(3):
                    vel[c, at, pl.ds(ROW + r, ROW), :] = sums[1 + c] * inv
        sums = [yb_in[step, 5 + m] for m in range(4)]
        if step == 0:
            gfy[...] = sums[0]
        fluid = gfy[...] > 0.0
        sums = [sums[m] + oy[m] + ey[m] for m in range(4)]
        if fs is not None:
            sums = [sums[m] + fs[0:1, :] * hmy[m] for m in range(4)]
        inv = jnp.where(fluid, 1.0 / jnp.where(fluid, sums[0], 1.0), 0.0)
        for c in range(3):
            u = sums[1 + c] * inv
            for s in (0, 1):
                for x in range(sx):
                    at = s * sx + x
                    vel[c, x + 1, pl.ds((ROW - 1, ROW + sy)[s], 1), :] = u[at : at + 1, :]

    def shift_heat(x, row, span):
        cells = hb[x, pl.ds(row, span), :]
        hzp[x, pl.ds(row, span), :] = shift_z(cells, 1)
        hzm[x, pl.ds(row, span), :] = shift_z(cells, -1)

    def heat_moments(x, row, span):
        cells = [
            (hzp[i, pl.ds(y, span), :], hzm[i, pl.ds(y, span), :])
            for i, y in ((x, row), (x - 1, row), (x + 1, row), (x, row - 1), (x, row + 1))
        ]
        diff = [a - b for a, b in cells]
        both = [a + b for a, b in cells]
        main, side = 3.0 * WEIGHT[5], 3.0 * WEIGHT[11]
        return (
            main * diff[0] + side * ((diff[1] + diff[2]) + (diff[3] + diff[4])),
            side * (diff[1] - diff[2]),
            side * (diff[3] - diff[4]),
            main * both[0] + side * ((both[1] + both[2]) + (both[3] + both[4])),
        )

    def heat_sums(columns):
        for x in columns:
            for r in range(0, sy, ROW):
                for m, value in enumerate(heat_moments(x + 1, ROW + r, ROW)):
                    hm[m, x, pl.ds(r, ROW), :] = value

    def near_heat():
        for x in range(1, sx + 3):
            for r in range(0, sy, ROW):
                shift_heat(x, ROW + r, ROW)
        for x in range(2, sx + 2):
            shift_heat(x, ROW - 2, 2)
            shift_heat(x, ROW + sy, 2)
        heat_sums(range(1, sx + 1))

    def far_heat():
        for x in (0, sx + 3):
            for r in range(0, sy, ROW):
                shift_heat(x, ROW + r, ROW)
        for x in (1, sx + 2):
            shift_heat(x, ROW - 1, 1)
            shift_heat(x, ROW + sy, 1)
        heat_sums((0, sx + 1))
        for s in (0, 1):
            for x in range(sx):
                for m, value in enumerate(heat_moments(x + 2, (ROW - 1, ROW + sy)[s], 1)):
                    hmy[m, pl.ds(s * sx + x, 1), :] = value

    def collided(tiles, fs, store):
        for x, r in tiles:
            mid = pl.ds(ROW + r, ROW)
            u = [vel[c, x + 1, mid, :] for c in range(3)]
            diff = []
            for a in range(3):
                diff.append(
                    (
                        vel[a, x + 2, mid, :] - vel[a, x, mid, :],
                        vel[a, x + 1, pl.ds(ROW + r + 1, ROW), :] - vel[a, x + 1, pl.ds(ROW + r - 1, ROW), :],
                        pltpu.roll(u[a], nz - 1, 1) - pltpu.roll(u[a], 1, 1),
                    )
                )
            own = diff[0][0] * diff[0][0] + diff[1][1] * diff[1][1] + diff[2][2] * diff[2][2]
            xy = diff[0][1] + diff[1][0]
            xz = diff[0][2] + diff[2][0]
            yz = diff[1][2] + diff[2][1]
            size = jnp.sqrt(0.5 * own + 0.25 * (xy * xy + xz * xz + yz * yz) + strain_floor)
            omega = 1.0 / (base_tau + 3.0 * smag_coef * size)
            solid = solid_s[x, pl.ds(r, ROW), :] != 0
            density = rho_s[x, pl.ds(r, ROW), :]
            still = 1.0 - 1.5 * (u[0] * u[0] + u[1] * u[1] + u[2] * u[2])
            reads = [rd[k, x, pl.ds(r, ROW), :] for k in range(19)]
            if fs is not None:
                for k in LIFTED:
                    cx, cy, cz = CS[k]
                    source = hzp if cz > 0 else hzm
                    reads[k] = reads[k] + (3.0 * WEIGHT[k] * cz) * (fs * source[x + 2 - cx, pl.ds(ROW + r - cy, ROW), :])
            scaled = {w: (w * density) * omega for w in sorted(set(WEIGHT))}
            keep = 1.0 - omega
            store(0, x, r, jnp.where(solid, reads[0], keep * reads[0] + scaled[WEIGHT[0]] * still))
            for k in range(1, 19, 2):
                other = OPP[k]
                project = None
                for c in range(3):
                    if CS[k][c]:
                        if project is None:
                            project = u[c] if CS[k][c] > 0 else -u[c]
                        else:
                            project = project + u[c] if CS[k][c] > 0 else project - u[c]
                even = still + 4.5 * project * project
                odd = 3.0 * project
                weight = scaled[WEIGHT[k]]
                store(k, x, r, jnp.where(solid, reads[other], keep * reads[k] + weight * (even + odd)))
                store(other, x, r, jnp.where(solid, reads[k], keep * reads[other] + weight * (even - odd)))

    load_h.wait()
    load_o.wait()
    load_t.wait()
    for x, r in blocks:
        rows = pl.ds(r, ROW)
        code = hl[x, rows, :]
        heat = jnp.zeros((ROW, nz), jnp.float32)
        for level in range(levels):
            heat = jnp.where(code == level, tb[level], heat)
        grid_y = gy * sy + r + row_no
        solid = (
            (ob[x, rows, :] == 1) | (grid_y == 0) | (grid_y == ngy * sy - 1) | first_lane | last_lane
        )
        solid_s[x, rows, :] = jnp.where(solid, 1, 0)
        hb[x + 2, pl.ds(ROW + r, ROW), :] = jnp.where(solid, 0.0, heat)

    load_p.wait()
    own_sums(0, blocks)
    pack_y_raw(0)
    corner_sums(0)
    pl.semaphore_wait(barrier, partners)
    if by_word:
        for s in (0, 1):

            @pl.when(has_y[s])
            def _():
                greet(in_sem, gx, y_of[s])

        for _, dy in column:
            other = lax.rem(gy + dy, ngy)

            @pl.when((other > gy + 1) | (other < gy - 1))
            def _():
                greet(col_sem, gx, other)

    sums_far, sums_near = send_x_sums(0)
    raw_far, raw_near = send_x_raw()
    sums_far()
    send_y(0, raw_fields, yr_recv)
    send_y(0, sum_fields, ym_recv)
    neighbours = jnp.where(has_up, 1, 0) + jnp.where(has_down, 1, 0)
    if by_word:
        pl.semaphore_wait(in_sem, neighbours)
    send_corner_raw(0)
    send_corner_sums(0)
    sums_near()
    raw_far()
    if by_word:
        pl.semaphore_wait(col_sem, len(column) - neighbours)
    raw_near()
    face_shares(0)
    edge_shares(0)
    send_heat()
    await_y_raw(0)
    await_x_raw()
    await_sums(0)
    finish_peak = spread_all(0, velocity_pass(0, None))
    edge_reads()
    ghost_pass(0, None)

    def store_st1(k, x, r, value):
        st1[k, x, pl.ds(ROW + r, ROW), :] = value

    collided(outer, None, store_st1)
    face_shares(1)
    shares_far, shares_near = send_x_shares()
    shares_far()
    collided(inner, None, store_st1)
    shares_near()
    send_corner_raw(1)
    pack_y_raw(1)
    send_y(1, raw_fields, yr_recv)
    own_sums(1, outer)
    for part in (*send_x_sums(1), *send_x_rest()):
        part()
    own_sums(1, inner)
    send_y(1, sum_fields, ym_recv)
    corner_sums(1)
    send_corner_sums(1)
    edge_shares(1)
    await_heat()
    near_heat()
    fs = finish_peak()
    await_y_raw(1)
    await_bytes(None, xo_in, xo_recv)
    finish_peak = spread_all(1, velocity_pass(1, fs))
    for x, r in blocks:
        for c in range(3):
            out_v[c, x, pl.ds(r, ROW), :] = vel[c, x + 1, pl.ds(ROW + r, ROW), :]
    far_heat()
    await_x_rest()
    for s in (0, 1):
        for r in range(0, sy, ROW):
            face_reads(s, r, face_rest(s, r))
    edge_reads()
    await_sums(1)
    ghost_pass(1, fs)

    def store_out(k, x, r, value):
        out_p[k, x, pl.ds(r, ROW), :] = value

    collided(blocks, fs, store_out)
    await_sends()
    fs = finish_peak()
    lift = {(x, r): fs * hb[x + 2, pl.ds(ROW + r, ROW), :] for x, r in blocks}
    for k in LIFTED:
        for x, r in blocks:
            rows = pl.ds(r, ROW)
            out_p[k, x, rows, :] = out_p[k, x, rows, :] + (3.0 * WEIGHT[k] * CS[k][2]) * lift[(x, r)]


def write_out(pops, vel, out_p, out_v, sems):
    copies = [
        pltpu.make_async_copy(pops, out_p, sems.at[0]),
        pltpu.make_async_copy(vel, out_v, sems.at[1]),
    ]
    for copy in copies:
        copy.start()
    for copy in copies:
        copy.wait()


def local(populations, heat_level, obstacle, heat_table):
    ngx = lax.axis_size("gx")
    ngy = lax.axis_size("gy")
    _, sx, sy, nz = populations.shape
    f32 = jnp.float32
    tall = sy + 2 * ROW
    dma = pltpu.SemaphoreType.DMA
    groups = peak_groups(ngx, ngy)
    phases = len(groups)
    vmem = pl.BlockSpec(memory_space=pltpu.VMEM)
    anywhere = pl.BlockSpec(memory_space=pltpu.HBM)
    shapes = (
        jax.ShapeDtypeStruct(populations.shape, f32),
        jax.ShapeDtypeStruct((3, sx, sy, nz), f32),
    )

    def floats(*shape):
        return pltpu.VMEM(shape, f32)

    def ints(*shape):
        return pltpu.VMEM(shape, jnp.int32)

    pops, velocity = pl.pallas_call(
        functools.partial(kernel, ngx, ngy),
        out_shape=shapes,
        in_specs=[anywhere] * 4,
        out_specs=[vmem] * 2,
        scratch_shapes=[
            floats(19, sx, tall, nz),
            floats(19, sx, tall, nz),
            floats(19, sx, sy, nz),
            floats(4, sx, sy, nz),
            floats(sx, sy, nz),
            floats(3, sx + 2, tall, nz),
            ints(sx, sy, nz),
            ints(sx, sy, nz),
            pltpu.SMEM(heat_table.shape, f32),
            ints(sx, sy, nz),
            floats(sx + 4, tall, nz),
            floats(sx + 4, tall, nz),
            floats(sx + 4, tall, nz),
            floats(4, sx + 2, sy, nz),
            floats(4, 2 * sx, nz),
            floats(2, 5, tall, nz),
            floats(STEPS, 2, 4, sy, nz),
            floats(STEPS, 2, 4, sy, nz),
            floats(STEPS, 9, 2 * sx, nz),
            floats(STEPS, 9, 2 * sx, nz),
            floats(8, ROW, nz),
            floats(STEPS, 6, ROW, nz),
            floats(STEPS, ROW, nz),
            floats(STEPS, 6, ROW, nz),
            floats(2, 3, sy, nz),
            floats(2, 2 * sy + ROW, nz),
            floats(2, 3, sy, nz),
            floats(2, 2 * sy + ROW, nz),
            floats(4, 2 * sx, nz),
            floats(5, 2 * sx, nz),
            floats(4, 2 * sx, nz),
            floats(2, ROW, nz),
            floats(4, ROW, nz),
            floats(4, 2 * sx, nz),
            floats(2, sy, nz),
            floats(2 * sx, nz),
            floats(8 * ROW, nz),
            floats(STEPS, phases, 1, nz),
            *[floats(STEPS, -(-len(group) // ROW) * ROW, nz) for group in groups],
            dma((4,)),
            pltpu.SemaphoreType.REGULAR,
            pltpu.SemaphoreType.REGULAR,
            dma,
            dma((2,)),
            dma((STEPS,)),
            dma((STEPS,)),
            dma,
            dma((STEPS, 2)),
            dma((STEPS, 2)),
            dma,
            dma((2,)),
            dma((phases,)),
            dma((STEPS, phases)),
        ],
        compiler_params=pltpu.CompilerParams(
            collective_id=0, has_side_effects=True, vmem_limit_bytes=24 * 1024 * 1024
        ),
        name="lattice_steps",
    )(*[pltpu.with_memory_space_constraint(a, pltpu.HBM) for a in (populations, heat_level, obstacle, heat_table)])
    return pl.pallas_call(
        write_out,
        out_shape=shapes,
        in_specs=[vmem] * 2,
        out_specs=[anywhere] * 2,
        scratch_shapes=[dma((2,))],
        compiler_params=pltpu.CompilerParams(vmem_limit_bytes=8 * 1024 * 1024),
        name="write_out",
    )(pops, velocity)


def solution(mesh):
    return jax.shard_map(
        local,
        mesh=mesh,
        in_specs=(
            P(None, ("member", "gx"), "gy", None),
            P(("member", "gx"), "gy", None),
            P(("member", "gx"), "gy", None),
            P(),
        ),
        out_specs=(P(None, ("member", "gx"), "gy", None), P(None, ("member", "gx"), "gy", None)),
        check_vma=False,
    )
```

```python
import functools

import jax
import jax.numpy as jnp
import numpy as np
from jax import lax
from jax.experimental import pallas as pl
from jax.experimental.pallas import tpu as pltpu
from jax.sharding import PartitionSpec as P

STEPS = 2
ROW = 8

lattice = np.array(
    [
        [0, 0, 0],
        [1, 0, 0],
        [-1, 0, 0],
        [0, 1, 0],
        [0, -1, 0],
        [0, 0, 1],
        [0, 0, -1],
        [1, 1, 0],
        [-1, -1, 0],
        [1, -1, 0],
        [-1, 1, 0],
        [1, 0, 1],
        [-1, 0, -1],
        [1, 0, -1],
        [-1, 0, 1],
        [0, 1, 1],
        [0, -1, -1],
        [0, 1, -1],
        [0, -1, 1],
    ]
)
CS = [tuple(int(c) for c in row) for row in lattice]
NUMBER = {c: k for k, c in enumerate(CS)}
WEIGHT = [1.0 / 3.0] + [1.0 / 18.0] * 6 + [1.0 / 36.0] * 12
OPP = [0, 2, 1, 4, 3, 6, 5, 8, 7, 10, 9, 12, 11, 14, 13, 16, 15, 18, 17]
base_tau = 0.52
smag_coef = 0.04
speed_cap = 0.1
strain_floor = 1e-06
LIFTED = [k for k in range(19) if CS[k][2] != 0]
ACROSS_X = {c: [NUMBER[(c, 0, 0)], NUMBER[(c, 1, 0)], NUMBER[(c, -1, 0)], NUMBER[(c, 0, 1)], NUMBER[(c, 0, -1)]] for c in (1, -1)}
ACROSS_Y = {c: [NUMBER[(0, c, 0)], NUMBER[(1, c, 0)], NUMBER[(-1, c, 0)], NUMBER[(0, c, 1)], NUMBER[(0, c, -1)]] for c in (1, -1)}
OUT = (-1, 1)
IN = (1, -1)


def tree_sum(items):
    items = list(items)
    while len(items) > 1:
        items = [items[i] + items[i + 1] if i + 1 < len(items) else items[i] for i in range(0, len(items), 2)]
    return items[0]


def peak_groups(ngx, ngy):
    if ngx * ngy <= 64:
        return [[(dx, dy) for dx in range(ngx) for dy in range(ngy) if dx or dy]]
    return [[(0, dy) for dy in range(1, ngy)], [(dx, 0) for dx in range(1, ngx)]]


def kernel(
    ngx, ngy,
    pops, heat_level, obstacle, table,
    out_p, out_v,
    st0, st1, rd, ms, rho_s, vel, hl, ob, tb, solid_s,
    hb, hzp, hzm, hm, hmy,
    xr, xm_out, xm_in, yb_out, yb_in, cg, cm_out, cr_in, cm_in,
    ox, ox2, xo_in, x2_in, oy, dr, dm, tu, ex, ey, gfx, gfy, flat, pm_src, *rest,
):
    (*pm_bufs, load_sem, in_sem, col_sem, x_send, y_send, xr_recv, xm_recv, xo_recv, yr_recv, ym_recv,
     cm_recv, hx_recv, hy_recv, p_send, p_recv) = rest
    _, sx, sy, nz = pops.shape
    levels = table.shape[0]
    gx = lax.axis_index("gx")
    gy = lax.axis_index("gy")
    has_up = gy < ngy - 1
    has_down = gy > 0
    right = lax.rem(gx + 1, ngx)
    left = lax.rem(gx + ngx - 1, ngx)
    own_y = pl.ds(ROW, sy)
    face_x = (0, sx - 1)
    edge_y = (0, sy - 1)
    x_of = (left, right)
    y_of = (gy - 1, gy + 1)
    has_y = (has_down, has_up)

    barrier = pltpu.get_barrier_semaphore()

    def greet(sem, x, y):
        pl.semaphore_signal(sem, inc=1, device_id={"gx": x, "gy": y}, device_id_type=pl.DeviceIdType.MESH)

    groups = peak_groups(ngx, ngy)
    beside = sorted({1, ngx - 1} - {0})
    column = [(0, dy) for dy in range(1, ngy)]
    by_word = len(groups) == 1 and ngx <= 5
    greeted = [(dx, 0) for dx in beside] + column if by_word else [place for group in groups for place in group]
    partners = len(greeted)
    for dx, dy in greeted:
        greet(barrier, lax.rem(gx + dx, ngx), lax.rem(gy + dy, ngy))
    if len(groups) > 1:
        partners = partners + 2 * (jnp.where(has_up, 1, 0) + jnp.where(has_down, 1, 0))
        for s in (0, 1):

            @pl.when(has_y[s])
            def _():
                greet(barrier, right, y_of[s])
                greet(barrier, left, y_of[s])

    load_p = pltpu.make_async_copy(pops, st0.at[:, :, own_y, :], load_sem.at[0])
    load_h = pltpu.make_async_copy(heat_level, hl, load_sem.at[1])
    load_o = pltpu.make_async_copy(obstacle, ob, load_sem.at[2])
    load_t = pltpu.make_async_copy(table, tb, load_sem.at[3])
    load_p.start()
    load_h.start()
    load_o.start()
    load_t.start()

    def zeros(ref, *index):
        part = ref.at[index]
        part[...] = jnp.zeros(part.shape, jnp.float32)

    every = slice(None)
    for row in (ROW - 1, ROW + sy):
        for st in (st0, st1):
            for c in (1, -1):
                for k in ACROSS_Y[c]:
                    zeros(st, k, every, pl.ds(row, 1), every)
        zeros(xr, every, every, pl.ds(row, 1), every)
    for ref in (cg, tu, ey):
        ref[...] = jnp.zeros(ref.shape, jnp.float32)

    for s in (0, 1):

        @pl.when(jnp.logical_not(has_y[s]))
        def _():
            zeros(yb_in, every, every, pl.ds(s * sx, sx), every)
            for xs in (0, 1):
                zeros(cr_in, every, pl.ds(xs * 2 + s, 1), every)
                zeros(cm_in, every, every, pl.ds(xs * 2 + s, 1), every)
            zeros(hb, every, pl.ds((ROW - 2, ROW + sy)[s], 2), every)

    def guarded(cond, fn):
        if cond is None:
            fn()
        else:
            pl.when(cond)(fn)

    def send(cond, pairs, send_sem, recv_sem, x, y):
        def go():
            for src, dst in pairs:
                pltpu.make_async_remote_copy(
                    src_ref=src, dst_ref=dst, send_sem=send_sem, recv_sem=recv_sem,
                    device_id={"gx": x, "gy": y}, device_id_type=pl.DeviceIdType.MESH,
                ).start()

        guarded(cond, go)

    def await_bytes(cond, view, sem):
        guarded(cond, lambda: pltpu.make_async_copy(view, view, sem).wait())

    states = (st0, st1)
    corners = [(xs, ys) for xs in (0, 1) for ys in (0, 1)]
    raw_fields = pl.ds(0, 5)
    sum_fields = pl.ds(5, 4)

    at_end = (gx == 0, gx == ngx - 1)

    def along_x(pairs_of, sem_of):
        def far():
            for s in (0, 1):
                send(at_end[s], pairs_of(s), x_send, sem_of(s), x_of[s], gy)

        def near():
            for s in (0, 1):
                send(jnp.logical_not(at_end[s]), pairs_of(s), x_send, sem_of(s), x_of[s], gy)

        return far, near

    def send_x_raw():
        return along_x(
            lambda s: [(st0.at[k, face_x[s], own_y, :], xr.at[1 - s, j, own_y, :]) for j, k in enumerate(ACROSS_X[OUT[s]])],
            lambda s: xr_recv.at[0],
        )

    def send_x_sums(step):
        return along_x(lambda s: [(xm_out.at[step, s], xm_in.at[step, 1 - s])], lambda s: xm_recv.at[step, 1 - s])

    rest_rows = pl.ds(0, 2 * sy + 2)

    def send_x_shares(s):
        send(None, [(ox.at[s], xo_in.at[1 - s])], x_send, xo_recv, x_of[s], gy)

    def send_x_rest():
        return along_x(lambda s: [(ox2.at[s, rest_rows, :], x2_in.at[1 - s, rest_rows, :])], lambda s: xr_recv.at[1])

    def send_heat():
        for part in along_x(lambda s: [(hb.at[pl.ds((2, sx)[s], 2), own_y, :], hb.at[pl.ds((sx + 2, 0)[s], 2), own_y, :])], lambda s: hx_recv):
            part()
        for s in (0, 1):
            src = hb.at[pl.ds(2, sx), pl.ds((ROW, ROW + sy - 2)[s], 2), :]
            dst = hb.at[pl.ds(2, sx), pl.ds((ROW + sy, ROW - 2)[s], 2), :]
            send(has_y[s], [(src, dst)], y_send.at[s], hy_recv.at[1 - s], gx, y_of[s])
        to_corners(
            lambda c, xs, ys: (
                hb.at[2 + face_x[xs], pl.ds(ROW + edge_y[ys], 1), :],
                hb.at[(sx + 2, 1)[xs], pl.ds((ROW + sy, ROW - 1)[ys], 1), :],
            ),
            lambda c: hy_recv.at[c % 2],
        )

    def send_y(step, fields, recv_sem):
        for s in (0, 1):
            src = yb_out.at[step, fields, pl.ds(s * sx, sx), :]
            dst = yb_in.at[step, fields, pl.ds((1 - s) * sx, sx), :]
            send(has_y[s], [(src, dst)], y_send.at[s], recv_sem.at[step, 1 - s], gx, y_of[s])

    def to_corners(pair_of, sem_of):
        for c, (xs, ys) in enumerate(corners):
            send(has_y[ys], [pair_of(c, xs, ys)], y_send.at[ys], sem_of(3 - c), x_of[xs], y_of[ys])

    def send_corner_raw(step):
        st = states[step]

        def pair(c, xs, ys):
            k = NUMBER[(OUT[xs], OUT[ys], 0)]
            return st.at[k, face_x[xs], pl.ds(ROW + edge_y[ys], 1), :], cr_in.at[step, pl.ds(3 - c, 1), :]

        to_corners(pair, lambda c: yr_recv.at[step, c % 2])

    def send_corner_sums(step):
        to_corners(
            lambda c, xs, ys: (cm_out.at[step, :, pl.ds(c, 1), :], cm_in.at[step, :, pl.ds(3 - c, 1), :]),
            lambda c: cm_recv.at[step, c],
        )

    def await_y_raw(step):
        for s in (0, 1):
            await_bytes(has_y[s], flat.at[pl.ds(0, 5 * sx + 2), :], yr_recv.at[step, s])

    def await_x_raw():
        await_bytes(None, xr.at[:, :, own_y, :], xr_recv.at[0])

    def await_x_rest():
        await_bytes(None, x2_in.at[:, rest_rows, :], xr_recv.at[1])

    def await_y_sums(step):
        for s in (0, 1):
            await_bytes(has_y[s], yb_in.at[step, sum_fields, pl.ds(s * sx, sx), :], ym_recv.at[step, s])

    def await_x_sums(step, s):
        for ys in (0, 1):
            await_bytes(has_y[ys], cm_in.at[step, :, pl.ds(2 * s + ys, 1), :], cm_recv.at[step, 2 * s + ys])
        await_bytes(None, xm_in.at[step, s], xm_recv.at[step, s])

    def await_heat():
        for s in (0, 1):
            await_bytes(has_y[s], flat.at[pl.ds(0, 2 * sx + 2), :], hy_recv.at[s])
        await_bytes(None, hb.at[pl.ds(0, 4), own_y, :], hx_recv)

    def await_sends():
        for view in (xr.at[:, :, own_y, :], xm_out, ox, ox2.at[:, rest_rows, :], hb.at[pl.ds(0, 4), own_y, :]):
            await_bytes(None, view, x_send)
        for s in (0, 1):
            for view in (yb_out.at[:, :, pl.ds(0, sx), :], flat.at[pl.ds(0, 2 * sx + STEPS * 14 + 2), :]):
                await_bytes(has_y[s], view, y_send.at[s])
        for phase, group in enumerate(groups):
            for step in range(STEPS):
                await_bytes(None, pm_bufs[phase].at[step, pl.ds(0, len(group)), :], p_send.at[phase])

    def spread(step, phase, value):
        group = peak_groups(ngx, ngy)[phase]
        count = len(group)
        buf = pm_bufs[phase]
        pm_src[step, phase] = value
        for d, (dx, dy) in sorted(enumerate(group, 1), key=lambda item: item[1][0] in (0, ngx // 2)):
            place = {"gx": lax.rem(gx + dx, ngx), "gy": lax.rem(gy + dy, ngy)}
            pltpu.make_async_remote_copy(
                src_ref=pm_src.at[step, phase],
                dst_ref=buf.at[step, pl.ds(d - 1, 1), :],
                send_sem=p_send.at[phase],
                recv_sem=p_recv.at[step, phase],
                device_id=place,
                device_id_type=pl.DeviceIdType.MESH,
            ).start()
        view = buf.at[step, pl.ds(0, count), :]

        def wait():
            await_bytes(None, view, p_recv.at[step, phase])
            return jnp.maximum(value, jnp.max(buf[step, pl.ds(0, count), :], axis=0, keepdims=True))

        return wait

    def spread_all(step, tile):
        wait = spread(step, 0, jnp.max(tile, axis=0, keepdims=True))

        def finish():
            best = wait()
            for phase in range(1, len(pm_bufs)):
                best = spread(step, phase, best)()
            peak = jnp.broadcast_to(jnp.max(best, axis=1, keepdims=True), (ROW, nz))
            return speed_cap * lax.rsqrt(speed_cap * speed_cap + peak)

        return finish

    blocks = [(x, r) for x in range(sx) for r in range(0, sy, ROW)]
    outer = [(x, r) for x, r in blocks if x in face_x]
    inner = [(x, r) for x, r in blocks if x not in face_x]
    lane = lax.broadcasted_iota(jnp.int32, (ROW, nz), 1)
    row_no = lax.broadcasted_iota(jnp.int32, (ROW, nz), 0)
    first_lane = lane == 0
    last_lane = lane == nz - 1
    edge_row = (row_no == 0, row_no == ROW - 1)
    pack_row = lax.broadcasted_iota(jnp.int32, (2 * sx, nz), 0)
    pack_sign = jnp.where(pack_row < sx, 1.0, -1.0)
    corner_x = jnp.where(row_no < 2, 1.0, -1.0)
    corner_y = jnp.where(lax.rem(row_no, 2) == 0, 1.0, -1.0)

    def shift_z(cells, cz):
        if not cz:
            return cells
        at = lax.broadcasted_iota(jnp.int32, cells.shape, 1)
        return jnp.where(at == (0 if cz > 0 else nz - 1), 0.0, pltpu.roll(cells, cz % nz, 1))

    def edges_of(r):
        return [s for s in (0, 1) if r == (0, sy - ROW)[s]]

    def own_sums(step, tiles):
        st = states[step]
        for x, r in tiles:
            rows = pl.ds(r, ROW)
            reads = {}
            for k, (cx, cy, cz) in enumerate(CS):
                if 0 <= x - cx < sx:
                    reads[k] = shift_z(st[k, x - cx, pl.ds(ROW + r - cy, ROW), :], cz)
                    rd[k, x, rows, :] = reads[k]
            sums = [tree_sum(list(reads.values()))]
            for c in range(3):
                plus = [reads[k] for k in reads if CS[k][c] > 0]
                minus = [reads[k] for k in reads if CS[k][c] < 0]
                if plus and minus:
                    sums.append(tree_sum(plus) - tree_sum(minus))
                else:
                    sums.append(tree_sum(plus) if plus else -tree_sum(minus))
            for m in range(4):
                ms[m, x, rows, :] = sums[m]
            sums[0] = jnp.where(solid_s[x, rows, :] != 0, 0.0, sums[0])
            for s in (0, 1):
                if x == face_x[s]:
                    for m in range(4):
                        xm_out[step, s, m, rows, :] = sums[m]
                if s in edges_of(r):
                    at = (0, ROW - 1)[s]
                    for m in range(4):
                        yb_out[step, 5 + m, pl.ds(s * sx + x, 1), :] = sums[m][at : at + 1, :]

    def pack_y_raw(step):
        st = states[step]
        for s in (0, 1):
            for j, k in enumerate(ACROSS_Y[OUT[s]]):
                for x in range(sx):
                    yb_out[step, j, pl.ds(s * sx + x, 1), :] = st[k, x, pl.ds(ROW + edge_y[s], 1), :]

    def corner_sums(step):
        st = states[step]
        for c, (xs, ys) in enumerate(corners):
            dx, dy = OUT[xs], OUT[ys]
            fx, fy = face_x[xs], edge_y[ys]
            places = [
                ((0, dy, 0), fx, fy), ((0, dy, 1), fx, fy), ((0, dy, -1), fx, fy), ((dx, dy, 0), fx - dx, fy),
                ((dx, 0, 0), fx, fy), ((dx, 0, 1), fx, fy), ((dx, 0, -1), fx, fy), ((dx, dy, 0), fx, fy - dy),
            ]
            for f, (direction, x, y) in enumerate(places):
                cg[f, pl.ds(c, 1), :] = st[NUMBER[direction], x, pl.ds(ROW + y, 1), :]
        for half, sign in ((0, -corner_x), (1, -corner_y)):
            a, b, d, e = (cg[4 * half + f] for f in range(4))
            b, d = shift_z(b, 1), shift_z(d, -1)
            cm_out[step, 3 * half + 0] = (a + b) + (d + e)
            cm_out[step, 3 * half + 1] = sign * e
            cm_out[step, 3 * half + 2] = b - d

    def packed(fields, fill):
        plus = jnp.where(lax.rem(pack_row, sx) == 0, 0.0, pltpu.roll(fields[1], 1, 0))
        minus = jnp.where(lax.rem(pack_row, sx) == sx - 1, 0.0, pltpu.roll(fields[2], 2 * sx - 1, 0))
        if fill is not None:
            for ys in (0, 1):
                plus = jnp.where(pack_row == ys * sx, fill(ys), plus)
                minus = jnp.where(pack_row == ys * sx + sx - 1, fill(2 + ys), minus)
        return [fields[0], plus, minus, shift_z(fields[3], 1), shift_z(fields[4], -1)]

    def face_shares(step, sides):
        st = states[step]
        for s in sides:
            for r in range(0, sy, ROW):
                ks = ACROSS_X[OUT[s]]
                a, b, c, d, e = (st[k, face_x[s], pl.ds(ROW + r - CS[k][1], ROW), :] for k in ks)
                d, e = shift_z(d, 1), shift_z(e, -1)
                ox[s, 0, pl.ds(r, ROW), :] = ((a + b) + (c + d)) + e
                ox[s, 1, pl.ds(r, ROW), :] = b - c
                ox[s, 2, pl.ds(r, ROW), :] = d - e
                if step == 1:
                    ox2[s, pl.ds(r, ROW), :] = b
                    ox2[s, pl.ds(sy + r, ROW), :] = d
            if step == 1:
                ox2[s, pl.ds(2 * sy, 1), :] = st[ACROSS_X[OUT[s]][2], face_x[s], pl.ds(ROW, 1), :]
                ox2[s, pl.ds(2 * sy + 1, 1), :] = st[ACROSS_X[OUT[s]][1], face_x[s], pl.ds(ROW + sy - 1, 1), :]

    def edge_shares(step):
        a, b, c, d, e = packed([yb_out[step, j] for j in range(5)], None)
        total = ((a + b) + (c + d)) + e
        oy[0] = total
        oy[1] = b - c
        oy[2] = -pack_sign * total
        oy[3] = d - e

    def velocity_pass(step, fs):
        fields = packed([yb_in[step, j] for j in range(5)], lambda c: cr_in[step, pl.ds(c, 1), :])
        for j in range(5):
            dr[j] = fields[j]
        a, b, c, d, e = fields
        total = ((a + b) + (c + d)) + e
        for m, value in enumerate((total, b - c, pack_sign * total, d - e)):
            dm[m] = value
        peak = jnp.zeros((ROW, nz), jnp.float32)
        for x, r in blocks:
            rows = pl.ds(r, ROW)
            sums = [ms[m, x, rows, :] for m in range(4)]
            for s in (0, 1):
                if x == face_x[s]:
                    if step == 0:
                        parts = face_raw(s, r)
                        shares = tree_sum(parts), parts[1] - parts[2], parts[3] - parts[4]
                        face_reads(s, r, parts)
                    else:
                        shares = [xo_in[s, m, rows, :] for m in range(3)]
                    sums[0] = sums[0] + shares[0]
                    sums[1] = sums[1] + shares[0] if s == 0 else sums[1] - shares[0]
                    sums[2] = sums[2] + shares[1]
                    sums[3] = sums[3] + shares[2]
            for s in edges_of(r):
                for m in range(4):
                    sums[m] = sums[m] + jnp.where(edge_row[s], dm[m, pl.ds(s * sx + x, 1), :], 0.0)
            if fs is not None:
                sums = [sums[m] + fs * hm[m, x + 1, rows, :] for m in range(4)]
            solid = solid_s[x, rows, :] != 0
            inv = jnp.where(solid, 0.0, 1.0 / jnp.where(solid, 1.0, sums[0]))
            rho_s[x, rows, :] = sums[0]
            speed = []
            for c in range(3):
                u = sums[1 + c] * inv
                vel[c, x + 1, pl.ds(ROW + r, ROW), :] = u
                speed.append(u * u)
            peak = jnp.maximum(peak, speed[0] + speed[1] + speed[2])
        return peak

    def face_raw(s, r):
        return [
            shift_z(xr[s, j, pl.ds(ROW + r - CS[k][1], ROW), :], CS[k][2]) for j, k in enumerate(ACROSS_X[IN[s]])
        ]

    def face_rest(s, r):
        total, along, height = (xo_in[s, m, pl.ds(r, ROW), :] for m in range(3))
        b, d = x2_in[s, pl.ds(r, ROW), :], x2_in[s, pl.ds(sy + r, ROW), :]
        c, e = b - along, d - height
        return [total - ((b + c) + (d + e)), b, c, d, e]

    def face_reads(s, r, parts):
        for k, part in zip(ACROSS_X[IN[s]], parts):
            rd[k, face_x[s], pl.ds(r, ROW), :] = part

    def edge_reads():
        for s in (0, 1):
            for j, k in enumerate(ACROSS_Y[IN[s]]):
                for x in range(sx):
                    rd[k, x, pl.ds(edge_y[s], 1), :] = dr[j, pl.ds(s * sx + x, 1), :]

    def ghost_x(step, fs, s):
        own = pl.ds(2 * s, 2)
        for ys in (0, 1):
            c = 2 * s + ys
            j = 1 if OUT[s] > 0 else 2
            tu[0, pl.ds(c, 1), :] = yb_in[step, j, pl.ds(ys * sx + face_x[s], 1), :]
            j = 1 if OUT[ys] > 0 else 2
            if step == 0:
                tu[1, pl.ds(c, 1), :] = xr[s, j, pl.ds(ROW + edge_y[ys], 1), :]
            else:
                tu[1, pl.ds(c, 1), :] = x2_in[s, pl.ds(2 * sy + ys, 1), :]
        sums = [cm_in[step, m, own, :] for m in range(6)]
        over, up = tu[0, own, :], tu[1, own, :]
        sign = jnp.where(lax.broadcasted_iota(jnp.int32, (2, nz), 0) == 0, 1.0, -1.0)
        total = sums[0] + over
        for m, value in enumerate((total, sums[1] + OUT[s] * over, sign * total, sums[2])):
            ex[m, own, :] = value
        total = sums[3] + up
        for m, value in enumerate((total, IN[s] * total, sums[4] - sign * up, sums[5])):
            for ys in (0, 1):
                ey[m, pl.ds(ys * sx + face_x[s], 1), :] = value[ys : ys + 1, :]
        for r in range(0, sy, ROW):
            rows = pl.ds(r, ROW)
            share = ox[s, 0, rows, :]
            sums = [xm_in[step, s, m, rows, :] for m in range(4)]
            if step == 0:
                gfx[s, rows, :] = sums[0]
            fluid = gfx[s, rows, :] > 0.0
            sums[0] = sums[0] + share
            sums[1] = sums[1] - share if s == 0 else sums[1] + share
            sums[2] = sums[2] + ox[s, 1, rows, :]
            sums[3] = sums[3] + ox[s, 2, rows, :]
            for ys in edges_of(r):
                for m in range(4):
                    sums[m] = sums[m] + jnp.where(edge_row[ys], ex[m, pl.ds(s * 2 + ys, 1), :], 0.0)
            at = (0, sx + 1)[s]
            if fs is not None:
                sums = [sums[m] + fs * hm[m, at, rows, :] for m in range(4)]
            inv = jnp.where(fluid, 1.0 / jnp.where(fluid, sums[0], 1.0), 0.0)
            for c in range(3):
                vel[c, at, pl.ds(ROW + r, ROW), :] = sums[1 + c] * inv

    def ghost_y(step, fs):
        sums = [yb_in[step, 5 + m] for m in range(4)]
        if step == 0:
            gfy[...] = sums[0]
        fluid = gfy[...] > 0.0
        sums = [sums[m] + oy[m] + ey[m] for m in range(4)]
        if fs is not None:
            sums = [sums[m] + fs[0:1, :] * hmy[m] for m in range(4)]
        inv = jnp.where(fluid, 1.0 / jnp.where(fluid, sums[0], 1.0), 0.0)
        for c in range(3):
            u = sums[1 + c] * inv
            for s in (0, 1):
                for x in range(sx):
                    at = s * sx + x
                    vel[c, x + 1, pl.ds((ROW - 1, ROW + sy)[s], 1), :] = u[at : at + 1, :]

    def shift_heat(x, row, span):
        cells = hb[x, pl.ds(row, span), :]
        hzp[x, pl.ds(row, span), :] = shift_z(cells, 1)
        hzm[x, pl.ds(row, span), :] = shift_z(cells, -1)

    def heat_moments(x, row, span):
        cells = [
            (hzp[i, pl.ds(y, span), :], hzm[i, pl.ds(y, span), :])
            for i, y in ((x, row), (x - 1, row), (x + 1, row), (x, row - 1), (x, row + 1))
        ]
        diff = [a - b for a, b in cells]
        both = [a + b for a, b in cells]
        main, side = 3.0 * WEIGHT[5], 3.0 * WEIGHT[11]
        return (
            main * diff[0] + side * ((diff[1] + diff[2]) + (diff[3] + diff[4])),
            side * (diff[1] - diff[2]),
            side * (diff[3] - diff[4]),
            main * both[0] + side * ((both[1] + both[2]) + (both[3] + both[4])),
        )

    def heat_sums(columns):
        for x in columns:
            for r in range(0, sy, ROW):
                for m, value in enumerate(heat_moments(x + 1, ROW + r, ROW)):
                    hm[m, x, pl.ds(r, ROW), :] = value

    def near_heat():
        for x in range(1, sx + 3):
            for r in range(0, sy, ROW):
                shift_heat(x, ROW + r, ROW)
        for x in range(2, sx + 2):
            shift_heat(x, ROW - 2, 2)
            shift_heat(x, ROW + sy, 2)
        heat_sums(range(1, sx + 1))

    def far_heat():
        for x in (0, sx + 3):
            for r in range(0, sy, ROW):
                shift_heat(x, ROW + r, ROW)
        for x in (1, sx + 2):
            shift_heat(x, ROW - 1, 1)
            shift_heat(x, ROW + sy, 1)
        heat_sums((0, sx + 1))
        for s in (0, 1):
            for x in range(sx):
                for m, value in enumerate(heat_moments(x + 2, (ROW - 1, ROW + sy)[s], 1)):
                    hmy[m, pl.ds(s * sx + x, 1), :] = value

    def collided(tiles, fs, store):
        for x, r in tiles:
            mid = pl.ds(ROW + r, ROW)
            u = [vel[c, x + 1, mid, :] for c in range(3)]
            diff = []
            for a in range(3):
                diff.append(
                    (
                        vel[a, x + 2, mid, :] - vel[a, x, mid, :],
                        vel[a, x + 1, pl.ds(ROW + r + 1, ROW), :] - vel[a, x + 1, pl.ds(ROW + r - 1, ROW), :],
                        pltpu.roll(u[a], nz - 1, 1) - pltpu.roll(u[a], 1, 1),
                    )
                )
            own = diff[0][0] * diff[0][0] + diff[1][1] * diff[1][1] + diff[2][2] * diff[2][2]
            xy = diff[0][1] + diff[1][0]
            xz = diff[0][2] + diff[2][0]
            yz = diff[1][2] + diff[2][1]
            size = jnp.sqrt(0.5 * own + 0.25 * (xy * xy + xz * xz + yz * yz) + strain_floor)
            omega = 1.0 / (base_tau + 3.0 * smag_coef * size)
            solid = solid_s[x, pl.ds(r, ROW), :] != 0
            density = rho_s[x, pl.ds(r, ROW), :]
            still = 1.0 - 1.5 * (u[0] * u[0] + u[1] * u[1] + u[2] * u[2])
            reads = [rd[k, x, pl.ds(r, ROW), :] for k in range(19)]
            if fs is not None:
                for k in LIFTED:
                    cx, cy, cz = CS[k]
                    source = hzp if cz > 0 else hzm
                    reads[k] = reads[k] + (3.0 * WEIGHT[k] * cz) * (fs * source[x + 2 - cx, pl.ds(ROW + r - cy, ROW), :])
            scaled = {w: (w * density) * omega for w in sorted(set(WEIGHT))}
            keep = 1.0 - omega
            store(0, x, r, jnp.where(solid, reads[0], keep * reads[0] + scaled[WEIGHT[0]] * still))
            for k in range(1, 19, 2):
                other = OPP[k]
                project = None
                for c in range(3):
                    if CS[k][c]:
                        if project is None:
                            project = u[c] if CS[k][c] > 0 else -u[c]
                        else:
                            project = project + u[c] if CS[k][c] > 0 else project - u[c]
                even = still + 4.5 * project * project
                odd = 3.0 * project
                weight = scaled[WEIGHT[k]]
                store(k, x, r, jnp.where(solid, reads[other], keep * reads[k] + weight * (even + odd)))
                store(other, x, r, jnp.where(solid, reads[k], keep * reads[other] + weight * (even - odd)))

    load_h.wait()
    load_o.wait()
    load_t.wait()
    for x, r in blocks:
        rows = pl.ds(r, ROW)
        code = hl[x, rows, :]
        heat = jnp.zeros((ROW, nz), jnp.float32)
        for level in range(levels):
            heat = jnp.where(code == level, tb[level], heat)
        grid_y = gy * sy + r + row_no
        solid = (
            (ob[x, rows, :] == 1) | (grid_y == 0) | (grid_y == ngy * sy - 1) | first_lane | last_lane
        )
        solid_s[x, rows, :] = jnp.where(solid, 1, 0)
        hb[x + 2, pl.ds(ROW + r, ROW), :] = jnp.where(solid, 0.0, heat)

    load_p.wait()
    own_sums(0, blocks)
    pack_y_raw(0)
    corner_sums(0)
    pl.semaphore_wait(barrier, partners)
    if by_word:
        for s in (0, 1):

            @pl.when(has_y[s])
            def _():
                greet(in_sem, gx, y_of[s])

        for _, dy in column:
            other = lax.rem(gy + dy, ngy)

            @pl.when((other > gy + 1) | (other < gy - 1))
            def _():
                greet(col_sem, gx, other)

    sums_far, sums_near = send_x_sums(0)
    raw_far, raw_near = send_x_raw()
    neighbours = jnp.where(has_up, 1, 0) + jnp.where(has_down, 1, 0)
    raw_far()
    sums_far()
    send_y(0, raw_fields, yr_recv)
    send_y(0, sum_fields, ym_recv)
    if by_word:
        pl.semaphore_wait(in_sem, neighbours)
    send_corner_raw(0)
    send_corner_sums(0)
    if by_word:
        pl.semaphore_wait(col_sem, len(column) - neighbours)
    raw_near()
    sums_near()
    face_shares(0, (0, 1))
    edge_shares(0)
    send_heat()
    await_y_raw(0)
    await_x_raw()
    finish_peak = spread_all(0, velocity_pass(0, None))
    edge_reads()
    await_y_sums(0)

    def store_st1(k, x, r, value):
        st1[k, x, pl.ds(ROW + r, ROW), :] = value

    def faces(sides):
        for s in sides:
            await_x_sums(0, s)
            ghost_x(0, None, s)
            ghost_y(0, None)
            collided([(x, r) for x, r in blocks if x == face_x[s]], None, store_st1)
            face_shares(1, (s,))
            send_x_shares(s)

    @pl.when(gx == ngx - 1)
    def _():
        faces((1, 0))

    @pl.when(gx != ngx - 1)
    def _():
        faces((0, 1))

    collided(inner, None, store_st1)
    send_corner_raw(1)
    pack_y_raw(1)
    send_y(1, raw_fields, yr_recv)
    own_sums(1, outer)
    for part in (*send_x_sums(1), *send_x_rest()):
        part()
    own_sums(1, inner)
    send_y(1, sum_fields, ym_recv)
    corner_sums(1)
    send_corner_sums(1)
    edge_shares(1)
    await_heat()
    near_heat()
    fs = finish_peak()
    await_y_raw(1)
    await_bytes(None, xo_in, xo_recv)
    finish_peak = spread_all(1, velocity_pass(1, fs))
    for x, r in blocks:
        for c in range(3):
            out_v[c, x, pl.ds(r, ROW), :] = vel[c, x + 1, pl.ds(ROW + r, ROW), :]
    far_heat()
    await_x_rest()
    for s in (0, 1):
        for r in range(0, sy, ROW):
            face_reads(s, r, face_rest(s, r))
    edge_reads()
    await_y_sums(1)
    for s in (0, 1):
        await_x_sums(1, s)
        ghost_x(1, fs, s)
    ghost_y(1, fs)

    def store_out(k, x, r, value):
        out_p[k, x, pl.ds(r, ROW), :] = value

    collided(blocks, fs, store_out)
    await_sends()
    fs = finish_peak()
    lift = {(x, r): fs * hb[x + 2, pl.ds(ROW + r, ROW), :] for x, r in blocks}
    for k in LIFTED:
        for x, r in blocks:
            rows = pl.ds(r, ROW)
            out_p[k, x, rows, :] = out_p[k, x, rows, :] + (3.0 * WEIGHT[k] * CS[k][2]) * lift[(x, r)]


def write_out(pops, vel, out_p, out_v, sems):
    copies = [
        pltpu.make_async_copy(pops, out_p, sems.at[0]),
        pltpu.make_async_copy(vel, out_v, sems.at[1]),
    ]
    for copy in copies:
        copy.start()
    for copy in copies:
        copy.wait()


def local(populations, heat_level, obstacle, heat_table):
    ngx = lax.axis_size("gx")
    ngy = lax.axis_size("gy")
    _, sx, sy, nz = populations.shape
    f32 = jnp.float32
    tall = sy + 2 * ROW
    dma = pltpu.SemaphoreType.DMA
    groups = peak_groups(ngx, ngy)
    phases = len(groups)
    vmem = pl.BlockSpec(memory_space=pltpu.VMEM)
    anywhere = pl.BlockSpec(memory_space=pltpu.HBM)
    shapes = (
        jax.ShapeDtypeStruct(populations.shape, f32),
        jax.ShapeDtypeStruct((3, sx, sy, nz), f32),
    )

    def floats(*shape):
        return pltpu.VMEM(shape, f32)

    def ints(*shape):
        return pltpu.VMEM(shape, jnp.int32)

    pops, velocity = pl.pallas_call(
        functools.partial(kernel, ngx, ngy),
        out_shape=shapes,
        in_specs=[anywhere] * 4,
        out_specs=[vmem] * 2,
        scratch_shapes=[
            floats(19, sx, tall, nz),
            floats(19, sx, tall, nz),
            floats(19, sx, sy, nz),
            floats(4, sx, sy, nz),
            floats(sx, sy, nz),
            floats(3, sx + 2, tall, nz),
            ints(sx, sy, nz),
            ints(sx, sy, nz),
            pltpu.SMEM(heat_table.shape, f32),
            ints(sx, sy, nz),
            floats(sx + 4, tall, nz),
            floats(sx + 4, tall, nz),
            floats(sx + 4, tall, nz),
            floats(4, sx + 2, sy, nz),
            floats(4, 2 * sx, nz),
            floats(2, 5, tall, nz),
            floats(STEPS, 2, 4, sy, nz),
            floats(STEPS, 2, 4, sy, nz),
            floats(STEPS, 9, 2 * sx, nz),
            floats(STEPS, 9, 2 * sx, nz),
            floats(8, ROW, nz),
            floats(STEPS, 6, ROW, nz),
            floats(STEPS, ROW, nz),
            floats(STEPS, 6, ROW, nz),
            floats(2, 3, sy, nz),
            floats(2, 2 * sy + ROW, nz),
            floats(2, 3, sy, nz),
            floats(2, 2 * sy + ROW, nz),
            floats(4, 2 * sx, nz),
            floats(5, 2 * sx, nz),
            floats(4, 2 * sx, nz),
            floats(2, ROW, nz),
            floats(4, ROW, nz),
            floats(4, 2 * sx, nz),
            floats(2, sy, nz),
            floats(2 * sx, nz),
            floats(8 * ROW, nz),
            floats(STEPS, phases, 1, nz),
            *[floats(STEPS, -(-len(group) // ROW) * ROW, nz) for group in groups],
            dma((4,)),
            pltpu.SemaphoreType.REGULAR,
            pltpu.SemaphoreType.REGULAR,
            dma,
            dma((2,)),
            dma((STEPS,)),
            dma((STEPS, 2)),
            dma,
            dma((STEPS, 2)),
            dma((STEPS, 2)),
            dma((STEPS, 4)),
            dma,
            dma((2,)),
            dma((phases,)),
            dma((STEPS, phases)),
        ],
        compiler_params=pltpu.CompilerParams(
            collective_id=0, has_side_effects=True, vmem_limit_bytes=24 * 1024 * 1024
        ),
        name="lattice_steps",
    )(*[pltpu.with_memory_space_constraint(a, pltpu.HBM) for a in (populations, heat_level, obstacle, heat_table)])
    return pl.pallas_call(
        write_out,
        out_shape=shapes,
        in_specs=[vmem] * 2,
        out_specs=[anywhere] * 2,
        scratch_shapes=[dma((2,))],
        compiler_params=pltpu.CompilerParams(vmem_limit_bytes=8 * 1024 * 1024),
        name="write_out",
    )(pops, velocity)


def solution(mesh):
    return jax.shard_map(
        local,
        mesh=mesh,
        in_specs=(
            P(None, ("member", "gx"), "gy", None),
            P(("member", "gx"), "gy", None),
            P(("member", "gx"), "gy", None),
            P(),
        ),
        out_specs=(P(None, ("member", "gx"), "gy", None), P(None, ("member", "gx"), "gy", None)),
        check_vma=False,
    )
```

```python
import functools

import jax
import jax.numpy as jnp
import numpy as np
from jax import lax
from jax.experimental import pallas as pl
from jax.experimental.pallas import tpu as pltpu
from jax.sharding import PartitionSpec as P

STEPS = 2
ROW = 8

lattice = np.array(
    [
        [0, 0, 0],
        [1, 0, 0],
        [-1, 0, 0],
        [0, 1, 0],
        [0, -1, 0],
        [0, 0, 1],
        [0, 0, -1],
        [1, 1, 0],
        [-1, -1, 0],
        [1, -1, 0],
        [-1, 1, 0],
        [1, 0, 1],
        [-1, 0, -1],
        [1, 0, -1],
        [-1, 0, 1],
        [0, 1, 1],
        [0, -1, -1],
        [0, 1, -1],
        [0, -1, 1],
    ]
)
CS = [tuple(int(c) for c in row) for row in lattice]
NUMBER = {c: k for k, c in enumerate(CS)}
WEIGHT = [1.0 / 3.0] + [1.0 / 18.0] * 6 + [1.0 / 36.0] * 12
OPP = [0, 2, 1, 4, 3, 6, 5, 8, 7, 10, 9, 12, 11, 14, 13, 16, 15, 18, 17]
base_tau = 0.52
smag_coef = 0.04
speed_cap = 0.1
strain_floor = 1e-06
LIFTED = [k for k in range(19) if CS[k][2] != 0]
ACROSS_X = {c: [NUMBER[(c, 0, 0)], NUMBER[(c, 1, 0)], NUMBER[(c, -1, 0)], NUMBER[(c, 0, 1)], NUMBER[(c, 0, -1)]] for c in (1, -1)}
ACROSS_Y = {c: [NUMBER[(0, c, 0)], NUMBER[(1, c, 0)], NUMBER[(-1, c, 0)], NUMBER[(0, c, 1)], NUMBER[(0, c, -1)]] for c in (1, -1)}
OUT = (-1, 1)
IN = (1, -1)


def tree_sum(items):
    items = list(items)
    while len(items) > 1:
        items = [items[i] + items[i + 1] if i + 1 < len(items) else items[i] for i in range(0, len(items), 2)]
    return items[0]


def peak_groups(ngx, ngy):
    if ngx * ngy <= 64:
        return [[(dx, dy) for dx in range(ngx) for dy in range(ngy) if dx or dy]]
    return [[(0, dy) for dy in range(1, ngy)], [(dx, 0) for dx in range(1, ngx)]]


def kernel(
    ngx, ngy,
    pops, heat_level, obstacle, table,
    out_p, out_v,
    st0, st1, rd, ms, rho_s, vel, hl, ob, tb, solid_s,
    hb, hzp, hzm, hm, hmy,
    xr, xp, xm_out, xm_in, yb_out, yb_in, cg, cm_out, cr_in, cm_in,
    ox, ox2, xo_in, x2_in, oy, dr, dm, tu, ex, ey, gfx, gfy, flat, pm_src, *rest,
):
    (*pm_bufs, load_sem, in_sem, col_sem, x_send, y_send, xr_recv, xm_recv, xo_recv, yr_recv, ym_recv,
     cm_recv, hx_recv, hy_recv, p_send, p_recv) = rest
    _, sx, sy, nz = pops.shape
    levels = table.shape[0]
    gx = lax.axis_index("gx")
    gy = lax.axis_index("gy")
    has_up = gy < ngy - 1
    has_down = gy > 0
    right = lax.rem(gx + 1, ngx)
    left = lax.rem(gx + ngx - 1, ngx)
    own_y = pl.ds(ROW, sy)
    face_x = (0, sx - 1)
    edge_y = (0, sy - 1)
    x_of = (left, right)
    y_of = (gy - 1, gy + 1)
    has_y = (has_down, has_up)

    barrier = pltpu.get_barrier_semaphore()

    def greet(sem, x, y):
        pl.semaphore_signal(sem, inc=1, device_id={"gx": x, "gy": y}, device_id_type=pl.DeviceIdType.MESH)

    groups = peak_groups(ngx, ngy)
    beside = sorted({1, ngx - 1} - {0})
    column = [(0, dy) for dy in range(1, ngy)]
    by_word = len(groups) == 1 and ngx <= 5
    greeted = [(dx, 0) for dx in beside] + column if by_word else [place for group in groups for place in group]
    partners = len(greeted)
    for dx, dy in greeted:
        greet(barrier, lax.rem(gx + dx, ngx), lax.rem(gy + dy, ngy))
    if len(groups) > 1:
        partners = partners + 2 * (jnp.where(has_up, 1, 0) + jnp.where(has_down, 1, 0))
        for s in (0, 1):

            @pl.when(has_y[s])
            def _():
                greet(barrier, right, y_of[s])
                greet(barrier, left, y_of[s])

    load_p = pltpu.make_async_copy(pops, st0.at[:, :, own_y, :], load_sem.at[0])
    load_h = pltpu.make_async_copy(heat_level, hl, load_sem.at[1])
    load_o = pltpu.make_async_copy(obstacle, ob, load_sem.at[2])
    load_t = pltpu.make_async_copy(table, tb, load_sem.at[3])
    load_p.start()
    load_h.start()
    load_o.start()
    load_t.start()

    def zeros(ref, *index):
        part = ref.at[index]
        part[...] = jnp.zeros(part.shape, jnp.float32)

    every = slice(None)
    for row in (ROW - 1, ROW + sy):
        for st in (st0, st1):
            for c in (1, -1):
                for k in ACROSS_Y[c]:
                    zeros(st, k, every, pl.ds(row, 1), every)
        zeros(xr, every, every, pl.ds(row, 1), every)
    for ref in (cg, tu, ey):
        ref[...] = jnp.zeros(ref.shape, jnp.float32)

    for s in (0, 1):

        @pl.when(jnp.logical_not(has_y[s]))
        def _():
            zeros(yb_in, every, every, pl.ds(s * sx, sx), every)
            for xs in (0, 1):
                zeros(cr_in, every, pl.ds(xs * 2 + s, 1), every)
                zeros(cm_in, every, every, pl.ds(xs * 2 + s, 1), every)
            zeros(hb, every, pl.ds((ROW - 2, ROW + sy)[s], 2), every)

    def guarded(cond, fn):
        if cond is None:
            fn()
        else:
            pl.when(cond)(fn)

    def send(cond, pairs, send_sem, recv_sem, x, y):
        def go():
            for src, dst in pairs:
                pltpu.make_async_remote_copy(
                    src_ref=src, dst_ref=dst, send_sem=send_sem, recv_sem=recv_sem,
                    device_id={"gx": x, "gy": y}, device_id_type=pl.DeviceIdType.MESH,
                ).start()

        guarded(cond, go)

    def await_bytes(cond, view, sem):
        guarded(cond, lambda: pltpu.make_async_copy(view, view, sem).wait())

    states = (st0, st1)
    corners = [(xs, ys) for xs in (0, 1) for ys in (0, 1)]
    raw_fields = pl.ds(0, 5)
    sum_fields = pl.ds(5, 4)

    at_end = (gx == 0, gx == ngx - 1)

    def along_x(pairs_of, sem_of):
        def far():
            for s in (0, 1):
                send(at_end[s], pairs_of(s), x_send, sem_of(s), x_of[s], gy)

        def near():
            for s in (0, 1):
                send(jnp.logical_not(at_end[s]), pairs_of(s), x_send, sem_of(s), x_of[s], gy)

        return far, near

    def send_x_raw():
        return along_x(
            lambda s: [(xp.at[s], xr.at[1 - s, :, own_y, :])],
            lambda s: xr_recv.at[0],
        )

    def send_x_sums(step):
        return along_x(lambda s: [(xm_out.at[step, s], xm_in.at[step, 1 - s])], lambda s: xm_recv.at[step, 1 - s])

    rest_rows = pl.ds(0, 2 * sy + 2)

    def send_x_shares(s):
        send(None, [(ox.at[s], xo_in.at[1 - s])], x_send, xo_recv, x_of[s], gy)

    def send_x_rest():
        return along_x(lambda s: [(ox2.at[s, rest_rows, :], x2_in.at[1 - s, rest_rows, :])], lambda s: xr_recv.at[1])

    def send_heat_x(layer):
        src, dst = ((2, sx + 1), (sx + 2, 1)) if layer == 0 else ((3, sx), (sx + 3, 0))
        for s in (0, 1):
            send(None, [(hb.at[src[s], own_y, :], hb.at[dst[s], own_y, :])], x_send, hx_recv.at[layer], x_of[s], gy)

    def send_heat():
        send_heat_x(0)
        for s in (0, 1):
            src = hb.at[pl.ds(2, sx), pl.ds((ROW, ROW + sy - 2)[s], 2), :]
            dst = hb.at[pl.ds(2, sx), pl.ds((ROW + sy, ROW - 2)[s], 2), :]
            send(has_y[s], [(src, dst)], y_send.at[s], hy_recv.at[1 - s], gx, y_of[s])
        to_corners(
            lambda c, xs, ys: (
                hb.at[2 + face_x[xs], pl.ds(ROW + edge_y[ys], 1), :],
                hb.at[(sx + 2, 1)[xs], pl.ds((ROW + sy, ROW - 1)[ys], 1), :],
            ),
            lambda c: hy_recv.at[c % 2],
        )

    def send_y(step, fields, recv_sem):
        for s in (0, 1):
            src = yb_out.at[step, fields, pl.ds(s * sx, sx), :]
            dst = yb_in.at[step, fields, pl.ds((1 - s) * sx, sx), :]
            send(has_y[s], [(src, dst)], y_send.at[s], recv_sem.at[step, 1 - s], gx, y_of[s])

    def to_corners(pair_of, sem_of):
        for c, (xs, ys) in enumerate(corners):
            send(has_y[ys], [pair_of(c, xs, ys)], y_send.at[ys], sem_of(3 - c), x_of[xs], y_of[ys])

    def send_corner_raw(step):
        st = states[step]

        def pair(c, xs, ys):
            k = NUMBER[(OUT[xs], OUT[ys], 0)]
            return st.at[k, face_x[xs], pl.ds(ROW + edge_y[ys], 1), :], cr_in.at[step, pl.ds(3 - c, 1), :]

        to_corners(pair, lambda c: yr_recv.at[step, c % 2])

    def send_corner_sums(step):
        to_corners(
            lambda c, xs, ys: (cm_out.at[step, :, pl.ds(c, 1), :], cm_in.at[step, :, pl.ds(3 - c, 1), :]),
            lambda c: cm_recv.at[step, c],
        )

    def await_y_raw(step):
        for s in (0, 1):
            await_bytes(has_y[s], flat.at[pl.ds(0, 5 * sx + 2), :], yr_recv.at[step, s])

    def await_x_raw():
        await_bytes(None, xr.at[:, :, own_y, :], xr_recv.at[0])

    def await_x_rest():
        await_bytes(None, x2_in.at[:, rest_rows, :], xr_recv.at[1])

    def await_y_sums(step):
        for s in (0, 1):
            await_bytes(has_y[s], yb_in.at[step, sum_fields, pl.ds(s * sx, sx), :], ym_recv.at[step, s])

    def await_x_sums(step, s):
        for ys in (0, 1):
            await_bytes(has_y[ys], cm_in.at[step, :, pl.ds(2 * s + ys, 1), :], cm_recv.at[step, 2 * s + ys])
        await_bytes(None, xm_in.at[step, s], xm_recv.at[step, s])

    def await_heat():
        for s in (0, 1):
            await_bytes(has_y[s], flat.at[pl.ds(0, 2 * sx + 2), :], hy_recv.at[s])
        await_bytes(None, hb.at[pl.ds(0, 2), own_y, :], hx_recv.at[0])

    def await_sends():
        for view in (xp, xm_out, ox, ox2.at[:, rest_rows, :], hb.at[pl.ds(0, 4), own_y, :]):
            await_bytes(None, view, x_send)
        for s in (0, 1):
            for view in (yb_out.at[:, :, pl.ds(0, sx), :], flat.at[pl.ds(0, 2 * sx + STEPS * 14 + 2), :]):
                await_bytes(has_y[s], view, y_send.at[s])
        for phase, group in enumerate(groups):
            for step in range(STEPS):
                await_bytes(None, pm_bufs[phase].at[step, pl.ds(0, len(group)), :], p_send.at[phase])

    def spread(step, phase, value):
        group = peak_groups(ngx, ngy)[phase]
        count = len(group)
        buf = pm_bufs[phase]
        pm_src[step, phase] = value
        for d, (dx, dy) in sorted(enumerate(group, 1), key=lambda item: item[1][0] in (0, ngx // 2)):
            place = {"gx": lax.rem(gx + dx, ngx), "gy": lax.rem(gy + dy, ngy)}
            pltpu.make_async_remote_copy(
                src_ref=pm_src.at[step, phase],
                dst_ref=buf.at[step, pl.ds(d - 1, 1), :],
                send_sem=p_send.at[phase],
                recv_sem=p_recv.at[step, phase],
                device_id=place,
                device_id_type=pl.DeviceIdType.MESH,
            ).start()
        view = buf.at[step, pl.ds(0, count), :]

        def wait():
            await_bytes(None, view, p_recv.at[step, phase])
            return jnp.maximum(value, jnp.max(buf[step, pl.ds(0, count), :], axis=0, keepdims=True))

        return wait

    def spread_all(step, tile):
        wait = spread(step, 0, jnp.max(tile, axis=0, keepdims=True))

        def finish():
            best = wait()
            for phase in range(1, len(pm_bufs)):
                best = spread(step, phase, best)()
            peak = jnp.broadcast_to(jnp.max(best, axis=1, keepdims=True), (ROW, nz))
            return speed_cap * lax.rsqrt(speed_cap * speed_cap + peak)

        return finish

    blocks = [(x, r) for x in range(sx) for r in range(0, sy, ROW)]
    outer = [(x, r) for x, r in blocks if x in face_x]
    inner = [(x, r) for x, r in blocks if x not in face_x]
    lane = lax.broadcasted_iota(jnp.int32, (ROW, nz), 1)
    row_no = lax.broadcasted_iota(jnp.int32, (ROW, nz), 0)
    first_lane = lane == 0
    last_lane = lane == nz - 1
    edge_row = (row_no == 0, row_no == ROW - 1)
    pack_row = lax.broadcasted_iota(jnp.int32, (2 * sx, nz), 0)
    pack_sign = jnp.where(pack_row < sx, 1.0, -1.0)
    corner_x = jnp.where(row_no < 2, 1.0, -1.0)
    corner_y = jnp.where(lax.rem(row_no, 2) == 0, 1.0, -1.0)

    def shift_z(cells, cz):
        if not cz:
            return cells
        at = lax.broadcasted_iota(jnp.int32, cells.shape, 1)
        return jnp.where(at == (0 if cz > 0 else nz - 1), 0.0, pltpu.roll(cells, cz % nz, 1))

    def edges_of(r):
        return [s for s in (0, 1) if r == (0, sy - ROW)[s]]

    def own_sums(step, tiles):
        st = states[step]
        for x, r in tiles:
            rows = pl.ds(r, ROW)
            reads = {}
            for k, (cx, cy, cz) in enumerate(CS):
                if 0 <= x - cx < sx:
                    reads[k] = shift_z(st[k, x - cx, pl.ds(ROW + r - cy, ROW), :], cz)
                    rd[k, x, rows, :] = reads[k]
            sums = [tree_sum(list(reads.values()))]
            for c in range(3):
                plus = [reads[k] for k in reads if CS[k][c] > 0]
                minus = [reads[k] for k in reads if CS[k][c] < 0]
                if plus and minus:
                    sums.append(tree_sum(plus) - tree_sum(minus))
                else:
                    sums.append(tree_sum(plus) if plus else -tree_sum(minus))
            for m in range(4):
                ms[m, x, rows, :] = sums[m]
            sums[0] = jnp.where(solid_s[x, rows, :] != 0, 0.0, sums[0])
            for s in (0, 1):
                if x == face_x[s]:
                    for m in range(4):
                        xm_out[step, s, m, rows, :] = sums[m]
                if s in edges_of(r):
                    at = (0, ROW - 1)[s]
                    for m in range(4):
                        yb_out[step, 5 + m, pl.ds(s * sx + x, 1), :] = sums[m][at : at + 1, :]

    def pack_x_raw():
        for s in (0, 1):
            for j, k in enumerate(ACROSS_X[OUT[s]]):
                xp[s, j] = st0[k, face_x[s], own_y, :]

    def pack_y_raw(step):
        st = states[step]
        for s in (0, 1):
            for j, k in enumerate(ACROSS_Y[OUT[s]]):
                for x in range(sx):
                    yb_out[step, j, pl.ds(s * sx + x, 1), :] = st[k, x, pl.ds(ROW + edge_y[s], 1), :]

    def corner_sums(step):
        st = states[step]
        for c, (xs, ys) in enumerate(corners):
            dx, dy = OUT[xs], OUT[ys]
            fx, fy = face_x[xs], edge_y[ys]
            places = [
                ((0, dy, 0), fx, fy), ((0, dy, 1), fx, fy), ((0, dy, -1), fx, fy), ((dx, dy, 0), fx - dx, fy),
                ((dx, 0, 0), fx, fy), ((dx, 0, 1), fx, fy), ((dx, 0, -1), fx, fy), ((dx, dy, 0), fx, fy - dy),
            ]
            for f, (direction, x, y) in enumerate(places):
                cg[f, pl.ds(c, 1), :] = st[NUMBER[direction], x, pl.ds(ROW + y, 1), :]
        for half, sign in ((0, -corner_x), (1, -corner_y)):
            a, b, d, e = (cg[4 * half + f] for f in range(4))
            b, d = shift_z(b, 1), shift_z(d, -1)
            cm_out[step, 3 * half + 0] = (a + b) + (d + e)
            cm_out[step, 3 * half + 1] = sign * e
            cm_out[step, 3 * half + 2] = b - d

    def packed(fields, fill):
        plus = jnp.where(lax.rem(pack_row, sx) == 0, 0.0, pltpu.roll(fields[1], 1, 0))
        minus = jnp.where(lax.rem(pack_row, sx) == sx - 1, 0.0, pltpu.roll(fields[2], 2 * sx - 1, 0))
        if fill is not None:
            for ys in (0, 1):
                plus = jnp.where(pack_row == ys * sx, fill(ys), plus)
                minus = jnp.where(pack_row == ys * sx + sx - 1, fill(2 + ys), minus)
        return [fields[0], plus, minus, shift_z(fields[3], 1), shift_z(fields[4], -1)]

    def face_shares(step, sides):
        st = states[step]
        for s in sides:
            for r in range(0, sy, ROW):
                ks = ACROSS_X[OUT[s]]
                a, b, c, d, e = (st[k, face_x[s], pl.ds(ROW + r - CS[k][1], ROW), :] for k in ks)
                d, e = shift_z(d, 1), shift_z(e, -1)
                ox[s, 0, pl.ds(r, ROW), :] = ((a + b) + (c + d)) + e
                ox[s, 1, pl.ds(r, ROW), :] = b - c
                ox[s, 2, pl.ds(r, ROW), :] = d - e
                if step == 1:
                    ox2[s, pl.ds(r, ROW), :] = b
                    ox2[s, pl.ds(sy + r, ROW), :] = d
            if step == 1:
                ox2[s, pl.ds(2 * sy, 1), :] = st[ACROSS_X[OUT[s]][2], face_x[s], pl.ds(ROW, 1), :]
                ox2[s, pl.ds(2 * sy + 1, 1), :] = st[ACROSS_X[OUT[s]][1], face_x[s], pl.ds(ROW + sy - 1, 1), :]

    def edge_shares(step):
        a, b, c, d, e = packed([yb_out[step, j] for j in range(5)], None)
        total = ((a + b) + (c + d)) + e
        oy[0] = total
        oy[1] = b - c
        oy[2] = -pack_sign * total
        oy[3] = d - e

    def edge_moments(step):
        fields = packed([yb_in[step, j] for j in range(5)], lambda c: cr_in[step, pl.ds(c, 1), :])
        for j in range(5):
            dr[j] = fields[j]
        a, b, c, d, e = fields
        total = ((a + b) + (c + d)) + e
        for m, value in enumerate((total, b - c, pack_sign * total, d - e)):
            dm[m] = value

    def velocity_pass(step, fs, tiles, peak):
        for x, r in tiles:
            rows = pl.ds(r, ROW)
            sums = [ms[m, x, rows, :] for m in range(4)]
            for s in (0, 1):
                if x == face_x[s]:
                    if step == 0:
                        parts = face_raw(s, r)
                        shares = tree_sum(parts), parts[1] - parts[2], parts[3] - parts[4]
                        face_reads(s, r, parts)
                    else:
                        shares = [xo_in[s, m, rows, :] for m in range(3)]
                    sums[0] = sums[0] + shares[0]
                    sums[1] = sums[1] + shares[0] if s == 0 else sums[1] - shares[0]
                    sums[2] = sums[2] + shares[1]
                    sums[3] = sums[3] + shares[2]
            for s in edges_of(r):
                for m in range(4):
                    sums[m] = sums[m] + jnp.where(edge_row[s], dm[m, pl.ds(s * sx + x, 1), :], 0.0)
            if fs is not None:
                sums = [sums[m] + fs * hm[m, x + 1, rows, :] for m in range(4)]
            solid = solid_s[x, rows, :] != 0
            inv = jnp.where(solid, 0.0, 1.0 / jnp.where(solid, 1.0, sums[0]))
            rho_s[x, rows, :] = sums[0]
            speed = []
            for c in range(3):
                u = sums[1 + c] * inv
                vel[c, x + 1, pl.ds(ROW + r, ROW), :] = u
                speed.append(u * u)
            peak = jnp.maximum(peak, speed[0] + speed[1] + speed[2])
        return peak

    def face_raw(s, r):
        return [
            shift_z(xr[s, j, pl.ds(ROW + r - CS[k][1], ROW), :], CS[k][2]) for j, k in enumerate(ACROSS_X[IN[s]])
        ]

    def face_rest(s, r):
        total, along, height = (xo_in[s, m, pl.ds(r, ROW), :] for m in range(3))
        b, d = x2_in[s, pl.ds(r, ROW), :], x2_in[s, pl.ds(sy + r, ROW), :]
        c, e = b - along, d - height
        return [total - ((b + c) + (d + e)), b, c, d, e]

    def face_reads(s, r, parts):
        for k, part in zip(ACROSS_X[IN[s]], parts):
            rd[k, face_x[s], pl.ds(r, ROW), :] = part

    def edge_reads():
        for s in (0, 1):
            for j, k in enumerate(ACROSS_Y[IN[s]]):
                for x in range(sx):
                    rd[k, x, pl.ds(edge_y[s], 1), :] = dr[j, pl.ds(s * sx + x, 1), :]

    def ghost_x(step, fs, s):
        own = pl.ds(2 * s, 2)
        for ys in (0, 1):
            c = 2 * s + ys
            j = 1 if OUT[s] > 0 else 2
            tu[0, pl.ds(c, 1), :] = yb_in[step, j, pl.ds(ys * sx + face_x[s], 1), :]
            j = 1 if OUT[ys] > 0 else 2
            if step == 0:
                tu[1, pl.ds(c, 1), :] = xr[s, j, pl.ds(ROW + edge_y[ys], 1), :]
            else:
                tu[1, pl.ds(c, 1), :] = x2_in[s, pl.ds(2 * sy + ys, 1), :]
        sums = [cm_in[step, m, own, :] for m in range(6)]
        over, up = tu[0, own, :], tu[1, own, :]
        sign = jnp.where(lax.broadcasted_iota(jnp.int32, (2, nz), 0) == 0, 1.0, -1.0)
        total = sums[0] + over
        for m, value in enumerate((total, sums[1] + OUT[s] * over, sign * total, sums[2])):
            ex[m, own, :] = value
        total = sums[3] + up
        for m, value in enumerate((total, IN[s] * total, sums[4] - sign * up, sums[5])):
            for ys in (0, 1):
                ey[m, pl.ds(ys * sx + face_x[s], 1), :] = value[ys : ys + 1, :]
        for r in range(0, sy, ROW):
            rows = pl.ds(r, ROW)
            share = ox[s, 0, rows, :]
            sums = [xm_in[step, s, m, rows, :] for m in range(4)]
            if step == 0:
                gfx[s, rows, :] = sums[0]
            fluid = gfx[s, rows, :] > 0.0
            sums[0] = sums[0] + share
            sums[1] = sums[1] - share if s == 0 else sums[1] + share
            sums[2] = sums[2] + ox[s, 1, rows, :]
            sums[3] = sums[3] + ox[s, 2, rows, :]
            for ys in edges_of(r):
                for m in range(4):
                    sums[m] = sums[m] + jnp.where(edge_row[ys], ex[m, pl.ds(s * 2 + ys, 1), :], 0.0)
            at = (0, sx + 1)[s]
            if fs is not None:
                sums = [sums[m] + fs * hm[m, at, rows, :] for m in range(4)]
            inv = jnp.where(fluid, 1.0 / jnp.where(fluid, sums[0], 1.0), 0.0)
            for c in range(3):
                vel[c, at, pl.ds(ROW + r, ROW), :] = sums[1 + c] * inv

    def ghost_y(step, fs):
        sums = [yb_in[step, 5 + m] for m in range(4)]
        if step == 0:
            gfy[...] = sums[0]
        fluid = gfy[...] > 0.0
        sums = [sums[m] + oy[m] + ey[m] for m in range(4)]
        if fs is not None:
            sums = [sums[m] + fs[0:1, :] * hmy[m] for m in range(4)]
        inv = jnp.where(fluid, 1.0 / jnp.where(fluid, sums[0], 1.0), 0.0)
        for c in range(3):
            u = sums[1 + c] * inv
            for s in (0, 1):
                for x in range(sx):
                    at = s * sx + x
                    vel[c, x + 1, pl.ds((ROW - 1, ROW + sy)[s], 1), :] = u[at : at + 1, :]

    def shift_heat(x, row, span):
        cells = hb[x, pl.ds(row, span), :]
        hzp[x, pl.ds(row, span), :] = shift_z(cells, 1)
        hzm[x, pl.ds(row, span), :] = shift_z(cells, -1)

    def heat_moments(x, row, span):
        cells = [
            (hzp[i, pl.ds(y, span), :], hzm[i, pl.ds(y, span), :])
            for i, y in ((x, row), (x - 1, row), (x + 1, row), (x, row - 1), (x, row + 1))
        ]
        diff = [a - b for a, b in cells]
        both = [a + b for a, b in cells]
        main, side = 3.0 * WEIGHT[5], 3.0 * WEIGHT[11]
        return (
            main * diff[0] + side * ((diff[1] + diff[2]) + (diff[3] + diff[4])),
            side * (diff[1] - diff[2]),
            side * (diff[3] - diff[4]),
            main * both[0] + side * ((both[1] + both[2]) + (both[3] + both[4])),
        )

    def heat_sums(columns):
        for x in columns:
            for r in range(0, sy, ROW):
                for m, value in enumerate(heat_moments(x + 1, ROW + r, ROW)):
                    hm[m, x, pl.ds(r, ROW), :] = value

    def near_heat():
        for x in range(1, sx + 3):
            for r in range(0, sy, ROW):
                shift_heat(x, ROW + r, ROW)
        for x in range(2, sx + 2):
            shift_heat(x, ROW - 2, 2)
            shift_heat(x, ROW + sy, 2)
        heat_sums(range(1, sx + 1))

    def far_heat():
        for x in (0, sx + 3):
            for r in range(0, sy, ROW):
                shift_heat(x, ROW + r, ROW)
        for x in (1, sx + 2):
            shift_heat(x, ROW - 1, 1)
            shift_heat(x, ROW + sy, 1)
        heat_sums((0, sx + 1))
        for s in (0, 1):
            for x in range(sx):
                for m, value in enumerate(heat_moments(x + 2, (ROW - 1, ROW + sy)[s], 1)):
                    hmy[m, pl.ds(s * sx + x, 1), :] = value

    def collided(tiles, fs, store):
        for x, r in tiles:
            mid = pl.ds(ROW + r, ROW)
            u = [vel[c, x + 1, mid, :] for c in range(3)]
            diff = []
            for a in range(3):
                diff.append(
                    (
                        vel[a, x + 2, mid, :] - vel[a, x, mid, :],
                        vel[a, x + 1, pl.ds(ROW + r + 1, ROW), :] - vel[a, x + 1, pl.ds(ROW + r - 1, ROW), :],
                        pltpu.roll(u[a], nz - 1, 1) - pltpu.roll(u[a], 1, 1),
                    )
                )
            own = diff[0][0] * diff[0][0] + diff[1][1] * diff[1][1] + diff[2][2] * diff[2][2]
            xy = diff[0][1] + diff[1][0]
            xz = diff[0][2] + diff[2][0]
            yz = diff[1][2] + diff[2][1]
            size = jnp.sqrt(0.5 * own + 0.25 * (xy * xy + xz * xz + yz * yz) + strain_floor)
            omega = 1.0 / (base_tau + 3.0 * smag_coef * size)
            solid = solid_s[x, pl.ds(r, ROW), :] != 0
            density = rho_s[x, pl.ds(r, ROW), :]
            still = 1.0 - 1.5 * (u[0] * u[0] + u[1] * u[1] + u[2] * u[2])
            reads = [rd[k, x, pl.ds(r, ROW), :] for k in range(19)]
            if fs is not None:
                for k in LIFTED:
                    cx, cy, cz = CS[k]
                    source = hzp if cz > 0 else hzm
                    reads[k] = reads[k] + (3.0 * WEIGHT[k] * cz) * (fs * source[x + 2 - cx, pl.ds(ROW + r - cy, ROW), :])
            scaled = {w: (w * density) * omega for w in sorted(set(WEIGHT))}
            keep = 1.0 - omega
            store(0, x, r, jnp.where(solid, reads[0], keep * reads[0] + scaled[WEIGHT[0]] * still))
            for k in range(1, 19, 2):
                other = OPP[k]
                project = None
                for c in range(3):
                    if CS[k][c]:
                        if project is None:
                            project = u[c] if CS[k][c] > 0 else -u[c]
                        else:
                            project = project + u[c] if CS[k][c] > 0 else project - u[c]
                even = still + 4.5 * project * project
                odd = 3.0 * project
                weight = scaled[WEIGHT[k]]
                store(k, x, r, jnp.where(solid, reads[other], keep * reads[k] + weight * (even + odd)))
                store(other, x, r, jnp.where(solid, reads[k], keep * reads[other] + weight * (even - odd)))

    load_h.wait()
    load_o.wait()
    load_t.wait()
    for x, r in blocks:
        rows = pl.ds(r, ROW)
        code = hl[x, rows, :]
        heat = jnp.zeros((ROW, nz), jnp.float32)
        for level in range(levels):
            heat = jnp.where(code == level, tb[level], heat)
        grid_y = gy * sy + r + row_no
        solid = (
            (ob[x, rows, :] == 1) | (grid_y == 0) | (grid_y == ngy * sy - 1) | first_lane | last_lane
        )
        solid_s[x, rows, :] = jnp.where(solid, 1, 0)
        hb[x + 2, pl.ds(ROW + r, ROW), :] = jnp.where(solid, 0.0, heat)

    neighbours = jnp.where(has_up, 1, 0) + jnp.where(has_down, 1, 0)
    sums_far, sums_near = send_x_sums(0)
    raw_far, raw_near = send_x_raw()
    neighbours = jnp.where(has_up, 1, 0) + jnp.where(has_down, 1, 0)
    sums_far, sums_near = send_x_sums(0)
    raw_far, raw_near = send_x_raw()
    load_p.wait()
    pack_x_raw()
    pl.semaphore_wait(barrier, partners)
    if by_word:
        for s in (0, 1):

            @pl.when(has_y[s])
            def _():
                greet(in_sem, gx, y_of[s])

    raw_far()
    own_sums(0, outer)
    sums_far()
    if by_word:
        for _, dy in column:
            other = lax.rem(gy + dy, ngy)

            @pl.when((other > gy + 1) | (other < gy - 1))
            def _():
                greet(col_sem, gx, other)

    pack_y_raw(0)
    send_y(0, raw_fields, yr_recv)
    corner_sums(0)
    own_sums(0, inner)
    send_y(0, sum_fields, ym_recv)
    if by_word:
        pl.semaphore_wait(in_sem, neighbours)
    send_corner_raw(0)
    send_corner_sums(0)
    if by_word:
        pl.semaphore_wait(col_sem, len(column) - neighbours)
    raw_near()
    sums_near()
    face_shares(0, (0, 1))
    edge_shares(0)
    send_heat()
    no_peak = jnp.zeros((ROW, nz), jnp.float32)
    await_y_raw(0)
    edge_moments(0)
    peak = velocity_pass(0, None, inner, no_peak)
    await_x_raw()
    finish_peak = spread_all(0, velocity_pass(0, None, outer, peak))
    edge_reads()
    await_y_sums(0)

    def store_st1(k, x, r, value):
        st1[k, x, pl.ds(ROW + r, ROW), :] = value

    def face(s):
        await_x_sums(0, s)
        ghost_x(0, None, s)
        ghost_y(0, None)
        collided([(x, r) for x, r in blocks if x == face_x[s]], None, store_st1)
        face_shares(1, (s,))
        send_x_shares(s)

    @pl.when(gx == ngx - 1)
    def _():
        face(1)
        face(0)

    @pl.when(gx != ngx - 1)
    def _():
        face(0)
        face(1)

    collided(inner, None, store_st1)
    send_corner_raw(1)
    pack_y_raw(1)
    send_y(1, raw_fields, yr_recv)
    own_sums(1, outer)
    for part in (*send_x_sums(1), *send_x_rest()):
        part()
    own_sums(1, inner)
    send_y(1, sum_fields, ym_recv)
    corner_sums(1)
    send_corner_sums(1)
    send_heat_x(1)
    edge_shares(1)
    await_heat()
    near_heat()
    fs = finish_peak()
    await_y_raw(1)
    edge_moments(1)
    peak = velocity_pass(1, fs, inner, no_peak)
    await_bytes(None, xo_in, xo_recv)
    finish_peak = spread_all(1, velocity_pass(1, fs, outer, peak))
    for x, r in blocks:
        for c in range(3):
            out_v[c, x, pl.ds(r, ROW), :] = vel[c, x + 1, pl.ds(ROW + r, ROW), :]
    await_bytes(None, hb.at[pl.ds(0, 2), own_y, :], hx_recv.at[1])
    far_heat()
    await_x_rest()
    for s in (0, 1):
        for r in range(0, sy, ROW):
            face_reads(s, r, face_rest(s, r))
    edge_reads()
    await_y_sums(1)
    for s in (0, 1):
        await_x_sums(1, s)
        ghost_x(1, fs, s)
    ghost_y(1, fs)

    def store_out(k, x, r, value):
        out_p[k, x, pl.ds(r, ROW), :] = value

    collided(blocks, fs, store_out)
    await_sends()
    fs = finish_peak()
    lift = {(x, r): fs * hb[x + 2, pl.ds(ROW + r, ROW), :] for x, r in blocks}
    for k in LIFTED:
        for x, r in blocks:
            rows = pl.ds(r, ROW)
            out_p[k, x, rows, :] = out_p[k, x, rows, :] + (3.0 * WEIGHT[k] * CS[k][2]) * lift[(x, r)]


def write_out(pops, vel, out_p, out_v, sems):
    copies = [
        pltpu.make_async_copy(pops, out_p, sems.at[0]),
        pltpu.make_async_copy(vel, out_v, sems.at[1]),
    ]
    for copy in copies:
        copy.start()
    for copy in copies:
        copy.wait()


def local(populations, heat_level, obstacle, heat_table):
    ngx = lax.axis_size("gx")
    ngy = lax.axis_size("gy")
    _, sx, sy, nz = populations.shape
    f32 = jnp.float32
    tall = sy + 2 * ROW
    dma = pltpu.SemaphoreType.DMA
    groups = peak_groups(ngx, ngy)
    phases = len(groups)
    vmem = pl.BlockSpec(memory_space=pltpu.VMEM)
    anywhere = pl.BlockSpec(memory_space=pltpu.HBM)
    shapes = (
        jax.ShapeDtypeStruct(populations.shape, f32),
        jax.ShapeDtypeStruct((3, sx, sy, nz), f32),
    )

    def floats(*shape):
        return pltpu.VMEM(shape, f32)

    def ints(*shape):
        return pltpu.VMEM(shape, jnp.int32)

    pops, velocity = pl.pallas_call(
        functools.partial(kernel, ngx, ngy),
        out_shape=shapes,
        in_specs=[anywhere] * 4,
        out_specs=[vmem] * 2,
        scratch_shapes=[
            floats(19, sx, tall, nz),
            floats(19, sx, tall, nz),
            floats(19, sx, sy, nz),
            floats(4, sx, sy, nz),
            floats(sx, sy, nz),
            floats(3, sx + 2, tall, nz),
            ints(sx, sy, nz),
            ints(sx, sy, nz),
            pltpu.SMEM(heat_table.shape, f32),
            ints(sx, sy, nz),
            floats(sx + 4, tall, nz),
            floats(sx + 4, tall, nz),
            floats(sx + 4, tall, nz),
            floats(4, sx + 2, sy, nz),
            floats(4, 2 * sx, nz),
            floats(2, 5, tall, nz),
            floats(2, 5, sy, nz),
            floats(STEPS, 2, 4, sy, nz),
            floats(STEPS, 2, 4, sy, nz),
            floats(STEPS, 9, 2 * sx, nz),
            floats(STEPS, 9, 2 * sx, nz),
            floats(8, ROW, nz),
            floats(STEPS, 6, ROW, nz),
            floats(STEPS, ROW, nz),
            floats(STEPS, 6, ROW, nz),
            floats(2, 3, sy, nz),
            floats(2, 2 * sy + ROW, nz),
            floats(2, 3, sy, nz),
            floats(2, 2 * sy + ROW, nz),
            floats(4, 2 * sx, nz),
            floats(5, 2 * sx, nz),
            floats(4, 2 * sx, nz),
            floats(2, ROW, nz),
            floats(4, ROW, nz),
            floats(4, 2 * sx, nz),
            floats(2, sy, nz),
            floats(2 * sx, nz),
            floats(8 * ROW, nz),
            floats(STEPS, phases, 1, nz),
            *[floats(STEPS, -(-len(group) // ROW) * ROW, nz) for group in groups],
            dma((4,)),
            pltpu.SemaphoreType.REGULAR,
            pltpu.SemaphoreType.REGULAR,
            dma,
            dma((2,)),
            dma((STEPS,)),
            dma((STEPS, 2)),
            dma,
            dma((STEPS, 2)),
            dma((STEPS, 2)),
            dma((STEPS, 4)),
            dma((2,)),
            dma((2,)),
            dma((phases,)),
            dma((STEPS, phases)),
        ],
        compiler_params=pltpu.CompilerParams(
            collective_id=0, has_side_effects=True, vmem_limit_bytes=24 * 1024 * 1024
        ),
        name="lattice_steps",
    )(*[pltpu.with_memory_space_constraint(a, pltpu.HBM) for a in (populations, heat_level, obstacle, heat_table)])
    return pl.pallas_call(
        write_out,
        out_shape=shapes,
        in_specs=[vmem] * 2,
        out_specs=[anywhere] * 2,
        scratch_shapes=[dma((2,))],
        compiler_params=pltpu.CompilerParams(vmem_limit_bytes=8 * 1024 * 1024),
        name="write_out",
    )(pops, velocity)


def solution(mesh):
    return jax.shard_map(
        local,
        mesh=mesh,
        in_specs=(
            P(None, ("member", "gx"), "gy", None),
            P(("member", "gx"), "gy", None),
            P(("member", "gx"), "gy", None),
            P(),
        ),
        out_specs=(P(None, ("member", "gx"), "gy", None), P(None, ("member", "gx"), "gy", None)),
        check_vma=False,
    )
```

```python
import functools

import jax
import jax.numpy as jnp
import numpy as np
from jax import lax
from jax.experimental import pallas as pl
from jax.experimental.pallas import tpu as pltpu
from jax.sharding import PartitionSpec as P

STEPS = 2
ROW = 8

lattice = np.array(
    [
        [0, 0, 0],
        [1, 0, 0],
        [-1, 0, 0],
        [0, 1, 0],
        [0, -1, 0],
        [0, 0, 1],
        [0, 0, -1],
        [1, 1, 0],
        [-1, -1, 0],
        [1, -1, 0],
        [-1, 1, 0],
        [1, 0, 1],
        [-1, 0, -1],
        [1, 0, -1],
        [-1, 0, 1],
        [0, 1, 1],
        [0, -1, -1],
        [0, 1, -1],
        [0, -1, 1],
    ]
)
CS = [tuple(int(c) for c in row) for row in lattice]
NUMBER = {c: k for k, c in enumerate(CS)}
WEIGHT = [1.0 / 3.0] + [1.0 / 18.0] * 6 + [1.0 / 36.0] * 12
OPP = [0, 2, 1, 4, 3, 6, 5, 8, 7, 10, 9, 12, 11, 14, 13, 16, 15, 18, 17]
base_tau = 0.52
smag_coef = 0.04
speed_cap = 0.1
strain_floor = 1e-06
LIFTED = [k for k in range(19) if CS[k][2] != 0]
ACROSS_X = {c: [NUMBER[(c, 0, 0)], NUMBER[(c, 1, 0)], NUMBER[(c, -1, 0)], NUMBER[(c, 0, 1)], NUMBER[(c, 0, -1)]] for c in (1, -1)}
ACROSS_Y = {c: [NUMBER[(0, c, 0)], NUMBER[(1, c, 0)], NUMBER[(-1, c, 0)], NUMBER[(0, c, 1)], NUMBER[(0, c, -1)]] for c in (1, -1)}
OUT = (-1, 1)
IN = (1, -1)


def tree_sum(items):
    items = list(items)
    while len(items) > 1:
        items = [items[i] + items[i + 1] if i + 1 < len(items) else items[i] for i in range(0, len(items), 2)]
    return items[0]


def peak_groups(ngx, ngy):
    if ngx * ngy <= 64:
        return [[(dx, dy) for dx in range(ngx) for dy in range(ngy) if dx or dy]]
    return [[(0, dy) for dy in range(1, ngy)], [(dx, 0) for dx in range(1, ngx)]]


def kernel(
    ngx, ngy,
    pops, heat_level, obstacle, table,
    out_p, out_v,
    st0, st1, rd, ms, rho_s, vel, hl, ob, tb, solid_s,
    hb, hzp, hzm, hm, hmy,
    xr, xp, xm_out, xm_in, yb_out, yb_in, cg, cm_out, cr_in, cm_in,
    ox, ox2, xo_in, x2_in, oy, dr, dm, tu, ex, ey, gfx, gfy, flat, pm_src, *rest,
):
    (*pm_bufs, load_sem, in_sem, col_sem, x_send, y_send, xr_recv, xm_recv, xo_recv, yr_recv, ym_recv,
     cm_recv, hx_recv, hy_recv, p_send, p_recv) = rest
    _, sx, sy, nz = pops.shape
    levels = table.shape[0]
    gx = lax.axis_index("gx")
    gy = lax.axis_index("gy")
    has_up = gy < ngy - 1
    has_down = gy > 0
    right = lax.rem(gx + 1, ngx)
    left = lax.rem(gx + ngx - 1, ngx)
    own_y = pl.ds(ROW, sy)
    face_x = (0, sx - 1)
    edge_y = (0, sy - 1)
    x_of = (left, right)
    y_of = (gy - 1, gy + 1)
    has_y = (has_down, has_up)

    barrier = pltpu.get_barrier_semaphore()

    def greet(sem, x, y):
        pl.semaphore_signal(sem, inc=1, device_id={"gx": x, "gy": y}, device_id_type=pl.DeviceIdType.MESH)

    groups = peak_groups(ngx, ngy)
    beside = sorted({1, ngx - 1} - {0})
    column = [(0, dy) for dy in range(1, ngy)]
    by_word = len(groups) == 1 and ngx <= 5
    greeted = [(dx, 0) for dx in beside] + column if by_word else [place for group in groups for place in group]
    partners = len(greeted)
    for dx, dy in greeted:
        greet(barrier, lax.rem(gx + dx, ngx), lax.rem(gy + dy, ngy))
    if len(groups) > 1:
        partners = partners + 2 * (jnp.where(has_up, 1, 0) + jnp.where(has_down, 1, 0))
        for s in (0, 1):

            @pl.when(has_y[s])
            def _():
                greet(barrier, right, y_of[s])
                greet(barrier, left, y_of[s])

    load_p = pltpu.make_async_copy(pops, st0.at[:, :, own_y, :], load_sem.at[0])
    load_h = pltpu.make_async_copy(heat_level, hl, load_sem.at[1])
    load_o = pltpu.make_async_copy(obstacle, ob, load_sem.at[2])
    load_t = pltpu.make_async_copy(table, tb, load_sem.at[3])
    load_p.start()
    load_h.start()
    load_o.start()
    load_t.start()

    def zeros(ref, *index):
        part = ref.at[index]
        part[...] = jnp.zeros(part.shape, jnp.float32)

    every = slice(None)
    for row in (ROW - 1, ROW + sy):
        for st in (st0, st1):
            for c in (1, -1):
                for k in ACROSS_Y[c]:
                    zeros(st, k, every, pl.ds(row, 1), every)
        zeros(xr, every, every, pl.ds(row, 1), every)
    for ref in (cg, tu, ey):
        ref[...] = jnp.zeros(ref.shape, jnp.float32)

    for s in (0, 1):

        @pl.when(jnp.logical_not(has_y[s]))
        def _():
            zeros(yb_in, every, every, pl.ds(s * sx, sx), every)
            for xs in (0, 1):
                zeros(cr_in, every, pl.ds(xs * 2 + s, 1), every)
                zeros(cm_in, every, every, pl.ds(xs * 2 + s, 1), every)
            zeros(hb, every, pl.ds((ROW - 2, ROW + sy)[s], 2), every)

    def guarded(cond, fn):
        if cond is None:
            fn()
        else:
            pl.when(cond)(fn)

    def send(cond, pairs, send_sem, recv_sem, x, y):
        def go():
            for src, dst in pairs:
                pltpu.make_async_remote_copy(
                    src_ref=src, dst_ref=dst, send_sem=send_sem, recv_sem=recv_sem,
                    device_id={"gx": x, "gy": y}, device_id_type=pl.DeviceIdType.MESH,
                ).start()

        guarded(cond, go)

    def await_bytes(cond, view, sem):
        guarded(cond, lambda: pltpu.make_async_copy(view, view, sem).wait())

    states = (st0, st1)
    corners = [(xs, ys) for xs in (0, 1) for ys in (0, 1)]
    raw_fields = pl.ds(0, 5)
    sum_fields = pl.ds(5, 4)

    at_end = (gx == 0, gx == ngx - 1)

    def along_x(pairs_of, sem_of):
        def far():
            for s in (0, 1):
                send(at_end[s], pairs_of(s), x_send, sem_of(s), x_of[s], gy)

        def near():
            for s in (0, 1):
                send(jnp.logical_not(at_end[s]), pairs_of(s), x_send, sem_of(s), x_of[s], gy)

        return far, near

    def send_x_raw():
        return along_x(
            lambda s: [(xp.at[s], xr.at[1 - s, :, own_y, :])],
            lambda s: xr_recv.at[0],
        )

    def send_x_sums(step):
        return along_x(lambda s: [(xm_out.at[step, s], xm_in.at[step, 1 - s])], lambda s: xm_recv.at[step, 1 - s])

    rest_rows = pl.ds(0, 2 * sy + 2)

    def send_x_shares(s):
        send(None, [(ox.at[s], xo_in.at[1 - s])], x_send, xo_recv, x_of[s], gy)

    def send_x_rest():
        return along_x(lambda s: [(ox2.at[s, rest_rows, :], x2_in.at[1 - s, rest_rows, :])], lambda s: xr_recv.at[1])

    def send_heat_x(layer):
        src, dst = ((2, sx + 1), (sx + 2, 1)) if layer == 0 else ((3, sx), (sx + 3, 0))
        for s in (0, 1):
            send(None, [(hb.at[src[s], own_y, :], hb.at[dst[s], own_y, :])], x_send, hx_recv.at[layer], x_of[s], gy)

    def send_heat():
        send_heat_x(0)
        for s in (0, 1):
            src = hb.at[pl.ds(2, sx), pl.ds((ROW, ROW + sy - 2)[s], 2), :]
            dst = hb.at[pl.ds(2, sx), pl.ds((ROW + sy, ROW - 2)[s], 2), :]
            send(has_y[s], [(src, dst)], y_send.at[s], hy_recv.at[1 - s], gx, y_of[s])
        to_corners(
            lambda c, xs, ys: (
                hb.at[2 + face_x[xs], pl.ds(ROW + edge_y[ys], 1), :],
                hb.at[(sx + 2, 1)[xs], pl.ds((ROW + sy, ROW - 1)[ys], 1), :],
            ),
            lambda c: hy_recv.at[c % 2],
        )

    def send_y(step, fields, recv_sem):
        for s in (0, 1):
            src = yb_out.at[step, fields, pl.ds(s * sx, sx), :]
            dst = yb_in.at[step, fields, pl.ds((1 - s) * sx, sx), :]
            send(has_y[s], [(src, dst)], y_send.at[s], recv_sem.at[step, 1 - s], gx, y_of[s])

    def to_corners(pair_of, sem_of):
        for c, (xs, ys) in enumerate(corners):
            send(has_y[ys], [pair_of(c, xs, ys)], y_send.at[ys], sem_of(3 - c), x_of[xs], y_of[ys])

    def send_corner_raw(step):
        st = states[step]

        def pair(c, xs, ys):
            k = NUMBER[(OUT[xs], OUT[ys], 0)]
            return st.at[k, face_x[xs], pl.ds(ROW + edge_y[ys], 1), :], cr_in.at[step, pl.ds(3 - c, 1), :]

        to_corners(pair, lambda c: yr_recv.at[step, c % 2])

    def send_corner_sums(step):
        to_corners(
            lambda c, xs, ys: (cm_out.at[step, :, pl.ds(c, 1), :], cm_in.at[step, :, pl.ds(3 - c, 1), :]),
            lambda c: cm_recv.at[step, c],
        )

    def await_y_raw(step):
        for s in (0, 1):
            await_bytes(has_y[s], flat.at[pl.ds(0, 5 * sx + 2), :], yr_recv.at[step, s])

    def await_x_raw():
        await_bytes(None, xr.at[:, :, own_y, :], xr_recv.at[0])

    def await_x_rest():
        await_bytes(None, x2_in.at[:, rest_rows, :], xr_recv.at[1])

    def await_y_sums(step):
        for s in (0, 1):
            await_bytes(has_y[s], yb_in.at[step, sum_fields, pl.ds(s * sx, sx), :], ym_recv.at[step, s])

    def await_x_sums(step, s):
        for ys in (0, 1):
            await_bytes(has_y[ys], cm_in.at[step, :, pl.ds(2 * s + ys, 1), :], cm_recv.at[step, 2 * s + ys])
        await_bytes(None, xm_in.at[step, s], xm_recv.at[step, s])

    def await_heat():
        for s in (0, 1):
            await_bytes(has_y[s], flat.at[pl.ds(0, 2 * sx + 2), :], hy_recv.at[s])
        await_bytes(None, hb.at[pl.ds(0, 2), own_y, :], hx_recv.at[0])

    def await_sends():
        for view in (xp, xm_out, ox, ox2.at[:, rest_rows, :], hb.at[pl.ds(0, 4), own_y, :]):
            await_bytes(None, view, x_send)
        for s in (0, 1):
            for view in (yb_out.at[:, :, pl.ds(0, sx), :], flat.at[pl.ds(0, 2 * sx + STEPS * 14 + 2), :]):
                await_bytes(has_y[s], view, y_send.at[s])

    def await_peak_sends():
        for phase, group in enumerate(groups):
            for step in range(STEPS):
                await_bytes(None, pm_bufs[phase].at[step, pl.ds(0, len(group)), :], p_send.at[phase])

    def spread(step, phase, value):
        group = peak_groups(ngx, ngy)[phase]
        count = len(group)
        buf = pm_bufs[phase]
        pm_src[step, phase] = value
        for d, (dx, dy) in sorted(enumerate(group, 1), key=lambda item: item[1][0] in (0, ngx // 2)):
            place = {"gx": lax.rem(gx + dx, ngx), "gy": lax.rem(gy + dy, ngy)}
            pltpu.make_async_remote_copy(
                src_ref=pm_src.at[step, phase],
                dst_ref=buf.at[step, pl.ds(d - 1, 1), :],
                send_sem=p_send.at[phase],
                recv_sem=p_recv.at[step, phase],
                device_id=place,
                device_id_type=pl.DeviceIdType.MESH,
            ).start()
        view = buf.at[step, pl.ds(0, count), :]

        def wait():
            await_bytes(None, view, p_recv.at[step, phase])
            return jnp.maximum(value, jnp.max(buf[step, pl.ds(0, count), :], axis=0, keepdims=True))

        return wait

    def spread_all(step, tile):
        wait = spread(step, 0, jnp.max(tile, axis=0, keepdims=True))

        def finish():
            best = wait()
            for phase in range(1, len(pm_bufs)):
                best = spread(step, phase, best)()
            peak = jnp.broadcast_to(jnp.max(best, axis=1, keepdims=True), (ROW, nz))
            return speed_cap * lax.rsqrt(speed_cap * speed_cap + peak)

        return finish

    blocks = [(x, r) for x in range(sx) for r in range(0, sy, ROW)]
    outer = [(x, r) for x, r in blocks if x in face_x]
    inner = [(x, r) for x, r in blocks if x not in face_x]
    lane = lax.broadcasted_iota(jnp.int32, (ROW, nz), 1)
    row_no = lax.broadcasted_iota(jnp.int32, (ROW, nz), 0)
    first_lane = lane == 0
    last_lane = lane == nz - 1
    edge_row = (row_no == 0, row_no == ROW - 1)
    pack_row = lax.broadcasted_iota(jnp.int32, (2 * sx, nz), 0)
    pack_sign = jnp.where(pack_row < sx, 1.0, -1.0)
    corner_x = jnp.where(row_no < 2, 1.0, -1.0)
    corner_y = jnp.where(lax.rem(row_no, 2) == 0, 1.0, -1.0)

    def shift_z(cells, cz):
        if not cz:
            return cells
        at = lax.broadcasted_iota(jnp.int32, cells.shape, 1)
        return jnp.where(at == (0 if cz > 0 else nz - 1), 0.0, pltpu.roll(cells, cz % nz, 1))

    def edges_of(r):
        return [s for s in (0, 1) if r == (0, sy - ROW)[s]]

    def own_sums(step, tiles):
        st = states[step]
        for x, r in tiles:
            rows = pl.ds(r, ROW)
            reads = {}
            for k, (cx, cy, cz) in enumerate(CS):
                if 0 <= x - cx < sx:
                    reads[k] = shift_z(st[k, x - cx, pl.ds(ROW + r - cy, ROW), :], cz)
                    rd[k, x, rows, :] = reads[k]
            sums = [tree_sum(list(reads.values()))]
            for c in range(3):
                plus = [reads[k] for k in reads if CS[k][c] > 0]
                minus = [reads[k] for k in reads if CS[k][c] < 0]
                if plus and minus:
                    sums.append(tree_sum(plus) - tree_sum(minus))
                else:
                    sums.append(tree_sum(plus) if plus else -tree_sum(minus))
            for m in range(4):
                ms[m, x, rows, :] = sums[m]
            sums[0] = jnp.where(solid_s[x, rows, :] != 0, 0.0, sums[0])
            for s in (0, 1):
                if x == face_x[s]:
                    for m in range(4):
                        xm_out[step, s, m, rows, :] = sums[m]
                if s in edges_of(r):
                    at = (0, ROW - 1)[s]
                    for m in range(4):
                        yb_out[step, 5 + m, pl.ds(s * sx + x, 1), :] = sums[m][at : at + 1, :]

    def pack_x_raw():
        for s in (0, 1):
            for j, k in enumerate(ACROSS_X[OUT[s]]):
                xp[s, j] = st0[k, face_x[s], own_y, :]

    def pack_y_raw(step):
        st = states[step]
        for s in (0, 1):
            for j, k in enumerate(ACROSS_Y[OUT[s]]):
                for x in range(sx):
                    yb_out[step, j, pl.ds(s * sx + x, 1), :] = st[k, x, pl.ds(ROW + edge_y[s], 1), :]

    def corner_sums(step):
        st = states[step]
        for c, (xs, ys) in enumerate(corners):
            dx, dy = OUT[xs], OUT[ys]
            fx, fy = face_x[xs], edge_y[ys]
            places = [
                ((0, dy, 0), fx, fy), ((0, dy, 1), fx, fy), ((0, dy, -1), fx, fy), ((dx, dy, 0), fx - dx, fy),
                ((dx, 0, 0), fx, fy), ((dx, 0, 1), fx, fy), ((dx, 0, -1), fx, fy), ((dx, dy, 0), fx, fy - dy),
            ]
            for f, (direction, x, y) in enumerate(places):
                cg[f, pl.ds(c, 1), :] = st[NUMBER[direction], x, pl.ds(ROW + y, 1), :]
        for half, sign in ((0, -corner_x), (1, -corner_y)):
            a, b, d, e = (cg[4 * half + f] for f in range(4))
            b, d = shift_z(b, 1), shift_z(d, -1)
            cm_out[step, 3 * half + 0] = (a + b) + (d + e)
            cm_out[step, 3 * half + 1] = sign * e
            cm_out[step, 3 * half + 2] = b - d

    def packed(fields, fill):
        plus = jnp.where(lax.rem(pack_row, sx) == 0, 0.0, pltpu.roll(fields[1], 1, 0))
        minus = jnp.where(lax.rem(pack_row, sx) == sx - 1, 0.0, pltpu.roll(fields[2], 2 * sx - 1, 0))
        if fill is not None:
            for ys in (0, 1):
                plus = jnp.where(pack_row == ys * sx, fill(ys), plus)
                minus = jnp.where(pack_row == ys * sx + sx - 1, fill(2 + ys), minus)
        return [fields[0], plus, minus, shift_z(fields[3], 1), shift_z(fields[4], -1)]

    def face_shares(step, sides):
        st = states[step]
        for s in sides:
            for r in range(0, sy, ROW):
                ks = ACROSS_X[OUT[s]]
                a, b, c, d, e = (st[k, face_x[s], pl.ds(ROW + r - CS[k][1], ROW), :] for k in ks)
                d, e = shift_z(d, 1), shift_z(e, -1)
                ox[s, 0, pl.ds(r, ROW), :] = ((a + b) + (c + d)) + e
                ox[s, 1, pl.ds(r, ROW), :] = b - c
                ox[s, 2, pl.ds(r, ROW), :] = d - e
                if step == 1:
                    ox2[s, pl.ds(r, ROW), :] = b
                    ox2[s, pl.ds(sy + r, ROW), :] = d
            if step == 1:
                ox2[s, pl.ds(2 * sy, 1), :] = st[ACROSS_X[OUT[s]][2], face_x[s], pl.ds(ROW, 1), :]
                ox2[s, pl.ds(2 * sy + 1, 1), :] = st[ACROSS_X[OUT[s]][1], face_x[s], pl.ds(ROW + sy - 1, 1), :]

    def edge_shares(step):
        a, b, c, d, e = packed([yb_out[step, j] for j in range(5)], None)
        total = ((a + b) + (c + d)) + e
        oy[0] = total
        oy[1] = b - c
        oy[2] = -pack_sign * total
        oy[3] = d - e

    def edge_moments(step):
        fields = packed([yb_in[step, j] for j in range(5)], lambda c: cr_in[step, pl.ds(c, 1), :])
        for j in range(5):
            dr[j] = fields[j]
        a, b, c, d, e = fields
        total = ((a + b) + (c + d)) + e
        for m, value in enumerate((total, b - c, pack_sign * total, d - e)):
            dm[m] = value

    def velocity_pass(step, fs, tiles, peak):
        for x, r in tiles:
            rows = pl.ds(r, ROW)
            sums = [ms[m, x, rows, :] for m in range(4)]
            for s in (0, 1):
                if x == face_x[s]:
                    if step == 0:
                        parts = face_raw(s, r)
                        shares = tree_sum(parts), parts[1] - parts[2], parts[3] - parts[4]
                        face_reads(s, r, parts)
                    else:
                        shares = [xo_in[s, m, rows, :] for m in range(3)]
                    sums[0] = sums[0] + shares[0]
                    sums[1] = sums[1] + shares[0] if s == 0 else sums[1] - shares[0]
                    sums[2] = sums[2] + shares[1]
                    sums[3] = sums[3] + shares[2]
            for s in edges_of(r):
                for m in range(4):
                    sums[m] = sums[m] + jnp.where(edge_row[s], dm[m, pl.ds(s * sx + x, 1), :], 0.0)
            if fs is not None:
                sums = [sums[m] + fs * hm[m, x + 1, rows, :] for m in range(4)]
            solid = solid_s[x, rows, :] != 0
            inv = jnp.where(solid, 0.0, 1.0 / jnp.where(solid, 1.0, sums[0]))
            rho_s[x, rows, :] = sums[0]
            speed = []
            for c in range(3):
                u = sums[1 + c] * inv
                vel[c, x + 1, pl.ds(ROW + r, ROW), :] = u
                speed.append(u * u)
            peak = jnp.maximum(peak, speed[0] + speed[1] + speed[2])
        return peak

    def face_raw(s, r):
        return [
            shift_z(xr[s, j, pl.ds(ROW + r - CS[k][1], ROW), :], CS[k][2]) for j, k in enumerate(ACROSS_X[IN[s]])
        ]

    def face_rest(s, r):
        total, along, height = (xo_in[s, m, pl.ds(r, ROW), :] for m in range(3))
        b, d = x2_in[s, pl.ds(r, ROW), :], x2_in[s, pl.ds(sy + r, ROW), :]
        c, e = b - along, d - height
        return [total - ((b + c) + (d + e)), b, c, d, e]

    def face_reads(s, r, parts):
        for k, part in zip(ACROSS_X[IN[s]], parts):
            rd[k, face_x[s], pl.ds(r, ROW), :] = part

    def edge_reads():
        for s in (0, 1):
            for j, k in enumerate(ACROSS_Y[IN[s]]):
                for x in range(sx):
                    rd[k, x, pl.ds(edge_y[s], 1), :] = dr[j, pl.ds(s * sx + x, 1), :]

    def ghost_x(step, fs, s):
        own = pl.ds(2 * s, 2)
        for ys in (0, 1):
            c = 2 * s + ys
            j = 1 if OUT[s] > 0 else 2
            tu[0, pl.ds(c, 1), :] = yb_in[step, j, pl.ds(ys * sx + face_x[s], 1), :]
            j = 1 if OUT[ys] > 0 else 2
            if step == 0:
                tu[1, pl.ds(c, 1), :] = xr[s, j, pl.ds(ROW + edge_y[ys], 1), :]
            else:
                tu[1, pl.ds(c, 1), :] = x2_in[s, pl.ds(2 * sy + ys, 1), :]
        sums = [cm_in[step, m, own, :] for m in range(6)]
        over, up = tu[0, own, :], tu[1, own, :]
        sign = jnp.where(lax.broadcasted_iota(jnp.int32, (2, nz), 0) == 0, 1.0, -1.0)
        total = sums[0] + over
        for m, value in enumerate((total, sums[1] + OUT[s] * over, sign * total, sums[2])):
            ex[m, own, :] = value
        total = sums[3] + up
        for m, value in enumerate((total, IN[s] * total, sums[4] - sign * up, sums[5])):
            for ys in (0, 1):
                ey[m, pl.ds(ys * sx + face_x[s], 1), :] = value[ys : ys + 1, :]
        for r in range(0, sy, ROW):
            rows = pl.ds(r, ROW)
            share = ox[s, 0, rows, :]
            sums = [xm_in[step, s, m, rows, :] for m in range(4)]
            if step == 0:
                gfx[s, rows, :] = sums[0]
            fluid = gfx[s, rows, :] > 0.0
            sums[0] = sums[0] + share
            sums[1] = sums[1] - share if s == 0 else sums[1] + share
            sums[2] = sums[2] + ox[s, 1, rows, :]
            sums[3] = sums[3] + ox[s, 2, rows, :]
            for ys in edges_of(r):
                for m in range(4):
                    sums[m] = sums[m] + jnp.where(edge_row[ys], ex[m, pl.ds(s * 2 + ys, 1), :], 0.0)
            at = (0, sx + 1)[s]
            if fs is not None:
                sums = [sums[m] + fs * hm[m, at, rows, :] for m in range(4)]
            inv = jnp.where(fluid, 1.0 / jnp.where(fluid, sums[0], 1.0), 0.0)
            for c in range(3):
                vel[c, at, pl.ds(ROW + r, ROW), :] = sums[1 + c] * inv

    def ghost_y(step, fs):
        sums = [yb_in[step, 5 + m] for m in range(4)]
        if step == 0:
            gfy[...] = sums[0]
        fluid = gfy[...] > 0.0
        sums = [sums[m] + oy[m] + ey[m] for m in range(4)]
        if fs is not None:
            sums = [sums[m] + fs[0:1, :] * hmy[m] for m in range(4)]
        inv = jnp.where(fluid, 1.0 / jnp.where(fluid, sums[0], 1.0), 0.0)
        for c in range(3):
            u = sums[1 + c] * inv
            for s in (0, 1):
                for x in range(sx):
                    at = s * sx + x
                    vel[c, x + 1, pl.ds((ROW - 1, ROW + sy)[s], 1), :] = u[at : at + 1, :]

    def shift_heat(x, row, span):
        cells = hb[x, pl.ds(row, span), :]
        hzp[x, pl.ds(row, span), :] = shift_z(cells, 1)
        hzm[x, pl.ds(row, span), :] = shift_z(cells, -1)

    def heat_moments(x, row, span):
        cells = [
            (hzp[i, pl.ds(y, span), :], hzm[i, pl.ds(y, span), :])
            for i, y in ((x, row), (x - 1, row), (x + 1, row), (x, row - 1), (x, row + 1))
        ]
        diff = [a - b for a, b in cells]
        both = [a + b for a, b in cells]
        main, side = 3.0 * WEIGHT[5], 3.0 * WEIGHT[11]
        return (
            main * diff[0] + side * ((diff[1] + diff[2]) + (diff[3] + diff[4])),
            side * (diff[1] - diff[2]),
            side * (diff[3] - diff[4]),
            main * both[0] + side * ((both[1] + both[2]) + (both[3] + both[4])),
        )

    def heat_sums(columns):
        for x in columns:
            for r in range(0, sy, ROW):
                for m, value in enumerate(heat_moments(x + 1, ROW + r, ROW)):
                    hm[m, x, pl.ds(r, ROW), :] = value

    def near_heat():
        for x in range(1, sx + 3):
            for r in range(0, sy, ROW):
                shift_heat(x, ROW + r, ROW)
        for x in range(2, sx + 2):
            shift_heat(x, ROW - 2, 2)
            shift_heat(x, ROW + sy, 2)
        heat_sums(range(1, sx + 1))

    def far_heat():
        for x in (0, sx + 3):
            for r in range(0, sy, ROW):
                shift_heat(x, ROW + r, ROW)
        for x in (1, sx + 2):
            shift_heat(x, ROW - 1, 1)
            shift_heat(x, ROW + sy, 1)
        heat_sums((0, sx + 1))
        for s in (0, 1):
            for x in range(sx):
                for m, value in enumerate(heat_moments(x + 2, (ROW - 1, ROW + sy)[s], 1)):
                    hmy[m, pl.ds(s * sx + x, 1), :] = value

    def collided(tiles, fs, store):
        for x, r in tiles:
            mid = pl.ds(ROW + r, ROW)
            u = [vel[c, x + 1, mid, :] for c in range(3)]
            diff = []
            for a in range(3):
                diff.append(
                    (
                        vel[a, x + 2, mid, :] - vel[a, x, mid, :],
                        vel[a, x + 1, pl.ds(ROW + r + 1, ROW), :] - vel[a, x + 1, pl.ds(ROW + r - 1, ROW), :],
                        pltpu.roll(u[a], nz - 1, 1) - pltpu.roll(u[a], 1, 1),
                    )
                )
            own = diff[0][0] * diff[0][0] + diff[1][1] * diff[1][1] + diff[2][2] * diff[2][2]
            xy = diff[0][1] + diff[1][0]
            xz = diff[0][2] + diff[2][0]
            yz = diff[1][2] + diff[2][1]
            size = jnp.sqrt(0.5 * own + 0.25 * (xy * xy + xz * xz + yz * yz) + strain_floor)
            omega = 1.0 / (base_tau + 3.0 * smag_coef * size)
            solid = solid_s[x, pl.ds(r, ROW), :] != 0
            density = rho_s[x, pl.ds(r, ROW), :]
            still = 1.0 - 1.5 * (u[0] * u[0] + u[1] * u[1] + u[2] * u[2])
            reads = [rd[k, x, pl.ds(r, ROW), :] for k in range(19)]
            if fs is not None:
                for k in LIFTED:
                    cx, cy, cz = CS[k]
                    source = hzp if cz > 0 else hzm
                    reads[k] = reads[k] + (3.0 * WEIGHT[k] * cz) * (fs * source[x + 2 - cx, pl.ds(ROW + r - cy, ROW), :])
            scaled = {w: (w * density) * omega for w in sorted(set(WEIGHT))}
            keep = 1.0 - omega
            store(0, x, r, jnp.where(solid, reads[0], keep * reads[0] + scaled[WEIGHT[0]] * still))
            for k in range(1, 19, 2):
                other = OPP[k]
                project = None
                for c in range(3):
                    if CS[k][c]:
                        if project is None:
                            project = u[c] if CS[k][c] > 0 else -u[c]
                        else:
                            project = project + u[c] if CS[k][c] > 0 else project - u[c]
                even = still + 4.5 * project * project
                odd = 3.0 * project
                weight = scaled[WEIGHT[k]]
                store(k, x, r, jnp.where(solid, reads[other], keep * reads[k] + weight * (even + odd)))
                store(other, x, r, jnp.where(solid, reads[k], keep * reads[other] + weight * (even - odd)))

    load_h.wait()
    load_o.wait()
    load_t.wait()
    for x, r in blocks:
        rows = pl.ds(r, ROW)
        code = hl[x, rows, :]
        heat = jnp.zeros((ROW, nz), jnp.float32)
        for level in range(levels):
            heat = jnp.where(code == level, tb[level], heat)
        grid_y = gy * sy + r + row_no
        solid = (
            (ob[x, rows, :] == 1) | (grid_y == 0) | (grid_y == ngy * sy - 1) | first_lane | last_lane
        )
        solid_s[x, rows, :] = jnp.where(solid, 1, 0)
        hb[x + 2, pl.ds(ROW + r, ROW), :] = jnp.where(solid, 0.0, heat)

    neighbours = jnp.where(has_up, 1, 0) + jnp.where(has_down, 1, 0)
    sums_far, sums_near = send_x_sums(0)
    raw_far, raw_near = send_x_raw()
    neighbours = jnp.where(has_up, 1, 0) + jnp.where(has_down, 1, 0)
    sums_far, sums_near = send_x_sums(0)
    raw_far, raw_near = send_x_raw()
    load_p.wait()
    pack_x_raw()
    pl.semaphore_wait(barrier, partners)
    if by_word:
        for s in (0, 1):

            @pl.when(has_y[s])
            def _():
                greet(in_sem, gx, y_of[s])

    raw_far()
    own_sums(0, outer)
    sums_far()
    if by_word:
        for _, dy in column:
            other = lax.rem(gy + dy, ngy)

            @pl.when((other > gy + 1) | (other < gy - 1))
            def _():
                greet(col_sem, gx, other)

    pack_y_raw(0)
    send_y(0, raw_fields, yr_recv)
    corner_sums(0)
    own_sums(0, inner)
    send_y(0, sum_fields, ym_recv)
    if by_word:
        pl.semaphore_wait(in_sem, neighbours)
    send_corner_raw(0)
    send_corner_sums(0)
    if by_word:
        pl.semaphore_wait(col_sem, len(column) - neighbours)
    raw_near()
    sums_near()
    face_shares(0, (0, 1))
    edge_shares(0)
    send_heat()
    no_peak = jnp.zeros((ROW, nz), jnp.float32)
    await_y_raw(0)
    edge_moments(0)
    peak = velocity_pass(0, None, inner, no_peak)
    await_x_raw()
    finish_peak = spread_all(0, velocity_pass(0, None, outer, peak))
    edge_reads()
    await_y_sums(0)

    def store_st1(k, x, r, value):
        st1[k, x, pl.ds(ROW + r, ROW), :] = value

    def face(s):
        await_x_sums(0, s)
        ghost_x(0, None, s)
        ghost_y(0, None)
        collided([(x, r) for x, r in blocks if x == face_x[s]], None, store_st1)
        face_shares(1, (s,))
        send_x_shares(s)

    @pl.when(gx == ngx - 1)
    def _():
        face(1)
        face(0)

    @pl.when(gx != ngx - 1)
    def _():
        face(0)
        face(1)

    collided(inner, None, store_st1)
    send_corner_raw(1)
    pack_y_raw(1)
    send_y(1, raw_fields, yr_recv)
    own_sums(1, outer)
    for part in (*send_x_sums(1), *send_x_rest()):
        part()
    own_sums(1, inner)
    send_y(1, sum_fields, ym_recv)
    corner_sums(1)
    send_corner_sums(1)
    send_heat_x(1)
    edge_shares(1)
    await_heat()
    near_heat()
    fs = finish_peak()
    await_y_raw(1)
    edge_moments(1)
    peak = velocity_pass(1, fs, inner, no_peak)
    await_bytes(None, xo_in, xo_recv)
    finish_peak = spread_all(1, velocity_pass(1, fs, outer, peak))
    for x, r in blocks:
        for c in range(3):
            out_v[c, x, pl.ds(r, ROW), :] = vel[c, x + 1, pl.ds(ROW + r, ROW), :]
    await_bytes(None, hb.at[pl.ds(0, 2), own_y, :], hx_recv.at[1])
    far_heat()
    await_x_rest()
    for s in (0, 1):
        for r in range(0, sy, ROW):
            face_reads(s, r, face_rest(s, r))
    edge_reads()
    await_y_sums(1)
    for s in (0, 1):
        await_x_sums(1, s)
        ghost_x(1, fs, s)
    ghost_y(1, fs)

    def store_out(k, x, r, value):
        out_p[k, x, pl.ds(r, ROW), :] = value

    collided(blocks, fs, store_out)
    await_sends()
    fs = finish_peak()
    await_peak_sends()
    lift = {(x, r): fs * hb[x + 2, pl.ds(ROW + r, ROW), :] for x, r in blocks}
    for k in LIFTED:
        for x, r in blocks:
            rows = pl.ds(r, ROW)
            out_p[k, x, rows, :] = out_p[k, x, rows, :] + (3.0 * WEIGHT[k] * CS[k][2]) * lift[(x, r)]


def write_out(pops, vel, out_p, out_v, sems):
    copies = [
        pltpu.make_async_copy(pops, out_p, sems.at[0]),
        pltpu.make_async_copy(vel, out_v, sems.at[1]),
    ]
    for copy in copies:
        copy.start()
    for copy in copies:
        copy.wait()


def local(populations, heat_level, obstacle, heat_table):
    ngx = lax.axis_size("gx")
    ngy = lax.axis_size("gy")
    _, sx, sy, nz = populations.shape
    f32 = jnp.float32
    tall = sy + 2 * ROW
    dma = pltpu.SemaphoreType.DMA
    groups = peak_groups(ngx, ngy)
    phases = len(groups)
    vmem = pl.BlockSpec(memory_space=pltpu.VMEM)
    anywhere = pl.BlockSpec(memory_space=pltpu.HBM)
    shapes = (
        jax.ShapeDtypeStruct(populations.shape, f32),
        jax.ShapeDtypeStruct((3, sx, sy, nz), f32),
    )

    def floats(*shape):
        return pltpu.VMEM(shape, f32)

    def ints(*shape):
        return pltpu.VMEM(shape, jnp.int32)

    pops, velocity = pl.pallas_call(
        functools.partial(kernel, ngx, ngy),
        out_shape=shapes,
        in_specs=[anywhere] * 4,
        out_specs=[vmem] * 2,
        scratch_shapes=[
            floats(19, sx, tall, nz),
            floats(19, sx, tall, nz),
            floats(19, sx, sy, nz),
            floats(4, sx, sy, nz),
            floats(sx, sy, nz),
            floats(3, sx + 2, tall, nz),
            ints(sx, sy, nz),
            ints(sx, sy, nz),
            pltpu.SMEM(heat_table.shape, f32),
            ints(sx, sy, nz),
            floats(sx + 4, tall, nz),
            floats(sx + 4, tall, nz),
            floats(sx + 4, tall, nz),
            floats(4, sx + 2, sy, nz),
            floats(4, 2 * sx, nz),
            floats(2, 5, tall, nz),
            floats(2, 5, sy, nz),
            floats(STEPS, 2, 4, sy, nz),
            floats(STEPS, 2, 4, sy, nz),
            floats(STEPS, 9, 2 * sx, nz),
            floats(STEPS, 9, 2 * sx, nz),
            floats(8, ROW, nz),
            floats(STEPS, 6, ROW, nz),
            floats(STEPS, ROW, nz),
            floats(STEPS, 6, ROW, nz),
            floats(2, 3, sy, nz),
            floats(2, 2 * sy + ROW, nz),
            floats(2, 3, sy, nz),
            floats(2, 2 * sy + ROW, nz),
            floats(4, 2 * sx, nz),
            floats(5, 2 * sx, nz),
            floats(4, 2 * sx, nz),
            floats(2, ROW, nz),
            floats(4, ROW, nz),
            floats(4, 2 * sx, nz),
            floats(2, sy, nz),
            floats(2 * sx, nz),
            floats(8 * ROW, nz),
            floats(STEPS, phases, 1, nz),
            *[floats(STEPS, -(-len(group) // ROW) * ROW, nz) for group in groups],
            dma((4,)),
            pltpu.SemaphoreType.REGULAR,
            pltpu.SemaphoreType.REGULAR,
            dma,
            dma((2,)),
            dma((STEPS,)),
            dma((STEPS, 2)),
            dma,
            dma((STEPS, 2)),
            dma((STEPS, 2)),
            dma((STEPS, 4)),
            dma((2,)),
            dma((2,)),
            dma((phases,)),
            dma((STEPS, phases)),
        ],
        compiler_params=pltpu.CompilerParams(
            collective_id=0, has_side_effects=True, vmem_limit_bytes=24 * 1024 * 1024
        ),
        name="lattice_steps",
    )(*[pltpu.with_memory_space_constraint(a, pltpu.HBM) for a in (populations, heat_level, obstacle, heat_table)])
    return pl.pallas_call(
        write_out,
        out_shape=shapes,
        in_specs=[vmem] * 2,
        out_specs=[anywhere] * 2,
        scratch_shapes=[dma((2,))],
        compiler_params=pltpu.CompilerParams(vmem_limit_bytes=8 * 1024 * 1024),
        name="write_out",
    )(pops, velocity)


def solution(mesh):
    return jax.shard_map(
        local,
        mesh=mesh,
        in_specs=(
            P(None, ("member", "gx"), "gy", None),
            P(("member", "gx"), "gy", None),
            P(("member", "gx"), "gy", None),
            P(),
        ),
        out_specs=(P(None, ("member", "gx"), "gy", None), P(None, ("member", "gx"), "gy", None)),
        check_vma=False,
    )
```

```python
import functools

import jax
import jax.numpy as jnp
import numpy as np
from jax import lax
from jax.experimental import pallas as pl
from jax.experimental.pallas import tpu as pltpu
from jax.sharding import PartitionSpec as P

STEPS = 2
ROW = 8

lattice = np.array(
    [
        [0, 0, 0],
        [1, 0, 0],
        [-1, 0, 0],
        [0, 1, 0],
        [0, -1, 0],
        [0, 0, 1],
        [0, 0, -1],
        [1, 1, 0],
        [-1, -1, 0],
        [1, -1, 0],
        [-1, 1, 0],
        [1, 0, 1],
        [-1, 0, -1],
        [1, 0, -1],
        [-1, 0, 1],
        [0, 1, 1],
        [0, -1, -1],
        [0, 1, -1],
        [0, -1, 1],
    ]
)
CS = [tuple(int(c) for c in row) for row in lattice]
NUMBER = {c: k for k, c in enumerate(CS)}
WEIGHT = [1.0 / 3.0] + [1.0 / 18.0] * 6 + [1.0 / 36.0] * 12
OPP = [0, 2, 1, 4, 3, 6, 5, 8, 7, 10, 9, 12, 11, 14, 13, 16, 15, 18, 17]
base_tau = 0.52
smag_coef = 0.04
speed_cap = 0.1
strain_floor = 1e-06
LIFTED = [k for k in range(19) if CS[k][2] != 0]
ACROSS_X = {c: [NUMBER[(c, 0, 0)], NUMBER[(c, 1, 0)], NUMBER[(c, -1, 0)], NUMBER[(c, 0, 1)], NUMBER[(c, 0, -1)]] for c in (1, -1)}
ACROSS_Y = {c: [NUMBER[(0, c, 0)], NUMBER[(1, c, 0)], NUMBER[(-1, c, 0)], NUMBER[(0, c, 1)], NUMBER[(0, c, -1)]] for c in (1, -1)}
OUT = (-1, 1)
IN = (1, -1)


def tree_sum(items):
    items = list(items)
    while len(items) > 1:
        items = [items[i] + items[i + 1] if i + 1 < len(items) else items[i] for i in range(0, len(items), 2)]
    return items[0]


def peak_groups(ngx, ngy):
    if ngx * ngy <= 64:
        return [[(dx, dy) for dx in range(ngx) for dy in range(ngy) if dx or dy]]
    return [[(0, dy) for dy in range(1, ngy)], [(dx, 0) for dx in range(1, ngx)]]


def kernel(
    ngx, ngy,
    pops, heat_level, obstacle, table,
    out_p, out_v,
    st0, st1, rd, ms, rho_s, vel, hl, ob, tb, solid_s,
    hb, hzp, hzm, hm, hmy,
    xr, xp, xm_out, xm_in, yb_out, yb_in, cg, cm_out, cr_in, cm_in,
    ox, ox2, xo_in, x2_in, oy, dr, dm, tu, ex, ey, gfx, gfy, flat, pm_src, *rest,
):
    (*pm_bufs, load_sem, in_sem, col_sem, x_send, y_send, xr_recv, xm_recv, xo_recv, yr_recv, ym_recv,
     cm_recv, hx_recv, hy_recv, p_send, p_recv) = rest
    _, sx, sy, nz = pops.shape
    levels = table.shape[0]
    gx = lax.axis_index("gx")
    gy = lax.axis_index("gy")
    has_up = gy < ngy - 1
    has_down = gy > 0
    right = lax.rem(gx + 1, ngx)
    left = lax.rem(gx + ngx - 1, ngx)
    own_y = pl.ds(ROW, sy)
    face_x = (0, sx - 1)
    edge_y = (0, sy - 1)
    x_of = (left, right)
    y_of = (gy - 1, gy + 1)
    has_y = (has_down, has_up)

    barrier = pltpu.get_barrier_semaphore()

    def greet(sem, x, y):
        pl.semaphore_signal(sem, inc=1, device_id={"gx": x, "gy": y}, device_id_type=pl.DeviceIdType.MESH)

    groups = peak_groups(ngx, ngy)
    beside = sorted({1, ngx - 1} - {0})
    column = [(0, dy) for dy in range(1, ngy)]
    by_word = len(groups) == 1 and ngx <= 5
    greeted = [(dx, 0) for dx in beside] + column if by_word else [place for group in groups for place in group]
    partners = len(greeted)
    for dx, dy in greeted:
        greet(barrier, lax.rem(gx + dx, ngx), lax.rem(gy + dy, ngy))
    if len(groups) > 1:
        partners = partners + 2 * (jnp.where(has_up, 1, 0) + jnp.where(has_down, 1, 0))
        for s in (0, 1):

            @pl.when(has_y[s])
            def _():
                greet(barrier, right, y_of[s])
                greet(barrier, left, y_of[s])

    load_p = pltpu.make_async_copy(pops, st0.at[:, :, own_y, :], load_sem.at[0])
    load_h = pltpu.make_async_copy(heat_level, hl, load_sem.at[1])
    load_o = pltpu.make_async_copy(obstacle, ob, load_sem.at[2])
    load_t = pltpu.make_async_copy(table, tb, load_sem.at[3])
    load_p.start()
    load_h.start()
    load_o.start()
    load_t.start()

    def zeros(ref, *index):
        part = ref.at[index]
        part[...] = jnp.zeros(part.shape, jnp.float32)

    every = slice(None)
    for row in (ROW - 1, ROW + sy):
        for st in (st0, st1):
            for c in (1, -1):
                for k in ACROSS_Y[c]:
                    zeros(st, k, every, pl.ds(row, 1), every)
        zeros(xr, every, every, pl.ds(row, 1), every)
    for ref in (cg, tu, ey):
        ref[...] = jnp.zeros(ref.shape, jnp.float32)

    for s in (0, 1):

        @pl.when(jnp.logical_not(has_y[s]))
        def _():
            zeros(yb_in, every, every, pl.ds(s * sx, sx), every)
            for xs in (0, 1):
                zeros(cr_in, every, pl.ds(xs * 2 + s, 1), every)
                zeros(cm_in, every, every, pl.ds(xs * 2 + s, 1), every)
            zeros(hb, every, pl.ds((ROW - 2, ROW + sy)[s], 2), every)

    def guarded(cond, fn):
        if cond is None:
            fn()
        else:
            pl.when(cond)(fn)

    def send(cond, pairs, send_sem, recv_sem, x, y):
        def go():
            for src, dst in pairs:
                pltpu.make_async_remote_copy(
                    src_ref=src, dst_ref=dst, send_sem=send_sem, recv_sem=recv_sem,
                    device_id={"gx": x, "gy": y}, device_id_type=pl.DeviceIdType.MESH,
                ).start()

        guarded(cond, go)

    def await_bytes(cond, view, sem):
        guarded(cond, lambda: pltpu.make_async_copy(view, view, sem).wait())

    states = (st0, st1)
    corners = [(xs, ys) for xs in (0, 1) for ys in (0, 1)]
    raw_fields = pl.ds(0, 5)
    sum_fields = pl.ds(5, 4)

    at_end = (gx == 0, gx == ngx - 1)

    def along_x(pairs_of, sem_of):
        def far():
            for s in (0, 1):
                send(at_end[s], pairs_of(s), x_send, sem_of(s), x_of[s], gy)

        def near():
            for s in (0, 1):
                send(jnp.logical_not(at_end[s]), pairs_of(s), x_send, sem_of(s), x_of[s], gy)

        return far, near

    def send_x_raw():
        return along_x(
            lambda s: [(xp.at[s], xr.at[1 - s, :, own_y, :])],
            lambda s: xr_recv.at[0],
        )

    def send_x_sums(step):
        return along_x(lambda s: [(xm_out.at[step, s], xm_in.at[step, 1 - s])], lambda s: xm_recv.at[step, 1 - s])

    rest_rows = pl.ds(0, 2 * sy + 2)

    def send_x_shares(s):
        send(None, [(ox.at[s], xo_in.at[1 - s])], x_send, xo_recv, x_of[s], gy)

    def send_x_rest():
        return along_x(lambda s: [(ox2.at[s, rest_rows, :], x2_in.at[1 - s, rest_rows, :])], lambda s: xr_recv.at[1])

    def send_heat_x(layer):
        src, dst = ((2, sx + 1), (sx + 2, 1)) if layer == 0 else ((3, sx), (sx + 3, 0))
        for s in (0, 1):
            send(None, [(hb.at[src[s], own_y, :], hb.at[dst[s], own_y, :])], x_send, hx_recv.at[layer], x_of[s], gy)

    def send_heat():
        send_heat_x(0)
        for s in (0, 1):
            src = hb.at[pl.ds(2, sx), pl.ds((ROW, ROW + sy - 2)[s], 2), :]
            dst = hb.at[pl.ds(2, sx), pl.ds((ROW + sy, ROW - 2)[s], 2), :]
            send(has_y[s], [(src, dst)], y_send.at[s], hy_recv.at[1 - s], gx, y_of[s])
        to_corners(
            lambda c, xs, ys: (
                hb.at[2 + face_x[xs], pl.ds(ROW + edge_y[ys], 1), :],
                hb.at[(sx + 2, 1)[xs], pl.ds((ROW + sy, ROW - 1)[ys], 1), :],
            ),
            lambda c: hy_recv.at[c % 2],
        )

    def send_y(step, fields, recv_sem):
        for s in (0, 1):
            src = yb_out.at[step, fields, pl.ds(s * sx, sx), :]
            dst = yb_in.at[step, fields, pl.ds((1 - s) * sx, sx), :]
            send(has_y[s], [(src, dst)], y_send.at[s], recv_sem.at[step, 1 - s], gx, y_of[s])

    def to_corners(pair_of, sem_of, sides=(0, 1)):
        for c, (xs, ys) in enumerate(corners):
            if xs in sides:
                send(has_y[ys], [pair_of(c, xs, ys)], y_send.at[ys], sem_of(3 - c), x_of[xs], y_of[ys])

    def send_corner_raw(step, sides):
        st = states[step]

        def pair(c, xs, ys):
            k = NUMBER[(OUT[xs], OUT[ys], 0)]
            return st.at[k, face_x[xs], pl.ds(ROW + edge_y[ys], 1), :], cr_in.at[step, pl.ds(3 - c, 1), :]

        to_corners(pair, lambda c: yr_recv.at[step, c % 2], sides)

    def send_corner_sums(step):
        to_corners(
            lambda c, xs, ys: (cm_out.at[step, :, pl.ds(c, 1), :], cm_in.at[step, :, pl.ds(3 - c, 1), :]),
            lambda c: cm_recv.at[step, c],
        )

    def await_y_raw(step):
        for s in (0, 1):
            await_bytes(has_y[s], flat.at[pl.ds(0, 5 * sx + 2), :], yr_recv.at[step, s])

    def await_x_raw():
        await_bytes(None, xr.at[:, :, own_y, :], xr_recv.at[0])

    def await_x_rest():
        await_bytes(None, x2_in.at[:, rest_rows, :], xr_recv.at[1])

    def await_y_sums(step):
        for s in (0, 1):
            await_bytes(has_y[s], yb_in.at[step, sum_fields, pl.ds(s * sx, sx), :], ym_recv.at[step, s])

    def await_x_sums(step, s):
        for ys in (0, 1):
            await_bytes(has_y[ys], cm_in.at[step, :, pl.ds(2 * s + ys, 1), :], cm_recv.at[step, 2 * s + ys])
        await_bytes(None, xm_in.at[step, s], xm_recv.at[step, s])

    def await_heat():
        for s in (0, 1):
            await_bytes(has_y[s], flat.at[pl.ds(0, 2 * sx + 2), :], hy_recv.at[s])
        await_bytes(None, hb.at[pl.ds(0, 2), own_y, :], hx_recv.at[0])

    def await_sends():
        for view in (xp, xm_out, ox, ox2.at[:, rest_rows, :], hb.at[pl.ds(0, 4), own_y, :]):
            await_bytes(None, view, x_send)
        for s in (0, 1):
            for view in (yb_out.at[:, :, pl.ds(0, sx), :], flat.at[pl.ds(0, 2 * sx + STEPS * 14 + 2), :]):
                await_bytes(has_y[s], view, y_send.at[s])

    def await_peak_sends():
        for phase, group in enumerate(groups):
            for step in range(STEPS):
                await_bytes(None, pm_bufs[phase].at[step, pl.ds(0, len(group)), :], p_send.at[phase])

    def spread(step, phase, value):
        group = peak_groups(ngx, ngy)[phase]
        count = len(group)
        buf = pm_bufs[phase]
        pm_src[step, phase] = value
        for d, (dx, dy) in sorted(enumerate(group, 1), key=lambda item: item[1][0] in (0, ngx // 2)):
            place = {"gx": lax.rem(gx + dx, ngx), "gy": lax.rem(gy + dy, ngy)}
            pltpu.make_async_remote_copy(
                src_ref=pm_src.at[step, phase],
                dst_ref=buf.at[step, pl.ds(d - 1, 1), :],
                send_sem=p_send.at[phase],
                recv_sem=p_recv.at[step, phase],
                device_id=place,
                device_id_type=pl.DeviceIdType.MESH,
            ).start()
        view = buf.at[step, pl.ds(0, count), :]

        def wait():
            await_bytes(None, view, p_recv.at[step, phase])
            return jnp.maximum(value, jnp.max(buf[step, pl.ds(0, count), :], axis=0, keepdims=True))

        return wait

    def spread_all(step, tile):
        wait = spread(step, 0, jnp.max(tile, axis=0, keepdims=True))

        def finish():
            best = wait()
            for phase in range(1, len(pm_bufs)):
                best = spread(step, phase, best)()
            peak = jnp.broadcast_to(jnp.max(best, axis=1, keepdims=True), (ROW, nz))
            return speed_cap * lax.rsqrt(speed_cap * speed_cap + peak)

        return finish

    blocks = [(x, r) for x in range(sx) for r in range(0, sy, ROW)]
    outer = [(x, r) for x, r in blocks if x in face_x]
    inner = [(x, r) for x, r in blocks if x not in face_x]
    lane = lax.broadcasted_iota(jnp.int32, (ROW, nz), 1)
    row_no = lax.broadcasted_iota(jnp.int32, (ROW, nz), 0)
    first_lane = lane == 0
    last_lane = lane == nz - 1
    edge_row = (row_no == 0, row_no == ROW - 1)
    pack_row = lax.broadcasted_iota(jnp.int32, (2 * sx, nz), 0)
    pack_sign = jnp.where(pack_row < sx, 1.0, -1.0)
    corner_x = jnp.where(row_no < 2, 1.0, -1.0)
    corner_y = jnp.where(lax.rem(row_no, 2) == 0, 1.0, -1.0)

    def shift_z(cells, cz):
        if not cz:
            return cells
        at = lax.broadcasted_iota(jnp.int32, cells.shape, 1)
        return jnp.where(at == (0 if cz > 0 else nz - 1), 0.0, pltpu.roll(cells, cz % nz, 1))

    def edges_of(r):
        return [s for s in (0, 1) if r == (0, sy - ROW)[s]]

    def own_sums(step, tiles):
        st = states[step]
        for x, r in tiles:
            rows = pl.ds(r, ROW)
            reads = {}
            for k, (cx, cy, cz) in enumerate(CS):
                if 0 <= x - cx < sx:
                    reads[k] = shift_z(st[k, x - cx, pl.ds(ROW + r - cy, ROW), :], cz)
                    rd[k, x, rows, :] = reads[k]
            sums = [tree_sum(list(reads.values()))]
            for c in range(3):
                plus = [reads[k] for k in reads if CS[k][c] > 0]
                minus = [reads[k] for k in reads if CS[k][c] < 0]
                if plus and minus:
                    sums.append(tree_sum(plus) - tree_sum(minus))
                else:
                    sums.append(tree_sum(plus) if plus else -tree_sum(minus))
            for m in range(4):
                ms[m, x, rows, :] = sums[m]
            sums[0] = jnp.where(solid_s[x, rows, :] != 0, 0.0, sums[0])
            for s in (0, 1):
                if x == face_x[s]:
                    for m in range(4):
                        xm_out[step, s, m, rows, :] = sums[m]
                if s in edges_of(r):
                    at = (0, ROW - 1)[s]
                    for m in range(4):
                        yb_out[step, 5 + m, pl.ds(s * sx + x, 1), :] = sums[m][at : at + 1, :]

    def pack_x_raw():
        for s in (0, 1):
            for j, k in enumerate(ACROSS_X[OUT[s]]):
                xp[s, j] = st0[k, face_x[s], own_y, :]

    def pack_y_raw(step):
        st = states[step]
        for s in (0, 1):
            for j, k in enumerate(ACROSS_Y[OUT[s]]):
                for x in range(sx):
                    yb_out[step, j, pl.ds(s * sx + x, 1), :] = st[k, x, pl.ds(ROW + edge_y[s], 1), :]

    def corner_sums(step):
        st = states[step]
        for c, (xs, ys) in enumerate(corners):
            dx, dy = OUT[xs], OUT[ys]
            fx, fy = face_x[xs], edge_y[ys]
            places = [
                ((0, dy, 0), fx, fy), ((0, dy, 1), fx, fy), ((0, dy, -1), fx, fy), ((dx, dy, 0), fx - dx, fy),
                ((dx, 0, 0), fx, fy), ((dx, 0, 1), fx, fy), ((dx, 0, -1), fx, fy), ((dx, dy, 0), fx, fy - dy),
            ]
            for f, (direction, x, y) in enumerate(places):
                cg[f, pl.ds(c, 1), :] = st[NUMBER[direction], x, pl.ds(ROW + y, 1), :]
        for half, sign in ((0, -corner_x), (1, -corner_y)):
            a, b, d, e = (cg[4 * half + f] for f in range(4))
            b, d = shift_z(b, 1), shift_z(d, -1)
            cm_out[step, 3 * half + 0] = (a + b) + (d + e)
            cm_out[step, 3 * half + 1] = sign * e
            cm_out[step, 3 * half + 2] = b - d

    def packed(fields, fill):
        plus = jnp.where(lax.rem(pack_row, sx) == 0, 0.0, pltpu.roll(fields[1], 1, 0))
        minus = jnp.where(lax.rem(pack_row, sx) == sx - 1, 0.0, pltpu.roll(fields[2], 2 * sx - 1, 0))
        if fill is not None:
            for ys in (0, 1):
                plus = jnp.where(pack_row == ys * sx, fill(ys), plus)
                minus = jnp.where(pack_row == ys * sx + sx - 1, fill(2 + ys), minus)
        return [fields[0], plus, minus, shift_z(fields[3], 1), shift_z(fields[4], -1)]

    def face_shares(step, sides):
        st = states[step]
        for s in sides:
            for r in range(0, sy, ROW):
                ks = ACROSS_X[OUT[s]]
                a, b, c, d, e = (st[k, face_x[s], pl.ds(ROW + r - CS[k][1], ROW), :] for k in ks)
                d, e = shift_z(d, 1), shift_z(e, -1)
                ox[s, 0, pl.ds(r, ROW), :] = ((a + b) + (c + d)) + e
                ox[s, 1, pl.ds(r, ROW), :] = b - c
                ox[s, 2, pl.ds(r, ROW), :] = d - e
                if step == 1:
                    ox2[s, pl.ds(r, ROW), :] = b
                    ox2[s, pl.ds(sy + r, ROW), :] = d
            if step == 1:
                ox2[s, pl.ds(2 * sy, 1), :] = st[ACROSS_X[OUT[s]][2], face_x[s], pl.ds(ROW, 1), :]
                ox2[s, pl.ds(2 * sy + 1, 1), :] = st[ACROSS_X[OUT[s]][1], face_x[s], pl.ds(ROW + sy - 1, 1), :]

    def edge_shares(step):
        a, b, c, d, e = packed([yb_out[step, j] for j in range(5)], None)
        total = ((a + b) + (c + d)) + e
        oy[0] = total
        oy[1] = b - c
        oy[2] = -pack_sign * total
        oy[3] = d - e

    def edge_moments(step):
        fields = packed([yb_in[step, j] for j in range(5)], lambda c: cr_in[step, pl.ds(c, 1), :])
        for j in range(5):
            dr[j] = fields[j]
        a, b, c, d, e = fields
        total = ((a + b) + (c + d)) + e
        for m, value in enumerate((total, b - c, pack_sign * total, d - e)):
            dm[m] = value

    def velocity_pass(step, fs, tiles, peak):
        for x, r in tiles:
            rows = pl.ds(r, ROW)
            sums = [ms[m, x, rows, :] for m in range(4)]
            for s in (0, 1):
                if x == face_x[s]:
                    if step == 0:
                        parts = face_raw(s, r)
                        shares = tree_sum(parts), parts[1] - parts[2], parts[3] - parts[4]
                        face_reads(s, r, parts)
                    else:
                        shares = [xo_in[s, m, rows, :] for m in range(3)]
                    sums[0] = sums[0] + shares[0]
                    sums[1] = sums[1] + shares[0] if s == 0 else sums[1] - shares[0]
                    sums[2] = sums[2] + shares[1]
                    sums[3] = sums[3] + shares[2]
            for s in edges_of(r):
                for m in range(4):
                    sums[m] = sums[m] + jnp.where(edge_row[s], dm[m, pl.ds(s * sx + x, 1), :], 0.0)
            if fs is not None:
                sums = [sums[m] + fs * hm[m, x + 1, rows, :] for m in range(4)]
            solid = solid_s[x, rows, :] != 0
            inv = jnp.where(solid, 0.0, 1.0 / jnp.where(solid, 1.0, sums[0]))
            rho_s[x, rows, :] = sums[0]
            speed = []
            for c in range(3):
                u = sums[1 + c] * inv
                vel[c, x + 1, pl.ds(ROW + r, ROW), :] = u
                speed.append(u * u)
            peak = jnp.maximum(peak, speed[0] + speed[1] + speed[2])
        return peak

    def face_raw(s, r):
        return [
            shift_z(xr[s, j, pl.ds(ROW + r - CS[k][1], ROW), :], CS[k][2]) for j, k in enumerate(ACROSS_X[IN[s]])
        ]

    def face_rest(s, r):
        total, along, height = (xo_in[s, m, pl.ds(r, ROW), :] for m in range(3))
        b, d = x2_in[s, pl.ds(r, ROW), :], x2_in[s, pl.ds(sy + r, ROW), :]
        c, e = b - along, d - height
        return [total - ((b + c) + (d + e)), b, c, d, e]

    def face_reads(s, r, parts):
        for k, part in zip(ACROSS_X[IN[s]], parts):
            rd[k, face_x[s], pl.ds(r, ROW), :] = part

    def edge_reads():
        for s in (0, 1):
            for j, k in enumerate(ACROSS_Y[IN[s]]):
                for x in range(sx):
                    rd[k, x, pl.ds(edge_y[s], 1), :] = dr[j, pl.ds(s * sx + x, 1), :]

    def ghost_x(step, fs, s):
        own = pl.ds(2 * s, 2)
        for ys in (0, 1):
            c = 2 * s + ys
            j = 1 if OUT[s] > 0 else 2
            tu[0, pl.ds(c, 1), :] = yb_in[step, j, pl.ds(ys * sx + face_x[s], 1), :]
            j = 1 if OUT[ys] > 0 else 2
            if step == 0:
                tu[1, pl.ds(c, 1), :] = xr[s, j, pl.ds(ROW + edge_y[ys], 1), :]
            else:
                tu[1, pl.ds(c, 1), :] = x2_in[s, pl.ds(2 * sy + ys, 1), :]
        sums = [cm_in[step, m, own, :] for m in range(6)]
        over, up = tu[0, own, :], tu[1, own, :]
        sign = jnp.where(lax.broadcasted_iota(jnp.int32, (2, nz), 0) == 0, 1.0, -1.0)
        total = sums[0] + over
        for m, value in enumerate((total, sums[1] + OUT[s] * over, sign * total, sums[2])):
            ex[m, own, :] = value
        total = sums[3] + up
        for m, value in enumerate((total, IN[s] * total, sums[4] - sign * up, sums[5])):
            for ys in (0, 1):
                ey[m, pl.ds(ys * sx + face_x[s], 1), :] = value[ys : ys + 1, :]
        for r in range(0, sy, ROW):
            rows = pl.ds(r, ROW)
            share = ox[s, 0, rows, :]
            sums = [xm_in[step, s, m, rows, :] for m in range(4)]
            if step == 0:
                gfx[s, rows, :] = sums[0]
            fluid = gfx[s, rows, :] > 0.0
            sums[0] = sums[0] + share
            sums[1] = sums[1] - share if s == 0 else sums[1] + share
            sums[2] = sums[2] + ox[s, 1, rows, :]
            sums[3] = sums[3] + ox[s, 2, rows, :]
            for ys in edges_of(r):
                for m in range(4):
                    sums[m] = sums[m] + jnp.where(edge_row[ys], ex[m, pl.ds(s * 2 + ys, 1), :], 0.0)
            at = (0, sx + 1)[s]
            if fs is not None:
                sums = [sums[m] + fs * hm[m, at, rows, :] for m in range(4)]
            inv = jnp.where(fluid, 1.0 / jnp.where(fluid, sums[0], 1.0), 0.0)
            for c in range(3):
                vel[c, at, pl.ds(ROW + r, ROW), :] = sums[1 + c] * inv

    def ghost_y(step, fs):
        sums = [yb_in[step, 5 + m] for m in range(4)]
        if step == 0:
            gfy[...] = sums[0]
        fluid = gfy[...] > 0.0
        sums = [sums[m] + oy[m] + ey[m] for m in range(4)]
        if fs is not None:
            sums = [sums[m] + fs[0:1, :] * hmy[m] for m in range(4)]
        inv = jnp.where(fluid, 1.0 / jnp.where(fluid, sums[0], 1.0), 0.0)
        for c in range(3):
            u = sums[1 + c] * inv
            for s in (0, 1):
                for x in range(sx):
                    at = s * sx + x
                    vel[c, x + 1, pl.ds((ROW - 1, ROW + sy)[s], 1), :] = u[at : at + 1, :]

    def shift_heat(x, row, span):
        cells = hb[x, pl.ds(row, span), :]
        hzp[x, pl.ds(row, span), :] = shift_z(cells, 1)
        hzm[x, pl.ds(row, span), :] = shift_z(cells, -1)

    def heat_moments(x, row, span):
        cells = [
            (hzp[i, pl.ds(y, span), :], hzm[i, pl.ds(y, span), :])
            for i, y in ((x, row), (x - 1, row), (x + 1, row), (x, row - 1), (x, row + 1))
        ]
        diff = [a - b for a, b in cells]
        both = [a + b for a, b in cells]
        main, side = 3.0 * WEIGHT[5], 3.0 * WEIGHT[11]
        return (
            main * diff[0] + side * ((diff[1] + diff[2]) + (diff[3] + diff[4])),
            side * (diff[1] - diff[2]),
            side * (diff[3] - diff[4]),
            main * both[0] + side * ((both[1] + both[2]) + (both[3] + both[4])),
        )

    def heat_sums(columns):
        for x in columns:
            for r in range(0, sy, ROW):
                for m, value in enumerate(heat_moments(x + 1, ROW + r, ROW)):
                    hm[m, x, pl.ds(r, ROW), :] = value

    def near_heat():
        for x in range(1, sx + 3):
            for r in range(0, sy, ROW):
                shift_heat(x, ROW + r, ROW)
        for x in range(2, sx + 2):
            shift_heat(x, ROW - 2, 2)
            shift_heat(x, ROW + sy, 2)
        heat_sums(range(1, sx + 1))

    def far_heat():
        for x in (0, sx + 3):
            for r in range(0, sy, ROW):
                shift_heat(x, ROW + r, ROW)
        for x in (1, sx + 2):
            shift_heat(x, ROW - 1, 1)
            shift_heat(x, ROW + sy, 1)
        heat_sums((0, sx + 1))
        for s in (0, 1):
            for x in range(sx):
                for m, value in enumerate(heat_moments(x + 2, (ROW - 1, ROW + sy)[s], 1)):
                    hmy[m, pl.ds(s * sx + x, 1), :] = value

    def collided(tiles, fs, store):
        for x, r in tiles:
            mid = pl.ds(ROW + r, ROW)
            u = [vel[c, x + 1, mid, :] for c in range(3)]
            diff = []
            for a in range(3):
                diff.append(
                    (
                        vel[a, x + 2, mid, :] - vel[a, x, mid, :],
                        vel[a, x + 1, pl.ds(ROW + r + 1, ROW), :] - vel[a, x + 1, pl.ds(ROW + r - 1, ROW), :],
                        pltpu.roll(u[a], nz - 1, 1) - pltpu.roll(u[a], 1, 1),
                    )
                )
            own = diff[0][0] * diff[0][0] + diff[1][1] * diff[1][1] + diff[2][2] * diff[2][2]
            xy = diff[0][1] + diff[1][0]
            xz = diff[0][2] + diff[2][0]
            yz = diff[1][2] + diff[2][1]
            size = jnp.sqrt(0.5 * own + 0.25 * (xy * xy + xz * xz + yz * yz) + strain_floor)
            omega = 1.0 / (base_tau + 3.0 * smag_coef * size)
            solid = solid_s[x, pl.ds(r, ROW), :] != 0
            density = rho_s[x, pl.ds(r, ROW), :]
            still = 1.0 - 1.5 * (u[0] * u[0] + u[1] * u[1] + u[2] * u[2])
            reads = [rd[k, x, pl.ds(r, ROW), :] for k in range(19)]
            if fs is not None:
                for k in LIFTED:
                    cx, cy, cz = CS[k]
                    source = hzp if cz > 0 else hzm
                    reads[k] = reads[k] + (3.0 * WEIGHT[k] * cz) * (fs * source[x + 2 - cx, pl.ds(ROW + r - cy, ROW), :])
            scaled = {w: (w * density) * omega for w in sorted(set(WEIGHT))}
            keep = 1.0 - omega
            store(0, x, r, jnp.where(solid, reads[0], keep * reads[0] + scaled[WEIGHT[0]] * still))
            for k in range(1, 19, 2):
                other = OPP[k]
                project = None
                for c in range(3):
                    if CS[k][c]:
                        if project is None:
                            project = u[c] if CS[k][c] > 0 else -u[c]
                        else:
                            project = project + u[c] if CS[k][c] > 0 else project - u[c]
                even = still + 4.5 * project * project
                odd = 3.0 * project
                weight = scaled[WEIGHT[k]]
                store(k, x, r, jnp.where(solid, reads[other], keep * reads[k] + weight * (even + odd)))
                store(other, x, r, jnp.where(solid, reads[k], keep * reads[other] + weight * (even - odd)))

    load_h.wait()
    load_o.wait()
    load_t.wait()
    for x, r in blocks:
        rows = pl.ds(r, ROW)
        code = hl[x, rows, :]
        heat = jnp.zeros((ROW, nz), jnp.float32)
        for level in range(levels):
            heat = jnp.where(code == level, tb[level], heat)
        grid_y = gy * sy + r + row_no
        solid = (
            (ob[x, rows, :] == 1) | (grid_y == 0) | (grid_y == ngy * sy - 1) | first_lane | last_lane
        )
        solid_s[x, rows, :] = jnp.where(solid, 1, 0)
        hb[x + 2, pl.ds(ROW + r, ROW), :] = jnp.where(solid, 0.0, heat)

    neighbours = jnp.where(has_up, 1, 0) + jnp.where(has_down, 1, 0)
    sums_far, sums_near = send_x_sums(0)
    raw_far, raw_near = send_x_raw()
    neighbours = jnp.where(has_up, 1, 0) + jnp.where(has_down, 1, 0)
    sums_far, sums_near = send_x_sums(0)
    raw_far, raw_near = send_x_raw()
    load_p.wait()
    pack_x_raw()
    pl.semaphore_wait(barrier, partners)
    if by_word:
        for s in (0, 1):

            @pl.when(has_y[s])
            def _():
                greet(in_sem, gx, y_of[s])

    raw_far()
    own_sums(0, outer)
    sums_far()
    if by_word:
        for _, dy in column:
            other = lax.rem(gy + dy, ngy)

            @pl.when((other > gy + 1) | (other < gy - 1))
            def _():
                greet(col_sem, gx, other)

    pack_y_raw(0)
    send_y(0, raw_fields, yr_recv)
    corner_sums(0)
    own_sums(0, inner)
    send_y(0, sum_fields, ym_recv)
    if by_word:
        pl.semaphore_wait(in_sem, neighbours)
    send_corner_raw(0, (0, 1))
    send_corner_sums(0)
    if by_word:
        pl.semaphore_wait(col_sem, len(column) - neighbours)
    raw_near()
    sums_near()
    face_shares(0, (0, 1))
    edge_shares(0)
    send_heat()
    no_peak = jnp.zeros((ROW, nz), jnp.float32)
    await_y_raw(0)
    edge_moments(0)
    peak = velocity_pass(0, None, inner, no_peak)
    await_x_raw()
    finish_peak = spread_all(0, velocity_pass(0, None, outer, peak))
    edge_reads()
    await_y_sums(0)

    def store_st1(k, x, r, value):
        st1[k, x, pl.ds(ROW + r, ROW), :] = value

    def face(s):
        await_x_sums(0, s)
        ghost_x(0, None, s)
        ghost_y(0, None)
        collided([(x, r) for x, r in blocks if x == face_x[s]], None, store_st1)
        send_corner_raw(1, (s,))
        face_shares(1, (s,))
        send_x_shares(s)

    @pl.when(gx == ngx - 1)
    def _():
        face(1)
        face(0)

    @pl.when(gx != ngx - 1)
    def _():
        face(0)
        face(1)

    collided(inner, None, store_st1)
    pack_y_raw(1)
    send_y(1, raw_fields, yr_recv)
    own_sums(1, outer)
    for part in (*send_x_sums(1), *send_x_rest()):
        part()
    own_sums(1, inner)
    send_y(1, sum_fields, ym_recv)
    corner_sums(1)
    send_corner_sums(1)
    send_heat_x(1)
    edge_shares(1)
    await_heat()
    near_heat()
    fs = finish_peak()
    await_y_raw(1)
    edge_moments(1)
    peak = velocity_pass(1, fs, inner, no_peak)
    await_bytes(None, xo_in, xo_recv)
    finish_peak = spread_all(1, velocity_pass(1, fs, outer, peak))
    for x, r in blocks:
        for c in range(3):
            out_v[c, x, pl.ds(r, ROW), :] = vel[c, x + 1, pl.ds(ROW + r, ROW), :]
    await_bytes(None, hb.at[pl.ds(0, 2), own_y, :], hx_recv.at[1])
    far_heat()
    await_x_rest()
    for s in (0, 1):
        for r in range(0, sy, ROW):
            face_reads(s, r, face_rest(s, r))
    edge_reads()
    await_y_sums(1)
    for s in (0, 1):
        await_x_sums(1, s)
        ghost_x(1, fs, s)
    ghost_y(1, fs)

    def store_out(k, x, r, value):
        out_p[k, x, pl.ds(r, ROW), :] = value

    collided(blocks, fs, store_out)
    await_sends()
    fs = finish_peak()
    await_peak_sends()
    lift = {(x, r): fs * hb[x + 2, pl.ds(ROW + r, ROW), :] for x, r in blocks}
    for k in LIFTED:
        for x, r in blocks:
            rows = pl.ds(r, ROW)
            out_p[k, x, rows, :] = out_p[k, x, rows, :] + (3.0 * WEIGHT[k] * CS[k][2]) * lift[(x, r)]


def write_out(pops, vel, out_p, out_v, sems):
    copies = [
        pltpu.make_async_copy(pops, out_p, sems.at[0]),
        pltpu.make_async_copy(vel, out_v, sems.at[1]),
    ]
    for copy in copies:
        copy.start()
    for copy in copies:
        copy.wait()


def local(populations, heat_level, obstacle, heat_table):
    ngx = lax.axis_size("gx")
    ngy = lax.axis_size("gy")
    _, sx, sy, nz = populations.shape
    f32 = jnp.float32
    tall = sy + 2 * ROW
    dma = pltpu.SemaphoreType.DMA
    groups = peak_groups(ngx, ngy)
    phases = len(groups)
    vmem = pl.BlockSpec(memory_space=pltpu.VMEM)
    anywhere = pl.BlockSpec(memory_space=pltpu.HBM)
    shapes = (
        jax.ShapeDtypeStruct(populations.shape, f32),
        jax.ShapeDtypeStruct((3, sx, sy, nz), f32),
    )

    def floats(*shape):
        return pltpu.VMEM(shape, f32)

    def ints(*shape):
        return pltpu.VMEM(shape, jnp.int32)

    pops, velocity = pl.pallas_call(
        functools.partial(kernel, ngx, ngy),
        out_shape=shapes,
        in_specs=[anywhere] * 4,
        out_specs=[vmem] * 2,
        scratch_shapes=[
            floats(19, sx, tall, nz),
            floats(19, sx, tall, nz),
            floats(19, sx, sy, nz),
            floats(4, sx, sy, nz),
            floats(sx, sy, nz),
            floats(3, sx + 2, tall, nz),
            ints(sx, sy, nz),
            ints(sx, sy, nz),
            pltpu.SMEM(heat_table.shape, f32),
            ints(sx, sy, nz),
            floats(sx + 4, tall, nz),
            floats(sx + 4, tall, nz),
            floats(sx + 4, tall, nz),
            floats(4, sx + 2, sy, nz),
            floats(4, 2 * sx, nz),
            floats(2, 5, tall, nz),
            floats(2, 5, sy, nz),
            floats(STEPS, 2, 4, sy, nz),
            floats(STEPS, 2, 4, sy, nz),
            floats(STEPS, 9, 2 * sx, nz),
            floats(STEPS, 9, 2 * sx, nz),
            floats(8, ROW, nz),
            floats(STEPS, 6, ROW, nz),
            floats(STEPS, ROW, nz),
            floats(STEPS, 6, ROW, nz),
            floats(2, 3, sy, nz),
            floats(2, 2 * sy + ROW, nz),
            floats(2, 3, sy, nz),
            floats(2, 2 * sy + ROW, nz),
            floats(4, 2 * sx, nz),
            floats(5, 2 * sx, nz),
            floats(4, 2 * sx, nz),
            floats(2, ROW, nz),
            floats(4, ROW, nz),
            floats(4, 2 * sx, nz),
            floats(2, sy, nz),
            floats(2 * sx, nz),
            floats(8 * ROW, nz),
            floats(STEPS, phases, 1, nz),
            *[floats(STEPS, -(-len(group) // ROW) * ROW, nz) for group in groups],
            dma((4,)),
            pltpu.SemaphoreType.REGULAR,
            pltpu.SemaphoreType.REGULAR,
            dma,
            dma((2,)),
            dma((STEPS,)),
            dma((STEPS, 2)),
            dma,
            dma((STEPS, 2)),
            dma((STEPS, 2)),
            dma((STEPS, 4)),
            dma((2,)),
            dma((2,)),
            dma((phases,)),
            dma((STEPS, phases)),
        ],
        compiler_params=pltpu.CompilerParams(
            collective_id=0, has_side_effects=True, vmem_limit_bytes=24 * 1024 * 1024
        ),
        name="lattice_steps",
    )(*[pltpu.with_memory_space_constraint(a, pltpu.HBM) for a in (populations, heat_level, obstacle, heat_table)])
    return pl.pallas_call(
        write_out,
        out_shape=shapes,
        in_specs=[vmem] * 2,
        out_specs=[anywhere] * 2,
        scratch_shapes=[dma((2,))],
        compiler_params=pltpu.CompilerParams(vmem_limit_bytes=8 * 1024 * 1024),
        name="write_out",
    )(pops, velocity)


def solution(mesh):
    return jax.shard_map(
        local,
        mesh=mesh,
        in_specs=(
            P(None, ("member", "gx"), "gy", None),
            P(("member", "gx"), "gy", None),
            P(("member", "gx"), "gy", None),
            P(),
        ),
        out_specs=(P(None, ("member", "gx"), "gy", None), P(None, ("member", "gx"), "gy", None)),
        check_vma=False,
    )
```

```python
import functools

import jax
import jax.numpy as jnp
import numpy as np
from jax import lax
from jax.experimental import pallas as pl
from jax.experimental.pallas import tpu as pltpu
from jax.sharding import PartitionSpec as P

STEPS = 2
ROW = 8

lattice = np.array(
    [
        [0, 0, 0],
        [1, 0, 0],
        [-1, 0, 0],
        [0, 1, 0],
        [0, -1, 0],
        [0, 0, 1],
        [0, 0, -1],
        [1, 1, 0],
        [-1, -1, 0],
        [1, -1, 0],
        [-1, 1, 0],
        [1, 0, 1],
        [-1, 0, -1],
        [1, 0, -1],
        [-1, 0, 1],
        [0, 1, 1],
        [0, -1, -1],
        [0, 1, -1],
        [0, -1, 1],
    ]
)
CS = [tuple(int(c) for c in row) for row in lattice]
NUMBER = {c: k for k, c in enumerate(CS)}
WEIGHT = [1.0 / 3.0] + [1.0 / 18.0] * 6 + [1.0 / 36.0] * 12
OPP = [0, 2, 1, 4, 3, 6, 5, 8, 7, 10, 9, 12, 11, 14, 13, 16, 15, 18, 17]
base_tau = 0.52
smag_coef = 0.04
speed_cap = 0.1
strain_floor = 1e-06
LIFTED = [k for k in range(19) if CS[k][2] != 0]
ACROSS_X = {c: [NUMBER[(c, 0, 0)], NUMBER[(c, 1, 0)], NUMBER[(c, -1, 0)], NUMBER[(c, 0, 1)], NUMBER[(c, 0, -1)]] for c in (1, -1)}
ACROSS_Y = {c: [NUMBER[(0, c, 0)], NUMBER[(1, c, 0)], NUMBER[(-1, c, 0)], NUMBER[(0, c, 1)], NUMBER[(0, c, -1)]] for c in (1, -1)}
OUT = (-1, 1)
IN = (1, -1)


def tree_sum(items):
    items = list(items)
    while len(items) > 1:
        items = [items[i] + items[i + 1] if i + 1 < len(items) else items[i] for i in range(0, len(items), 2)]
    return items[0]


def peak_groups(ngx, ngy):
    if ngx * ngy <= 64:
        return [[(dx, dy) for dx in range(ngx) for dy in range(ngy) if dx or dy]]
    return [[(0, dy) for dy in range(1, ngy)], [(dx, 0) for dx in range(1, ngx)]]


def kernel(
    ngx, ngy,
    pops, heat_level, obstacle, table,
    out_p, out_v,
    st0, st1, rd, ms, rho_s, vel, hl, ob, tb, solid_s,
    hb, hzp, hzm, hm, hmy,
    xr, xp, xm_out, xm_in, yb_out, yb_in, cg, cm_out, cr_in, cm_in,
    ox, ox2, xo_in, x2_in, oy, dr, dm, tu, ex, ey, gfx, gfy, flat, pm_src, *rest,
):
    (*pm_bufs, load_sem, in_sem, col_sem, x_send, y_send, xr_recv, xm_recv, xo_recv, yr_recv, ym_recv,
     cm_recv, hx_recv, hy_recv, p_send, p_recv) = rest
    _, sx, sy, nz = pops.shape
    levels = table.shape[0]
    gx = lax.axis_index("gx")
    gy = lax.axis_index("gy")
    has_up = gy < ngy - 1
    has_down = gy > 0
    right = lax.rem(gx + 1, ngx)
    left = lax.rem(gx + ngx - 1, ngx)
    own_y = pl.ds(ROW, sy)
    face_x = (0, sx - 1)
    edge_y = (0, sy - 1)
    x_of = (left, right)
    y_of = (gy - 1, gy + 1)
    has_y = (has_down, has_up)

    barrier = pltpu.get_barrier_semaphore()

    def greet(sem, x, y):
        pl.semaphore_signal(sem, inc=1, device_id={"gx": x, "gy": y}, device_id_type=pl.DeviceIdType.MESH)

    groups = peak_groups(ngx, ngy)
    beside = sorted({1, ngx - 1} - {0})
    column = [(0, dy) for dy in range(1, ngy)]
    by_word = len(groups) == 1 and ngx <= 5
    greeted = [(dx, 0) for dx in beside] + column if by_word else [place for group in groups for place in group]
    partners = len(greeted)
    for dx, dy in greeted:
        greet(barrier, lax.rem(gx + dx, ngx), lax.rem(gy + dy, ngy))
    if len(groups) > 1:
        partners = partners + 2 * (jnp.where(has_up, 1, 0) + jnp.where(has_down, 1, 0))
        for s in (0, 1):

            @pl.when(has_y[s])
            def _():
                greet(barrier, right, y_of[s])
                greet(barrier, left, y_of[s])

    load_p = pltpu.make_async_copy(pops, st0.at[:, :, own_y, :], load_sem.at[0])
    load_h = pltpu.make_async_copy(heat_level, hl, load_sem.at[1])
    load_o = pltpu.make_async_copy(obstacle, ob, load_sem.at[2])
    load_t = pltpu.make_async_copy(table, tb, load_sem.at[3])
    load_p.start()
    load_h.start()
    load_o.start()
    load_t.start()

    def zeros(ref, *index):
        part = ref.at[index]
        part[...] = jnp.zeros(part.shape, jnp.float32)

    every = slice(None)
    for row in (ROW - 1, ROW + sy):
        for st in (st0, st1):
            for c in (1, -1):
                for k in ACROSS_Y[c]:
                    zeros(st, k, every, pl.ds(row, 1), every)
        zeros(xr, every, every, pl.ds(row, 1), every)
    for ref in (cg, tu, ey):
        ref[...] = jnp.zeros(ref.shape, jnp.float32)

    for s in (0, 1):

        @pl.when(jnp.logical_not(has_y[s]))
        def _():
            zeros(yb_in, every, every, pl.ds(s * sx, sx), every)
            for xs in (0, 1):
                zeros(cr_in, every, pl.ds(xs * 2 + s, 1), every)
                zeros(cm_in, every, every, pl.ds(xs * 2 + s, 1), every)
            zeros(hb, every, pl.ds((ROW - 2, ROW + sy)[s], 2), every)

    def guarded(cond, fn):
        if cond is None:
            fn()
        else:
            pl.when(cond)(fn)

    def send(cond, pairs, send_sem, recv_sem, x, y):
        def go():
            for src, dst in pairs:
                pltpu.make_async_remote_copy(
                    src_ref=src, dst_ref=dst, send_sem=send_sem, recv_sem=recv_sem,
                    device_id={"gx": x, "gy": y}, device_id_type=pl.DeviceIdType.MESH,
                ).start()

        guarded(cond, go)

    def await_bytes(cond, view, sem):
        guarded(cond, lambda: pltpu.make_async_copy(view, view, sem).wait())

    states = (st0, st1)
    corners = [(xs, ys) for xs in (0, 1) for ys in (0, 1)]
    raw_fields = pl.ds(0, 5)
    sum_fields = pl.ds(5, 4)

    at_end = (gx == 0, gx == ngx - 1)

    def along_x(pairs_of, sem_of):
        def far():
            for s in (0, 1):
                send(at_end[s], pairs_of(s), x_send, sem_of(s), x_of[s], gy)

        def near():
            for s in (0, 1):
                send(jnp.logical_not(at_end[s]), pairs_of(s), x_send, sem_of(s), x_of[s], gy)

        return far, near

    def send_x_raw():
        return along_x(
            lambda s: [(xp.at[s], xr.at[1 - s, :, own_y, :])],
            lambda s: xr_recv.at[0],
        )

    def send_x_sums(step):
        return along_x(lambda s: [(xm_out.at[step, s], xm_in.at[step, 1 - s])], lambda s: xm_recv.at[step, 1 - s])

    rest_rows = pl.ds(0, 2 * sy + 2)

    def send_x_shares(s):
        send(None, [(ox.at[s], xo_in.at[1 - s])], x_send, xo_recv, x_of[s], gy)

    def send_x_rest():
        return along_x(lambda s: [(ox2.at[s, rest_rows, :], x2_in.at[1 - s, rest_rows, :])], lambda s: xr_recv.at[1])

    def send_heat_x(layer):
        src, dst = ((2, sx + 1), (sx + 2, 1)) if layer == 0 else ((3, sx), (sx + 3, 0))
        for s in (0, 1):
            send(None, [(hb.at[src[s], own_y, :], hb.at[dst[s], own_y, :])], x_send, hx_recv.at[layer], x_of[s], gy)

    def send_heat():
        send_heat_x(0)
        for s in (0, 1):
            src = hb.at[pl.ds(2, sx), pl.ds((ROW, ROW + sy - 2)[s], 2), :]
            dst = hb.at[pl.ds(2, sx), pl.ds((ROW + sy, ROW - 2)[s], 2), :]
            send(has_y[s], [(src, dst)], y_send.at[s], hy_recv.at[1 - s], gx, y_of[s])
        to_corners(
            lambda c, xs, ys: (
                hb.at[2 + face_x[xs], pl.ds(ROW + edge_y[ys], 1), :],
                hb.at[(sx + 2, 1)[xs], pl.ds((ROW + sy, ROW - 1)[ys], 1), :],
            ),
            lambda c: hy_recv.at[c % 2],
        )

    def send_y(step, fields, recv_sem):
        for s in (0, 1):
            src = yb_out.at[step, fields, pl.ds(s * sx, sx), :]
            dst = yb_in.at[step, fields, pl.ds((1 - s) * sx, sx), :]
            send(has_y[s], [(src, dst)], y_send.at[s], recv_sem.at[step, 1 - s], gx, y_of[s])

    def to_corners(pair_of, sem_of, sides=(0, 1)):
        for c, (xs, ys) in enumerate(corners):
            if xs in sides:
                send(has_y[ys], [pair_of(c, xs, ys)], y_send.at[ys], sem_of(3 - c), x_of[xs], y_of[ys])

    def send_corner_raw(step, sides):
        st = states[step]

        def pair(c, xs, ys):
            k = NUMBER[(OUT[xs], OUT[ys], 0)]
            return st.at[k, face_x[xs], pl.ds(ROW + edge_y[ys], 1), :], cr_in.at[step, pl.ds(3 - c, 1), :]

        to_corners(pair, lambda c: yr_recv.at[step, c % 2], sides)

    def send_corner_sums(step):
        to_corners(
            lambda c, xs, ys: (cm_out.at[step, :, pl.ds(c, 1), :], cm_in.at[step, :, pl.ds(3 - c, 1), :]),
            lambda c: cm_recv.at[step, c],
        )

    def await_y_raw(step):
        for s in (0, 1):
            await_bytes(has_y[s], flat.at[pl.ds(0, 5 * sx + 2), :], yr_recv.at[step, s])

    def await_x_raw():
        await_bytes(None, xr.at[:, :, own_y, :], xr_recv.at[0])

    def await_x_rest():
        await_bytes(None, x2_in.at[:, rest_rows, :], xr_recv.at[1])

    def await_y_sums(step):
        for s in (0, 1):
            await_bytes(has_y[s], yb_in.at[step, sum_fields, pl.ds(s * sx, sx), :], ym_recv.at[step, s])

    def await_x_sums(step, s):
        for ys in (0, 1):
            await_bytes(has_y[ys], cm_in.at[step, :, pl.ds(2 * s + ys, 1), :], cm_recv.at[step, 2 * s + ys])
        await_bytes(None, xm_in.at[step, s], xm_recv.at[step, s])

    def await_heat():
        for s in (0, 1):
            await_bytes(has_y[s], flat.at[pl.ds(0, 2 * sx + 2), :], hy_recv.at[s])
        await_bytes(None, hb.at[pl.ds(0, 2), own_y, :], hx_recv.at[0])

    def await_sends():
        for view in (xp, xm_out, ox, ox2.at[:, rest_rows, :], hb.at[pl.ds(0, 4), own_y, :]):
            await_bytes(None, view, x_send)
        for s in (0, 1):
            for view in (yb_out.at[:, :, pl.ds(0, sx), :], flat.at[pl.ds(0, 2 * sx + STEPS * 14 + 2), :]):
                await_bytes(has_y[s], view, y_send.at[s])

    def await_peak_sends():
        for phase, group in enumerate(groups):
            for step in range(STEPS):
                await_bytes(None, pm_bufs[phase].at[step, pl.ds(0, len(group)), :], p_send.at[phase])

    def spread(step, phase, value):
        group = peak_groups(ngx, ngy)[phase]
        count = len(group)
        buf = pm_bufs[phase]
        pm_src[step, phase] = value
        for d, (dx, dy) in sorted(enumerate(group, 1), key=lambda item: item[1][0] in (0, ngx // 2)):
            place = {"gx": lax.rem(gx + dx, ngx), "gy": lax.rem(gy + dy, ngy)}
            pltpu.make_async_remote_copy(
                src_ref=pm_src.at[step, phase],
                dst_ref=buf.at[step, pl.ds(d - 1, 1), :],
                send_sem=p_send.at[phase],
                recv_sem=p_recv.at[step, phase],
                device_id=place,
                device_id_type=pl.DeviceIdType.MESH,
            ).start()
        view = buf.at[step, pl.ds(0, count), :]

        def wait():
            await_bytes(None, view, p_recv.at[step, phase])
            return jnp.maximum(value, jnp.max(buf[step, pl.ds(0, count), :], axis=0, keepdims=True))

        return wait

    def spread_all(step, tile):
        wait = spread(step, 0, jnp.max(tile, axis=0, keepdims=True))

        def finish():
            best = wait()
            for phase in range(1, len(pm_bufs)):
                best = spread(step, phase, best)()
            peak = jnp.broadcast_to(jnp.max(best, axis=1, keepdims=True), (ROW, nz))
            return speed_cap * lax.rsqrt(speed_cap * speed_cap + peak)

        return finish

    blocks = [(x, r) for x in range(sx) for r in range(0, sy, ROW)]
    outer = [(x, r) for x, r in blocks if x in face_x]
    inner = [(x, r) for x, r in blocks if x not in face_x]
    lane = lax.broadcasted_iota(jnp.int32, (ROW, nz), 1)
    row_no = lax.broadcasted_iota(jnp.int32, (ROW, nz), 0)
    first_lane = lane == 0
    last_lane = lane == nz - 1
    edge_row = (row_no == 0, row_no == ROW - 1)
    pack_row = lax.broadcasted_iota(jnp.int32, (2 * sx, nz), 0)
    pack_sign = jnp.where(pack_row < sx, 1.0, -1.0)
    corner_x = jnp.where(row_no < 2, 1.0, -1.0)
    corner_y = jnp.where(lax.rem(row_no, 2) == 0, 1.0, -1.0)

    def shift_z(cells, cz):
        if not cz:
            return cells
        at = lax.broadcasted_iota(jnp.int32, cells.shape, 1)
        return jnp.where(at == (0 if cz > 0 else nz - 1), 0.0, pltpu.roll(cells, cz % nz, 1))

    def edges_of(r):
        return [s for s in (0, 1) if r == (0, sy - ROW)[s]]

    def own_sums(step, tiles):
        st = states[step]
        for x, r in tiles:
            rows = pl.ds(r, ROW)
            reads = {}
            for k, (cx, cy, cz) in enumerate(CS):
                if 0 <= x - cx < sx:
                    reads[k] = shift_z(st[k, x - cx, pl.ds(ROW + r - cy, ROW), :], cz)
                    rd[k, x, rows, :] = reads[k]
            sums = [tree_sum(list(reads.values()))]
            for c in range(3):
                plus = [reads[k] for k in reads if CS[k][c] > 0]
                minus = [reads[k] for k in reads if CS[k][c] < 0]
                if plus and minus:
                    sums.append(tree_sum(plus) - tree_sum(minus))
                else:
                    sums.append(tree_sum(plus) if plus else -tree_sum(minus))
            for m in range(4):
                ms[m, x, rows, :] = sums[m]
            sums[0] = jnp.where(solid_s[x, rows, :] != 0, 0.0, sums[0])
            for s in (0, 1):
                if x == face_x[s]:
                    for m in range(4):
                        xm_out[step, s, m, rows, :] = sums[m]
                if s in edges_of(r):
                    at = (0, ROW - 1)[s]
                    for m in range(4):
                        yb_out[step, 5 + m, pl.ds(s * sx + x, 1), :] = sums[m][at : at + 1, :]

    def pack_x_raw():
        for s in (0, 1):
            for j, k in enumerate(ACROSS_X[OUT[s]]):
                xp[s, j] = st0[k, face_x[s], own_y, :]

    def pack_y_raw(step):
        st = states[step]
        for s in (0, 1):
            for j, k in enumerate(ACROSS_Y[OUT[s]]):
                for x in range(sx):
                    yb_out[step, j, pl.ds(s * sx + x, 1), :] = st[k, x, pl.ds(ROW + edge_y[s], 1), :]

    def corner_sums(step):
        st = states[step]
        for c, (xs, ys) in enumerate(corners):
            dx, dy = OUT[xs], OUT[ys]
            fx, fy = face_x[xs], edge_y[ys]
            places = [
                ((0, dy, 0), fx, fy), ((0, dy, 1), fx, fy), ((0, dy, -1), fx, fy), ((dx, dy, 0), fx - dx, fy),
                ((dx, 0, 0), fx, fy), ((dx, 0, 1), fx, fy), ((dx, 0, -1), fx, fy), ((dx, dy, 0), fx, fy - dy),
            ]
            for f, (direction, x, y) in enumerate(places):
                cg[f, pl.ds(c, 1), :] = st[NUMBER[direction], x, pl.ds(ROW + y, 1), :]
        for half, sign in ((0, -corner_x), (1, -corner_y)):
            a, b, d, e = (cg[4 * half + f] for f in range(4))
            b, d = shift_z(b, 1), shift_z(d, -1)
            cm_out[step, 3 * half + 0] = (a + b) + (d + e)
            cm_out[step, 3 * half + 1] = sign * e
            cm_out[step, 3 * half + 2] = b - d

    def packed(fields, fill):
        plus = jnp.where(lax.rem(pack_row, sx) == 0, 0.0, pltpu.roll(fields[1], 1, 0))
        minus = jnp.where(lax.rem(pack_row, sx) == sx - 1, 0.0, pltpu.roll(fields[2], 2 * sx - 1, 0))
        if fill is not None:
            for ys in (0, 1):
                plus = jnp.where(pack_row == ys * sx, fill(ys), plus)
                minus = jnp.where(pack_row == ys * sx + sx - 1, fill(2 + ys), minus)
        return [fields[0], plus, minus, shift_z(fields[3], 1), shift_z(fields[4], -1)]

    def face_shares(step, sides):
        st = states[step]
        for s in sides:
            for r in range(0, sy, ROW):
                ks = ACROSS_X[OUT[s]]
                a, b, c, d, e = (st[k, face_x[s], pl.ds(ROW + r - CS[k][1], ROW), :] for k in ks)
                d, e = shift_z(d, 1), shift_z(e, -1)
                ox[s, 0, pl.ds(r, ROW), :] = ((a + b) + (c + d)) + e
                ox[s, 1, pl.ds(r, ROW), :] = b - c
                ox[s, 2, pl.ds(r, ROW), :] = d - e
                if step == 1:
                    ox2[s, pl.ds(r, ROW), :] = b
                    ox2[s, pl.ds(sy + r, ROW), :] = d
            if step == 1:
                ox2[s, pl.ds(2 * sy, 1), :] = st[ACROSS_X[OUT[s]][2], face_x[s], pl.ds(ROW, 1), :]
                ox2[s, pl.ds(2 * sy + 1, 1), :] = st[ACROSS_X[OUT[s]][1], face_x[s], pl.ds(ROW + sy - 1, 1), :]

    def edge_shares(step):
        a, b, c, d, e = packed([yb_out[step, j] for j in range(5)], None)
        total = ((a + b) + (c + d)) + e
        oy[0] = total
        oy[1] = b - c
        oy[2] = -pack_sign * total
        oy[3] = d - e

    def edge_moments(step):
        fields = packed([yb_in[step, j] for j in range(5)], lambda c: cr_in[step, pl.ds(c, 1), :])
        for j in range(5):
            dr[j] = fields[j]
        a, b, c, d, e = fields
        total = ((a + b) + (c + d)) + e
        for m, value in enumerate((total, b - c, pack_sign * total, d - e)):
            dm[m] = value

    def velocity_pass(step, fs, tiles, peak):
        for x, r in tiles:
            rows = pl.ds(r, ROW)
            sums = [ms[m, x, rows, :] for m in range(4)]
            for s in (0, 1):
                if x == face_x[s]:
                    if step == 0:
                        parts = face_raw(s, r)
                        shares = tree_sum(parts), parts[1] - parts[2], parts[3] - parts[4]
                        face_reads(s, r, parts)
                    else:
                        shares = [xo_in[s, m, rows, :] for m in range(3)]
                    sums[0] = sums[0] + shares[0]
                    sums[1] = sums[1] + shares[0] if s == 0 else sums[1] - shares[0]
                    sums[2] = sums[2] + shares[1]
                    sums[3] = sums[3] + shares[2]
            for s in edges_of(r):
                for m in range(4):
                    sums[m] = sums[m] + jnp.where(edge_row[s], dm[m, pl.ds(s * sx + x, 1), :], 0.0)
            if fs is not None:
                sums = [sums[m] + fs * hm[m, x + 1, rows, :] for m in range(4)]
            solid = solid_s[x, rows, :] != 0
            inv = jnp.where(solid, 0.0, 1.0 / jnp.where(solid, 1.0, sums[0]))
            rho_s[x, rows, :] = sums[0]
            speed = []
            for c in range(3):
                u = sums[1 + c] * inv
                vel[c, x + 1, pl.ds(ROW + r, ROW), :] = u
                speed.append(u * u)
            peak = jnp.maximum(peak, speed[0] + speed[1] + speed[2])
        return peak

    def face_raw(s, r):
        return [
            shift_z(xr[s, j, pl.ds(ROW + r - CS[k][1], ROW), :], CS[k][2]) for j, k in enumerate(ACROSS_X[IN[s]])
        ]

    def face_rest(s, r):
        total, along, height = (xo_in[s, m, pl.ds(r, ROW), :] for m in range(3))
        b, d = x2_in[s, pl.ds(r, ROW), :], x2_in[s, pl.ds(sy + r, ROW), :]
        c, e = b - along, d - height
        return [total - ((b + c) + (d + e)), b, c, d, e]

    def face_reads(s, r, parts):
        for k, part in zip(ACROSS_X[IN[s]], parts):
            rd[k, face_x[s], pl.ds(r, ROW), :] = part

    def edge_reads():
        for s in (0, 1):
            for j, k in enumerate(ACROSS_Y[IN[s]]):
                for x in range(sx):
                    rd[k, x, pl.ds(edge_y[s], 1), :] = dr[j, pl.ds(s * sx + x, 1), :]

    def ghost_x(step, fs, s):
        own = pl.ds(2 * s, 2)
        for ys in (0, 1):
            c = 2 * s + ys
            j = 1 if OUT[s] > 0 else 2
            tu[0, pl.ds(c, 1), :] = yb_in[step, j, pl.ds(ys * sx + face_x[s], 1), :]
            j = 1 if OUT[ys] > 0 else 2
            if step == 0:
                tu[1, pl.ds(c, 1), :] = xr[s, j, pl.ds(ROW + edge_y[ys], 1), :]
            else:
                tu[1, pl.ds(c, 1), :] = x2_in[s, pl.ds(2 * sy + ys, 1), :]
        sums = [cm_in[step, m, own, :] for m in range(6)]
        over, up = tu[0, own, :], tu[1, own, :]
        sign = jnp.where(lax.broadcasted_iota(jnp.int32, (2, nz), 0) == 0, 1.0, -1.0)
        total = sums[0] + over
        for m, value in enumerate((total, sums[1] + OUT[s] * over, sign * total, sums[2])):
            ex[m, own, :] = value
        total = sums[3] + up
        for m, value in enumerate((total, IN[s] * total, sums[4] - sign * up, sums[5])):
            for ys in (0, 1):
                ey[m, pl.ds(ys * sx + face_x[s], 1), :] = value[ys : ys + 1, :]
        for r in range(0, sy, ROW):
            rows = pl.ds(r, ROW)
            share = ox[s, 0, rows, :]
            sums = [xm_in[step, s, m, rows, :] for m in range(4)]
            if step == 0:
                gfx[s, rows, :] = sums[0]
            fluid = gfx[s, rows, :] > 0.0
            sums[0] = sums[0] + share
            sums[1] = sums[1] - share if s == 0 else sums[1] + share
            sums[2] = sums[2] + ox[s, 1, rows, :]
            sums[3] = sums[3] + ox[s, 2, rows, :]
            for ys in edges_of(r):
                for m in range(4):
                    sums[m] = sums[m] + jnp.where(edge_row[ys], ex[m, pl.ds(s * 2 + ys, 1), :], 0.0)
            at = (0, sx + 1)[s]
            if fs is not None:
                sums = [sums[m] + fs * hm[m, at, rows, :] for m in range(4)]
            inv = jnp.where(fluid, 1.0 / jnp.where(fluid, sums[0], 1.0), 0.0)
            for c in range(3):
                vel[c, at, pl.ds(ROW + r, ROW), :] = sums[1 + c] * inv

    def ghost_y(step, fs):
        sums = [yb_in[step, 5 + m] for m in range(4)]
        if step == 0:
            gfy[...] = sums[0]
        fluid = gfy[...] > 0.0
        sums = [sums[m] + oy[m] + ey[m] for m in range(4)]
        if fs is not None:
            sums = [sums[m] + fs[0:1, :] * hmy[m] for m in range(4)]
        inv = jnp.where(fluid, 1.0 / jnp.where(fluid, sums[0], 1.0), 0.0)
        for c in range(3):
            u = sums[1 + c] * inv
            for s in (0, 1):
                for x in range(sx):
                    at = s * sx + x
                    vel[c, x + 1, pl.ds((ROW - 1, ROW + sy)[s], 1), :] = u[at : at + 1, :]

    def shift_heat(x, row, span):
        cells = hb[x, pl.ds(row, span), :]
        hzp[x, pl.ds(row, span), :] = shift_z(cells, 1)
        hzm[x, pl.ds(row, span), :] = shift_z(cells, -1)

    def heat_moments(x, row, span):
        cells = [
            (hzp[i, pl.ds(y, span), :], hzm[i, pl.ds(y, span), :])
            for i, y in ((x, row), (x - 1, row), (x + 1, row), (x, row - 1), (x, row + 1))
        ]
        diff = [a - b for a, b in cells]
        both = [a + b for a, b in cells]
        main, side = 3.0 * WEIGHT[5], 3.0 * WEIGHT[11]
        return (
            main * diff[0] + side * ((diff[1] + diff[2]) + (diff[3] + diff[4])),
            side * (diff[1] - diff[2]),
            side * (diff[3] - diff[4]),
            main * both[0] + side * ((both[1] + both[2]) + (both[3] + both[4])),
        )

    def heat_sums(columns):
        for x in columns:
            for r in range(0, sy, ROW):
                for m, value in enumerate(heat_moments(x + 1, ROW + r, ROW)):
                    hm[m, x, pl.ds(r, ROW), :] = value

    def near_heat():
        for x in range(1, sx + 3):
            for r in range(0, sy, ROW):
                shift_heat(x, ROW + r, ROW)
        for x in range(2, sx + 2):
            shift_heat(x, ROW - 2, 2)
            shift_heat(x, ROW + sy, 2)
        heat_sums(range(1, sx + 1))

    def far_heat():
        for x in (0, sx + 3):
            for r in range(0, sy, ROW):
                shift_heat(x, ROW + r, ROW)
        for x in (1, sx + 2):
            shift_heat(x, ROW - 1, 1)
            shift_heat(x, ROW + sy, 1)
        heat_sums((0, sx + 1))
        for s in (0, 1):
            for x in range(sx):
                for m, value in enumerate(heat_moments(x + 2, (ROW - 1, ROW + sy)[s], 1)):
                    hmy[m, pl.ds(s * sx + x, 1), :] = value

    def collided(tiles, fs, store):
        for x, r in tiles:
            mid = pl.ds(ROW + r, ROW)
            u = [vel[c, x + 1, mid, :] for c in range(3)]
            diff = []
            for a in range(3):
                diff.append(
                    (
                        vel[a, x + 2, mid, :] - vel[a, x, mid, :],
                        vel[a, x + 1, pl.ds(ROW + r + 1, ROW), :] - vel[a, x + 1, pl.ds(ROW + r - 1, ROW), :],
                        pltpu.roll(u[a], nz - 1, 1) - pltpu.roll(u[a], 1, 1),
                    )
                )
            own = diff[0][0] * diff[0][0] + diff[1][1] * diff[1][1] + diff[2][2] * diff[2][2]
            xy = diff[0][1] + diff[1][0]
            xz = diff[0][2] + diff[2][0]
            yz = diff[1][2] + diff[2][1]
            size = jnp.sqrt(0.5 * own + 0.25 * (xy * xy + xz * xz + yz * yz) + strain_floor)
            omega = 1.0 / (base_tau + 3.0 * smag_coef * size)
            solid = solid_s[x, pl.ds(r, ROW), :] != 0
            density = rho_s[x, pl.ds(r, ROW), :]
            still = 1.0 - 1.5 * (u[0] * u[0] + u[1] * u[1] + u[2] * u[2])
            reads = [rd[k, x, pl.ds(r, ROW), :] for k in range(19)]
            if fs is not None:
                for k in LIFTED:
                    cx, cy, cz = CS[k]
                    source = hzp if cz > 0 else hzm
                    reads[k] = reads[k] + (3.0 * WEIGHT[k] * cz) * (fs * source[x + 2 - cx, pl.ds(ROW + r - cy, ROW), :])
            scaled = {w: (w * density) * omega for w in sorted(set(WEIGHT))}
            keep = 1.0 - omega
            store(0, x, r, jnp.where(solid, reads[0], keep * reads[0] + scaled[WEIGHT[0]] * still))
            for k in range(1, 19, 2):
                other = OPP[k]
                project = None
                for c in range(3):
                    if CS[k][c]:
                        if project is None:
                            project = u[c] if CS[k][c] > 0 else -u[c]
                        else:
                            project = project + u[c] if CS[k][c] > 0 else project - u[c]
                even = still + 4.5 * project * project
                odd = 3.0 * project
                weight = scaled[WEIGHT[k]]
                store(k, x, r, jnp.where(solid, reads[other], keep * reads[k] + weight * (even + odd)))
                store(other, x, r, jnp.where(solid, reads[k], keep * reads[other] + weight * (even - odd)))

    load_h.wait()
    load_o.wait()
    load_t.wait()
    for x, r in blocks:
        rows = pl.ds(r, ROW)
        code = hl[x, rows, :]
        heat = jnp.zeros((ROW, nz), jnp.float32)
        for level in range(levels):
            heat = jnp.where(code == level, tb[level], heat)
        grid_y = gy * sy + r + row_no
        solid = (
            (ob[x, rows, :] == 1) | (grid_y == 0) | (grid_y == ngy * sy - 1) | first_lane | last_lane
        )
        solid_s[x, rows, :] = jnp.where(solid, 1, 0)
        hb[x + 2, pl.ds(ROW + r, ROW), :] = jnp.where(solid, 0.0, heat)

    neighbours = jnp.where(has_up, 1, 0) + jnp.where(has_down, 1, 0)
    sums_far, sums_near = send_x_sums(0)
    raw_far, raw_near = send_x_raw()
    neighbours = jnp.where(has_up, 1, 0) + jnp.where(has_down, 1, 0)
    sums_far, sums_near = send_x_sums(0)
    raw_far, raw_near = send_x_raw()
    load_p.wait()
    pack_x_raw()
    pl.semaphore_wait(barrier, partners)
    if by_word:
        for s in (0, 1):

            @pl.when(has_y[s])
            def _():
                greet(in_sem, gx, y_of[s])

    raw_far()
    own_sums(0, outer)
    sums_far()
    if by_word:
        for _, dy in column:
            other = lax.rem(gy + dy, ngy)

            @pl.when((other > gy + 1) | (other < gy - 1))
            def _():
                greet(col_sem, gx, other)

    pack_y_raw(0)
    send_y(0, raw_fields, yr_recv)
    corner_sums(0)
    own_sums(0, inner)
    send_y(0, sum_fields, ym_recv)
    if by_word:
        pl.semaphore_wait(in_sem, neighbours)
    send_corner_raw(0, (0, 1))
    send_corner_sums(0)
    if by_word:
        pl.semaphore_wait(col_sem, len(column) - neighbours)
    raw_near()
    sums_near()
    face_shares(0, (0, 1))
    edge_shares(0)
    send_heat()
    no_peak = jnp.zeros((ROW, nz), jnp.float32)
    await_y_raw(0)
    edge_moments(0)
    peak = velocity_pass(0, None, inner, no_peak)
    await_x_raw()
    finish_peak = spread_all(0, velocity_pass(0, None, outer, peak))
    edge_reads()
    await_y_sums(0)

    def store_st1(k, x, r, value):
        st1[k, x, pl.ds(ROW + r, ROW), :] = value

    def face(s):
        await_x_sums(0, s)
        ghost_x(0, None, s)
        ghost_y(0, None)
        collided([(x, r) for x, r in blocks if x == face_x[s]], None, store_st1)
        send_corner_raw(1, (s,))
        face_shares(1, (s,))
        send_x_shares(s)

    @pl.when(gx == ngx - 1)
    def _():
        face(1)
        face(0)

    @pl.when(gx != ngx - 1)
    def _():
        face(0)
        face(1)

    collided(inner, None, store_st1)
    pack_y_raw(1)
    send_y(1, raw_fields, yr_recv)
    own_sums(1, outer)
    for part in (*send_x_rest(), *send_x_sums(1)):
        part()
    own_sums(1, inner)
    send_y(1, sum_fields, ym_recv)
    corner_sums(1)
    send_corner_sums(1)
    send_heat_x(1)
    edge_shares(1)
    await_heat()
    near_heat()
    fs = finish_peak()
    await_y_raw(1)
    edge_moments(1)
    peak = velocity_pass(1, fs, inner, no_peak)
    await_bytes(None, xo_in, xo_recv)
    finish_peak = spread_all(1, velocity_pass(1, fs, outer, peak))
    for x, r in blocks:
        for c in range(3):
            out_v[c, x, pl.ds(r, ROW), :] = vel[c, x + 1, pl.ds(ROW + r, ROW), :]
    await_bytes(None, hb.at[pl.ds(0, 2), own_y, :], hx_recv.at[1])
    far_heat()
    await_x_rest()
    for s in (0, 1):
        for r in range(0, sy, ROW):
            face_reads(s, r, face_rest(s, r))
    edge_reads()
    await_y_sums(1)
    for s in (0, 1):
        await_x_sums(1, s)
        ghost_x(1, fs, s)
    ghost_y(1, fs)

    def store_out(k, x, r, value):
        out_p[k, x, pl.ds(r, ROW), :] = value

    collided(blocks, fs, store_out)
    await_sends()
    fs = finish_peak()
    await_peak_sends()
    lift = {(x, r): fs * hb[x + 2, pl.ds(ROW + r, ROW), :] for x, r in blocks}
    for k in LIFTED:
        for x, r in blocks:
            rows = pl.ds(r, ROW)
            out_p[k, x, rows, :] = out_p[k, x, rows, :] + (3.0 * WEIGHT[k] * CS[k][2]) * lift[(x, r)]


def write_out(pops, vel, out_p, out_v, sems):
    copies = [
        pltpu.make_async_copy(pops, out_p, sems.at[0]),
        pltpu.make_async_copy(vel, out_v, sems.at[1]),
    ]
    for copy in copies:
        copy.start()
    for copy in copies:
        copy.wait()


def local(populations, heat_level, obstacle, heat_table):
    ngx = lax.axis_size("gx")
    ngy = lax.axis_size("gy")
    _, sx, sy, nz = populations.shape
    f32 = jnp.float32
    tall = sy + 2 * ROW
    dma = pltpu.SemaphoreType.DMA
    groups = peak_groups(ngx, ngy)
    phases = len(groups)
    vmem = pl.BlockSpec(memory_space=pltpu.VMEM)
    anywhere = pl.BlockSpec(memory_space=pltpu.HBM)
    shapes = (
        jax.ShapeDtypeStruct(populations.shape, f32),
        jax.ShapeDtypeStruct((3, sx, sy, nz), f32),
    )

    def floats(*shape):
        return pltpu.VMEM(shape, f32)

    def ints(*shape):
        return pltpu.VMEM(shape, jnp.int32)

    pops, velocity = pl.pallas_call(
        functools.partial(kernel, ngx, ngy),
        out_shape=shapes,
        in_specs=[anywhere] * 4,
        out_specs=[vmem] * 2,
        scratch_shapes=[
            floats(19, sx, tall, nz),
            floats(19, sx, tall, nz),
            floats(19, sx, sy, nz),
            floats(4, sx, sy, nz),
            floats(sx, sy, nz),
            floats(3, sx + 2, tall, nz),
            ints(sx, sy, nz),
            ints(sx, sy, nz),
            pltpu.SMEM(heat_table.shape, f32),
            ints(sx, sy, nz),
            floats(sx + 4, tall, nz),
            floats(sx + 4, tall, nz),
            floats(sx + 4, tall, nz),
            floats(4, sx + 2, sy, nz),
            floats(4, 2 * sx, nz),
            floats(2, 5, tall, nz),
            floats(2, 5, sy, nz),
            floats(STEPS, 2, 4, sy, nz),
            floats(STEPS, 2, 4, sy, nz),
            floats(STEPS, 9, 2 * sx, nz),
            floats(STEPS, 9, 2 * sx, nz),
            floats(8, ROW, nz),
            floats(STEPS, 6, ROW, nz),
            floats(STEPS, ROW, nz),
            floats(STEPS, 6, ROW, nz),
            floats(2, 3, sy, nz),
            floats(2, 2 * sy + ROW, nz),
            floats(2, 3, sy, nz),
            floats(2, 2 * sy + ROW, nz),
            floats(4, 2 * sx, nz),
            floats(5, 2 * sx, nz),
            floats(4, 2 * sx, nz),
            floats(2, ROW, nz),
            floats(4, ROW, nz),
            floats(4, 2 * sx, nz),
            floats(2, sy, nz),
            floats(2 * sx, nz),
            floats(8 * ROW, nz),
            floats(STEPS, phases, 1, nz),
            *[floats(STEPS, -(-len(group) // ROW) * ROW, nz) for group in groups],
            dma((4,)),
            pltpu.SemaphoreType.REGULAR,
            pltpu.SemaphoreType.REGULAR,
            dma,
            dma((2,)),
            dma((STEPS,)),
            dma((STEPS, 2)),
            dma,
            dma((STEPS, 2)),
            dma((STEPS, 2)),
            dma((STEPS, 4)),
            dma((2,)),
            dma((2,)),
            dma((phases,)),
            dma((STEPS, phases)),
        ],
        compiler_params=pltpu.CompilerParams(
            collective_id=0, has_side_effects=True, vmem_limit_bytes=24 * 1024 * 1024
        ),
        name="lattice_steps",
    )(*[pltpu.with_memory_space_constraint(a, pltpu.HBM) for a in (populations, heat_level, obstacle, heat_table)])
    return pl.pallas_call(
        write_out,
        out_shape=shapes,
        in_specs=[vmem] * 2,
        out_specs=[anywhere] * 2,
        scratch_shapes=[dma((2,))],
        compiler_params=pltpu.CompilerParams(vmem_limit_bytes=8 * 1024 * 1024),
        name="write_out",
    )(pops, velocity)


def solution(mesh):
    return jax.shard_map(
        local,
        mesh=mesh,
        in_specs=(
            P(None, ("member", "gx"), "gy", None),
            P(("member", "gx"), "gy", None),
            P(("member", "gx"), "gy", None),
            P(),
        ),
        out_specs=(P(None, ("member", "gx"), "gy", None), P(None, ("member", "gx"), "gy", None)),
        check_vma=False,
    )
```
